512 devices in a mesh: cons: 16 (over y, x_lo), blk: 32 (over x_hi, z, core).
Axes of the slice: x: 4 (x_hi: 2, x_lo: 2; x = x_hi * 2 + x_lo), y: 8, z: 8, core: 2. Of those that a mesh axis runs over, the one named last changes fastest.
Arguments:
- elevation: bfloat16 [16, 1280, 6144], P('cons', 'blk'), may hold values from -6 to 6
- legendre: bfloat16 [1280, 768, 768], P('blk', 'cons'), may hold values from -5 to 5, as said below
- cycle_weight: float32 [1280], P('blk'), may hold values from 0.0001782951 to 0.0014263608
- love_factor: float32 [768], replicated, may hold values from 0.000390625 to 0.0052083335
- assignment: int32 [16], replicated, may hold values from 0 to 15, each once
Outputs:
- loading: float32 [16, 1280, 6144], P('cons', 'blk')
The draws below stay inside these ranges and needn't reach their ends.
Inputs may be any that keep to these rules, and one draw needn't show every extreme that they name: `legendre`: fully normalized associated Legendre functions (the square integrates to 1 over [-1, 1]) of each cycle's latitude, every cycle within 26 degrees of the equator; zero where the degree is below the order.
All inputs are finite; a program needn't handle non-finite values.
Results may differ from the reference program's by a relative error of at most 0.02.
Values may be sent and summed in bfloat16 or wider, within the bound.
No kernel may reach another device: no remote copies, remote signals or barrier semaphores. Data moves between devices by JAX's collectives and lax.ppermute only.
A program may use at most 128 MiB of HBM per device.

```python
import math
import jax
import jax.numpy as jnp
from jax import lax

FIELDS = 16
DEGREES = 768
ORDERS = 768
LONS = 6144
CYCLE_DEV = 40
CYCLES = 1280
N_BLK = 32


def draw_legendre(key, part):
    cosine_vals = jax.random.uniform(jax.random.fold_in(key, 11), (CYCLES,), jnp.float32, -0.43, 0.43)
    sine_vals = jnp.sqrt(1.0 - cosine_vals * cosine_vals)
    order_vals = jnp.arange(ORDERS).astype(jnp.float32)
    growth = 0.5 * jnp.log((2.0 * order_vals + 1.0) / jnp.maximum(2.0 * order_vals, 1.0))
    log_steps = jnp.where(order_vals[None, :] > 0.0, growth[None, :] + jnp.log(sine_vals)[:, None], 0.0)
    diagonal = jnp.exp(0.5 * jnp.log(0.5) + jnp.cumsum(log_steps, axis=1))
    order_sq = order_vals[None, :] * order_vals[None, :]

    def advance(state, degree):
        previous, earlier = state
        level = degree.astype(jnp.float32)
        coef_now = jnp.sqrt((4.0 * level * level - 1.0) / jnp.maximum(level * level - order_sq, 1.0))
        lower = level - 1.0
        coef_before = jnp.sqrt(jnp.maximum(4.0 * lower * lower - 1.0, 1.0) / jnp.maximum(lower * lower - order_sq, 1.0))
        generic = coef_now * (cosine_vals[:, None] * previous - earlier / coef_before)
        first_up = jnp.sqrt(2.0 * order_vals[None, :] + 3.0) * cosine_vals[:, None] * previous
        values = jnp.where(level == order_vals[None, :], diagonal, jnp.where(level == order_vals[None, :] + 1.0, first_up, jnp.where(level > order_vals[None, :] + 1.0, generic, 0.0)))
        return ((values, previous), values)
    zeros = jnp.zeros((CYCLES, ORDERS), jnp.float32)
    _, table = lax.scan(advance, (zeros, zeros), jnp.arange(DEGREES, dtype=jnp.int32))
    return jnp.transpose(table, (1, 2, 0)).astype(jnp.bfloat16)


def level_of(own_key, dims, shards, smallest, high):
    def one(dim, shards_of):
        steps = jax.random.uniform(jax.random.fold_in(jax.random.fold_in(own_key, 6), dim), (shards_of,), jnp.float32, smallest / len(shards), high / len(shards))
        return jnp.repeat(jnp.exp(steps), dims[dim] // shards_of).reshape((-1,) + (1,) * (len(dims) - dim - 1))

    level = one(*shards[0])
    for cut in shards[1:]:
        level = level * one(*cut)
    return level


def normal_values(own_key, dims, deviation, bound, split=(), kind=jnp.bfloat16):
    entries = jax.random.normal(own_key, dims, jnp.float32) * deviation
    if len(split) > 0:
        entries = level_of(own_key, dims, split, -0.22, 0.18) * entries
    return jnp.clip(entries, min=-bound, max=bound).astype(kind)


def setup_inputs(seed: int = 0) -> dict:
    keys = jax.random.split(jax.random.key(seed), 6)
    return {
        "elevation": normal_values(keys[0], (FIELDS, CYCLES, LONS), 1.0, 6.0, ((0, 16), (1, 32))),
        "legendre": draw_legendre(jax.random.fold_in(keys[5], 71), 0),
        "cycle_weight": jnp.clip(jnp.exp(math.log(0.0014263608) - 2.0794415 * jax.random.uniform(keys[2], (CYCLES,), jnp.float32) ** level_of(keys[2], (CYCLES,), ((0, 32),), -0.2, 0.2)), 0.0001782951, 0.0014263608),
        "love_factor": jnp.clip(jnp.exp(jax.random.uniform(keys[3], (DEGREES,), jnp.float32, math.log(0.000390625), math.log(0.0052083335))), 0.000390625, 0.0052083335),
        "assignment": jax.random.permutation(keys[4], FIELDS).astype(jnp.int32),
    }


def fourier_block(offset, length, period, orders):
    lon_index = offset + jnp.arange(length, dtype=jnp.int32)
    order_index = jnp.arange(orders, dtype=jnp.int32)
    phases = (lon_index[:, None] * order_index[None, :]) % period
    angles = phases.astype(jnp.float32) * jnp.float32(2.0 * 3.141592653589793 / period)
    stacked = jnp.stack([jnp.cos(angles), -jnp.sin(angles)], axis=2)
    return stacked.reshape(length, 2 * orders).astype(jnp.bfloat16)


def reference(elevation, legendre, cycle_weight, love_factor, assignment):
    table = fourier_block(0, LONS, LONS, ORDERS)

    def forward(field):
        summed = jnp.dot(field, table, preferred_element_type=jnp.float32)
        return (summed * cycle_weight[:, None]).astype(jnp.bfloat16)

    spectra = lax.map(forward, elevation)
    ordered = spectra[assignment].reshape(FIELDS, CYCLES, ORDERS, 2)

    def add_block(running, block_index):
        start = (block_index * CYCLE_DEV).astype(jnp.int32)
        values = lax.dynamic_slice_in_dim(legendre, start, CYCLE_DEV, 0).astype(jnp.float32)
        spec_block = lax.dynamic_slice_in_dim(ordered, start, CYCLE_DEV, 1).astype(jnp.float32)
        partial_value = jnp.einsum('jml,gjmp->lpgm', values, spec_block)
        rounded = lax.optimization_barrier(partial_value.astype(jnp.bfloat16))
        return running + rounded.astype(jnp.float32), None

    zeros = jnp.zeros((DEGREES, 2, FIELDS, ORDERS), jnp.float32)
    analysis, _ = lax.scan(add_block, zeros, jnp.arange(N_BLK, dtype=jnp.int32))
    coefficients = (analysis * love_factor[:, None, None, None]).astype(jnp.bfloat16)
    order_factor = jnp.where(jnp.arange(ORDERS) == 0, 1.0, 2.0).astype(jnp.float32)

    def synth_block(block_index):
        start = (block_index * CYCLE_DEV).astype(jnp.int32)
        values = lax.dynamic_slice_in_dim(legendre, start, CYCLE_DEV, 0).astype(jnp.float32)
        summed = jnp.einsum('jml,lpgm->gjmp', values, coefficients.astype(jnp.float32))
        return (summed * order_factor[None, None, :, None]).astype(jnp.bfloat16)

    blocks = lax.map(synth_block, jnp.arange(N_BLK, dtype=jnp.int32))
    synthesis = jnp.moveaxis(blocks, 0, 1).reshape(FIELDS, CYCLES, 2 * ORDERS)

    def inverse(field):
        return jnp.dot(field, table.T, preferred_element_type=jnp.float32)

    return lax.map(inverse, synthesis)
```

```python
import functools

import jax
import jax.numpy as jnp
import numpy as np
from jax import lax
from jax.experimental import pallas as pl
from jax.experimental.pallas import tpu as pltpu
from jax.sharding import Mesh
from jax.sharding import PartitionSpec as P

BLK = ("blk_0", "blk_1", "blk_2")
FAR = ("blk_0", "blk_1")
TEAM = ("cons", "blk_2")
FINE = 16
INNER = FINE * FINE


def angle_tables(steps, stride, period, orders):
    phases = (np.arange(steps)[:, None] * stride * np.arange(orders)[None, :]) % period
    angles = phases * (2.0 * np.pi / period)
    return np.stack([np.cos(angles), np.sin(angles)]).astype(np.float32)


def inner_table(coarse_ref, fine_ref, table_ref, lanes):
    fine_cos, fine_sin = fine_ref[0, :, lanes], fine_ref[1, :, lanes]
    for step in range(FINE):
        rows = slice(step * FINE, (step + 1) * FINE)
        coarse_cos = coarse_ref[0, step : step + 1, lanes]
        coarse_sin = coarse_ref[1, step : step + 1, lanes]
        cosine = coarse_cos * fine_cos - coarse_sin * fine_sin
        sine = coarse_sin * fine_cos + coarse_cos * fine_sin
        table_ref[0, rows, lanes] = cosine.astype(jnp.bfloat16)
        table_ref[1, rows, lanes] = (-sine).astype(jnp.bfloat16)


def forward_kernel(
    elevation_ref, weight_ref, coarse_ref, fine_ref, turn_ref, out_ref, rows_ref, table_ref
):
    cycles = elevation_ref.shape[0]
    turns = turn_ref.shape[1]

    @pl.when(pl.program_id(0) == 0)
    def _():
        for turn in range(turns):
            rows_ref[turn * cycles : (turn + 1) * cycles, :] = elevation_ref[
                :, turn * INNER : (turn + 1) * INNER
            ]

    lanes = slice(None)
    inner_table(coarse_ref, fine_ref, table_ref, lanes)
    even = jnp.dot(rows_ref[...], table_ref[0], preferred_element_type=jnp.float32)
    odd = jnp.dot(rows_ref[...], table_ref[1], preferred_element_type=jnp.float32)
    first = second = None
    for turn in range(turns):
        rows = slice(turn * cycles, (turn + 1) * cycles)
        cosine, sine = turn_ref[0, turn : turn + 1, :], turn_ref[1, turn : turn + 1, :]
        one = even[rows] * cosine + odd[rows] * sine
        two = odd[rows] * cosine - even[rows] * sine
        first = one if first is None else first + one
        second = two if second is None else second + two
    weight = weight_ref[...]
    out_ref[0] = (first * weight).astype(jnp.bfloat16)
    out_ref[1] = (second * weight).astype(jnp.bfloat16)


def forward(elevation, weight, coarse, fine, turn):
    cycles, longitudes = elevation.shape
    orders = coarse.shape[2]
    turns = longitudes // INNER
    width = 256
    whole = lambda m: (0, 0)
    part = lambda m: (0, 0, m)
    return pl.pallas_call(
        forward_kernel,
        grid=(orders // width,),
        in_specs=[
            pl.BlockSpec((cycles, longitudes), whole),
            pl.BlockSpec((cycles, 1), whole),
            pl.BlockSpec((2, FINE, width), part),
            pl.BlockSpec((2, FINE, width), part),
            pl.BlockSpec((2, turns, width), part),
        ],
        out_specs=pl.BlockSpec((2, cycles, width), part),
        out_shape=jax.ShapeDtypeStruct((2, cycles, orders), jnp.bfloat16),
        scratch_shapes=[
            pltpu.VMEM((turns * cycles, INNER), jnp.bfloat16),
            pltpu.VMEM((2, INNER, width), jnp.bfloat16),
        ],
        cost_estimate=pl.CostEstimate(
            flops=4 * cycles * longitudes * orders, bytes_accessed=1 << 20, transcendentals=0
        ),
        name="forward_dft",
    )(elevation, weight, coarse, fine, turn)


def inverse_kernel(
    synthesis_ref, coarse_ref, fine_ref, turn_ref, out_ref, rows_ref, table_ref
):
    cycles = synthesis_ref.shape[1]
    count = out_ref.shape[1] // INNER

    @pl.when(pl.program_id(0) == 0)
    def _():
        inner_table(coarse_ref, fine_ref, table_ref, slice(None))

    first = synthesis_ref[0].astype(jnp.float32)
    second = synthesis_ref[1].astype(jnp.float32)
    base = pl.program_id(0) * count
    for step in range(count):
        rows = slice(step * cycles, (step + 1) * cycles)
        cosine = turn_ref[0, pl.ds(base + step, 1), :]
        sine = turn_ref[1, pl.ds(base + step, 1), :]
        rows_ref[0, rows, :] = (first * cosine - second * sine).astype(jnp.bfloat16)
        rows_ref[1, rows, :] = (first * sine + second * cosine).astype(jnp.bfloat16)
    dims = (((1,), (1,)), ((), ()))
    result = lax.dot_general(
        rows_ref[0], table_ref[0], dims, preferred_element_type=jnp.float32
    ) + lax.dot_general(rows_ref[1], table_ref[1], dims, preferred_element_type=jnp.float32)
    for step in range(count):
        out_ref[:, step * INNER : (step + 1) * INNER] = result[
            step * cycles : (step + 1) * cycles
        ]


def inverse(synthesis, coarse, fine, turn, longitudes):
    _, cycles, orders = synthesis.shape
    turns = longitudes // INNER
    count = 6
    whole = lambda a: (0, 0, 0)
    return pl.pallas_call(
        inverse_kernel,
        grid=(turns // count,),
        in_specs=[
            pl.BlockSpec((2, cycles, orders), whole),
            pl.BlockSpec((2, FINE, orders), whole),
            pl.BlockSpec((2, FINE, orders), whole),
            pl.BlockSpec((2, turns, orders), whole),
        ],
        out_specs=pl.BlockSpec((cycles, count * INNER), lambda a: (0, a)),
        out_shape=jax.ShapeDtypeStruct((cycles, longitudes), jnp.float32),
        scratch_shapes=[
            pltpu.VMEM((2, count * cycles, orders), jnp.bfloat16),
            pltpu.VMEM((2, INNER, orders), jnp.bfloat16),
        ],
        cost_estimate=pl.CostEstimate(
            flops=4 * cycles * longitudes * orders, bytes_accessed=1 << 20, transcendentals=0
        ),
        name="inverse_dft",
    )(synthesis, coarse, fine, turn)


def local(elevation, legendre, cycle_weight, love_factor, assignment):
    fld_dev, cycle_dev, longitudes = elevation.shape
    orders_dev, degrees = legendre.shape[1:]
    groups = lax.axis_size("cons")
    cores = lax.axis_size("blk_2")
    far = lax.axis_size("blk_0") * lax.axis_size("blk_1")
    orders = orders_dev * groups
    half = orders_dev // cores
    core = lax.axis_index("blk_2")
    coarse = jnp.asarray(angle_tables(FINE, FINE, longitudes, orders))
    fine = jnp.asarray(angle_tables(FINE, 1, longitudes, orders))
    turn = jnp.asarray(angle_tables(longitudes // INNER, INNER, longitudes, orders))

    def half_of(index):
        return lax.dynamic_slice_in_dim(legendre, index * half, half, 1)

    swapped = lax.ppermute(half_of(1 - core), "blk_2", [(0, 1), (1, 0)])
    own = half_of(core)
    is_first = core == 0
    values = jnp.stack(
        [jnp.where(is_first, own, swapped), jnp.where(is_first, swapped, own)], axis=0
    )

    spectra = forward(elevation[0], cycle_weight[:, None], coarse, fine, turn)
    outgoing = spectra.reshape(2, cycle_dev, groups * cores, half)
    outgoing = outgoing.transpose(2, 0, 1, 3).reshape(groups * cores, -1)
    moved = lax.all_to_all(outgoing, TEAM, 0, 0, tiled=True)
    moved = moved.reshape(groups, cores, 2, cycle_dev, half)
    one_hot = (
        assignment[:, None] == jnp.arange(groups, dtype=jnp.int32)[None, :]
    ).astype(jnp.bfloat16)
    ordered = jnp.einsum(
        "gf,fspjm->gspjm", one_hot, moved, preferred_element_type=jnp.float32
    ).astype(jnp.bfloat16)
    partial = jnp.einsum(
        "sjml,gspjm->mpgl", values, ordered, preferred_element_type=jnp.float32
    ).astype(jnp.bfloat16)
    lines = half * 2 * groups
    arrived = lax.all_to_all(
        partial.reshape(far, lines // far, degrees), FAR, 0, 0, tiled=True
    )
    analysis = jnp.sum(arrived.astype(jnp.float32), axis=0)
    scaled = (analysis * love_factor[None, :]).astype(jnp.bfloat16)
    copies = jnp.broadcast_to(scaled[None], (far, lines // far, degrees))
    coefficients = lax.all_to_all(copies, FAR, 0, 0, tiled=True)
    coefficients = coefficients.reshape(half, 2, groups, degrees)
    summed = jnp.einsum(
        "sjml,mpgl->gspjm", values, coefficients, preferred_element_type=jnp.float32
    )
    order_index = lax.axis_index("cons") * orders_dev + core * half + jnp.arange(half)
    order_factor = jnp.where(order_index == 0, 1.0, 2.0).astype(jnp.float32)
    synthesis = (summed * order_factor).astype(jnp.bfloat16)
    returned = lax.all_to_all(
        synthesis.reshape(groups * cores, -1), TEAM, 0, 0, tiled=True
    )
    returned = returned.reshape(groups * cores, 2, cycle_dev, half)
    returned = returned.transpose(1, 2, 0, 3).reshape(2, cycle_dev, orders)
    return inverse(returned, coarse, fine, turn, longitudes)[None]


def solution(mesh):
    torus = Mesh(
        mesh.devices.reshape(mesh.shape["cons"], 2, 8, 2), ("cons", "blk_0", "blk_1", "blk_2")
    )
    placed = (P("cons", BLK, None), P(BLK, "cons", None), P(BLK), P(), P())
    return jax.shard_map(
        local, mesh=torus, in_specs=placed, out_specs=P("cons", BLK, None), check_vma=False
    )
```

```python
import functools

import jax
import jax.numpy as jnp
import numpy as np
from jax import lax
from jax.experimental import pallas as pl
from jax.experimental.pallas import tpu as pltpu
from jax.sharding import Mesh
from jax.sharding import PartitionSpec as P

BLK = ("blk_0", "blk_1", "blk_2", "blk_3")
NEAR = ("blk_0", "blk_2", "blk_3")
FAR = "blk_1"
TEAM = ("cons", *NEAR)
FINE = 16
INNER = FINE * FINE
LANES = 128
NEAR_SIZE = 8
SHARE = 6


def angle_tables(steps, stride, period, orders):
    phases = (np.arange(steps)[:, None] * stride * np.arange(orders)[None, :]) % period
    angles = phases * (2.0 * np.pi / period)
    return np.stack([np.cos(angles), np.sin(angles)]).astype(np.float32)


def inner_table(coarse_ref, fine_ref, table_ref, lanes):
    fine_cos, fine_sin = fine_ref[0, :, lanes], fine_ref[1, :, lanes]
    for step in range(FINE):
        rows = slice(step * FINE, (step + 1) * FINE)
        coarse_cos = coarse_ref[0, step : step + 1, lanes]
        coarse_sin = coarse_ref[1, step : step + 1, lanes]
        cosine = coarse_cos * fine_cos - coarse_sin * fine_sin
        sine = coarse_sin * fine_cos + coarse_cos * fine_sin
        table_ref[0, rows, lanes] = cosine.astype(jnp.bfloat16)
        table_ref[1, rows, lanes] = (-sine).astype(jnp.bfloat16)


def shift(values, amount):
    amount %= LANES
    return values if amount == 0 else pltpu.roll(values, amount, values.ndim - 1)


def side_by_side(pieces, width):
    lane = lax.broadcasted_iota(jnp.int32, pieces[0].shape, pieces[0].ndim - 1)
    joined = jnp.zeros_like(pieces[0])
    for index, piece in reversed(list(enumerate(pieces))):
        joined = jnp.where(lane < (index + 1) * width, shift(piece, index * width), joined)
    return jnp.where(lane < len(pieces) * width, joined, 0.0)


def forward_kernel(
    elevation_ref,
    weight_ref,
    coarse_ref,
    fine_ref,
    turn_ref,
    out_ref,
    rows_ref,
    table_ref,
    flip_ref,
    pack_ref,
):
    cycles = elevation_ref.shape[0]
    turns = turn_ref.shape[1]
    width = coarse_ref.shape[2]
    orders = flip_ref.shape[1]
    part = pl.program_id(0)

    @pl.when(part == 0)
    def _():
        for turn in range(turns):
            rows_ref[turn * cycles : (turn + 1) * cycles, :] = elevation_ref[
                :, turn * INNER : (turn + 1) * INNER
            ]

    inner_table(coarse_ref, fine_ref, table_ref, slice(None))
    even = jnp.dot(rows_ref[...], table_ref[0], preferred_element_type=jnp.float32)
    odd = jnp.dot(rows_ref[...], table_ref[1], preferred_element_type=jnp.float32)
    first = second = None
    for turn in range(turns):
        rows = slice(turn * cycles, (turn + 1) * cycles)
        cosine, sine = turn_ref[0, turn : turn + 1, :], turn_ref[1, turn : turn + 1, :]
        one = even[rows] * cosine + odd[rows] * sine
        two = odd[rows] * cosine - even[rows] * sine
        first = one if first is None else first + one
        second = two if second is None else second + two
    weight = weight_ref[...]
    here = pl.ds(pl.multiple_of(part * width, width), width)
    flip_ref[0, here, :cycles] = jnp.transpose(first * weight)
    flip_ref[1, here, :cycles] = jnp.transpose(second * weight)

    @pl.when(part == pl.num_programs(0) - 1)
    def _():
        beside = LANES // cycles
        lines = out_ref.shape[0]
        share = SHARE
        peers = orders // share
        deep = lines // peers
        for row in range(deep):
            pieces = []
            for column in range(beside):
                which, order = divmod(deep * column + row, share)
                pieces.append(flip_ref[which, pl.ds(order, peers, stride=share), :])
            pack_ref[pl.ds(row, peers, stride=deep), :] = side_by_side(pieces, cycles)
        out_ref[...] = pack_ref[...].astype(jnp.bfloat16)


def forward(elevation, weight, coarse, fine, turn, lines):
    cycles, longitudes = elevation.shape
    orders = coarse.shape[2]
    turns = longitudes // INNER
    width = 256
    whole = lambda m: (0, 0)
    part = lambda m: (0, 0, m)
    return pl.pallas_call(
        forward_kernel,
        grid=(orders // width,),
        in_specs=[
            pl.BlockSpec((cycles, longitudes), whole),
            pl.BlockSpec((cycles, 1), whole),
            pl.BlockSpec((2, FINE, width), part),
            pl.BlockSpec((2, FINE, width), part),
            pl.BlockSpec((2, turns, width), part),
        ],
        out_specs=pl.BlockSpec((lines, LANES), whole),
        out_shape=jax.ShapeDtypeStruct((lines, LANES), jnp.bfloat16),
        scratch_shapes=[
            pltpu.VMEM((turns * cycles, INNER), jnp.bfloat16),
            pltpu.VMEM((2, INNER, width), jnp.bfloat16),
            pltpu.VMEM((2, orders, LANES), jnp.float32),
            pltpu.VMEM((lines, LANES), jnp.float32),
        ],
        cost_estimate=pl.CostEstimate(
            flops=4 * cycles * longitudes * orders, bytes_accessed=1 << 20, transcendentals=0
        ),
        name="forward_dft",
    )(elevation, weight, coarse, fine, turn)


def analysis_kernel(spot_ref, *refs):
    near = NEAR_SIZE
    assignment_ref, moved_ref, *value_refs = refs[: near + 2]
    out_ref, row_ref, left_ref = refs[near + 2 :]
    share, _, two_fields, _ = left_ref.shape
    fields = two_fields // 2
    cycles = value_refs[0].shape[1]
    beside = LANES // cycles
    lines = moved_ref.shape[0]
    block = lines // fields
    deep = block // near
    spot = spot_ref[0]

    @pl.when(pl.program_id(0) == 0)
    def _():
        for slot in range(fields):
            source = pl.multiple_of(assignment_ref[slot] * block, block)
            row_ref[slot * block : (slot + 1) * block, :] = moved_ref[
                pl.ds(source, block), :
            ].astype(jnp.float32)
        for other in range(near):
            peer = jnp.bitwise_xor(spot, other)
            for row in range(deep):
                taken = row_ref[pl.ds(peer * deep + row, fields, stride=block), :]
                for column in range(beside):
                    which, order = divmod(deep * column + row, share)
                    left_ref[order, other, which * fields : (which + 1) * fields, :] = shift(
                        taken, -column * cycles
                    ).astype(jnp.bfloat16)

    order = pl.program_id(0)
    total = None
    for other in range(near):
        product = jnp.dot(
            left_ref[order, other][:, :cycles],
            value_refs[other][0],
            preferred_element_type=jnp.float32,
        )
        total = product if total is None else total + product
    out_ref[...] = total.astype(jnp.bfloat16)


def analyse(spot, assignment, moved, values):
    share, cycles, degrees = values[0].shape
    fields = assignment.shape[0]
    return pl.pallas_call(
        analysis_kernel,
        grid_spec=pltpu.PrefetchScalarGridSpec(
            num_scalar_prefetch=2,
            grid=(share,),
            in_specs=[pl.BlockSpec(moved.shape, lambda m, *_: (0, 0))]
            + [pl.BlockSpec((1, cycles, degrees), lambda m, *_: (m, 0, 0))] * len(values),
            out_specs=pl.BlockSpec((2 * fields, degrees), lambda m, *_: (m, 0)),
            scratch_shapes=[
                pltpu.VMEM(moved.shape, jnp.float32),
                pltpu.VMEM((share, len(values), 2 * fields, LANES), jnp.bfloat16),
            ],
        ),
        out_shape=jax.ShapeDtypeStruct((share * 2 * fields, degrees), jnp.bfloat16),
        cost_estimate=pl.CostEstimate(
            flops=4 * fields * share * cycles * degrees * len(values),
            bytes_accessed=4 << 20,
            transcendentals=0,
        ),
        name="analysis",
    )(spot, assignment, moved, *values)


def synthesis_kernel(spot_ref, first_ref, *refs):
    near = NEAR_SIZE
    coefficient_ref, *value_refs = refs[: near + 1]
    out_ref, right_ref, row_ref = refs[near + 1 :]
    share, _, two_fields, _ = right_ref.shape
    fields = two_fields // 2
    cycles = value_refs[0].shape[1]
    beside = LANES // cycles
    lines = out_ref.shape[0]
    block = lines // fields
    deep = block // near
    order = pl.program_id(0)
    factor = jnp.where(first_ref[0] + order == 0, 1.0, 2.0).astype(jnp.float32)
    dims = (((1,), (1,)), ((), ()))
    for other in range(near):
        product = lax.dot_general(
            coefficient_ref[...], value_refs[other][0], dims, preferred_element_type=jnp.float32
        )
        right_ref[order, other, :, :cycles] = product * factor

    @pl.when(order == pl.num_programs(0) - 1)
    def _():
        for other in range(near):
            peer = jnp.bitwise_xor(spot_ref[0], other)
            for row in range(deep):
                pieces = []
                for column in range(beside):
                    which, own = divmod(deep * column + row, share)
                    pieces.append(
                        right_ref[own, other, which * fields : (which + 1) * fields, :]
                    )
                row_ref[pl.ds(peer * deep + row, fields, stride=block), :] = side_by_side(
                    pieces, cycles
                )
        out_ref[...] = row_ref[...].astype(jnp.bfloat16)


def synthesise(spot, first, coefficients, values, lines):
    share, cycles, degrees = values[0].shape
    fields = coefficients.shape[0] // (2 * share)
    return pl.pallas_call(
        synthesis_kernel,
        grid_spec=pltpu.PrefetchScalarGridSpec(
            num_scalar_prefetch=2,
            grid=(share,),
            in_specs=[pl.BlockSpec((2 * fields, degrees), lambda m, *_: (m, 0))]
            + [pl.BlockSpec((1, cycles, degrees), lambda m, *_: (m, 0, 0))] * len(values),
            out_specs=pl.BlockSpec((lines, LANES), lambda m, *_: (0, 0)),
            scratch_shapes=[
                pltpu.VMEM((share, len(values), 2 * fields, LANES), jnp.float32),
                pltpu.VMEM((lines, LANES), jnp.float32),
            ],
        ),
        out_shape=jax.ShapeDtypeStruct((lines, LANES), jnp.bfloat16),
        cost_estimate=pl.CostEstimate(
            flops=4 * fields * share * cycles * degrees * len(values),
            bytes_accessed=4 << 20,
            transcendentals=0,
        ),
        name="synthesis",
    )(spot, first, coefficients, *values)


def inverse_kernel(
    moved_ref, coarse_ref, fine_ref, turn_ref, out_ref, rows_ref, table_ref, row_ref, flip_ref, wave_ref
):
    cycles = out_ref.shape[0]
    count = out_ref.shape[1] // INNER
    orders = wave_ref.shape[2]

    @pl.when(pl.program_id(0) == 0)
    def _():
        inner_table(coarse_ref, fine_ref, table_ref, slice(None))
        row_ref[...] = moved_ref[...].astype(jnp.float32)
        share = SHARE
        peers = orders // share
        deep = moved_ref.shape[0] // peers
        for row in range(deep):
            taken = row_ref[pl.ds(row, peers, stride=deep), :]
            for column in range(LANES // cycles):
                which, order = divmod(deep * column + row, share)
                flip_ref[which, pl.ds(order, peers, stride=share), :] = shift(
                    taken, -column * cycles
                )
        wave_ref[0] = jnp.transpose(flip_ref[0])[:cycles]
        wave_ref[1] = jnp.transpose(flip_ref[1])[:cycles]

    first, second = wave_ref[0], wave_ref[1]
    base = pl.program_id(0) * count
    for step in range(count):
        rows = slice(step * cycles, (step + 1) * cycles)
        cosine = turn_ref[0, pl.ds(base + step, 1), :]
        sine = turn_ref[1, pl.ds(base + step, 1), :]
        rows_ref[0, rows, :] = (first * cosine - second * sine).astype(jnp.bfloat16)
        rows_ref[1, rows, :] = (first * sine + second * cosine).astype(jnp.bfloat16)
    dims = (((1,), (1,)), ((), ()))
    result = lax.dot_general(
        rows_ref[0], table_ref[0], dims, preferred_element_type=jnp.float32
    ) + lax.dot_general(rows_ref[1], table_ref[1], dims, preferred_element_type=jnp.float32)
    for step in range(count):
        out_ref[:, step * INNER : (step + 1) * INNER] = result[
            step * cycles : (step + 1) * cycles
        ]


def inverse(moved, coarse, fine, turn, cycles, longitudes):
    orders = coarse.shape[2]
    turns = longitudes // INNER
    count = 6
    whole = lambda a: (0, 0, 0)
    return pl.pallas_call(
        inverse_kernel,
        grid=(turns // count,),
        in_specs=[
            pl.BlockSpec(moved.shape, lambda a: (0, 0)),
            pl.BlockSpec((2, FINE, orders), whole),
            pl.BlockSpec((2, FINE, orders), whole),
            pl.BlockSpec((2, turns, orders), whole),
        ],
        out_specs=pl.BlockSpec((cycles, count * INNER), lambda a: (0, a)),
        out_shape=jax.ShapeDtypeStruct((cycles, longitudes), jnp.float32),
        scratch_shapes=[
            pltpu.VMEM((2, count * cycles, orders), jnp.bfloat16),
            pltpu.VMEM((2, INNER, orders), jnp.bfloat16),
            pltpu.VMEM(moved.shape, jnp.float32),
            pltpu.VMEM((2, orders, LANES), jnp.float32),
            pltpu.VMEM((2, cycles, orders), jnp.float32),
        ],
        cost_estimate=pl.CostEstimate(
            flops=4 * cycles * longitudes * orders, bytes_accessed=1 << 20, transcendentals=0
        ),
        name="inverse_dft",
    )(moved, coarse, fine, turn)


def local(elevation, legendre, cycle_weight, love_factor, assignment):
    fld_dev, cycle_dev, longitudes = elevation.shape
    orders_dev, degrees = legendre.shape[1:]
    groups = lax.axis_size("cons")
    near = lax.axis_size(NEAR)
    far = lax.axis_size(FAR)
    orders = orders_dev * groups
    share = orders_dev // near
    spot = lax.axis_index(NEAR)
    coarse = jnp.asarray(angle_tables(FINE, FINE, longitudes, orders))
    fine = jnp.asarray(angle_tables(FINE, 1, longitudes, orders))
    turn = jnp.asarray(angle_tables(longitudes // INNER, INNER, longitudes, orders))

    by_order = legendre.transpose(1, 0, 2).reshape(near, share, cycle_dev, degrees)

    def chunk(other):
        return lax.dynamic_index_in_dim(by_order, spot ^ other, 0, keepdims=False)

    values = [chunk(0)] + [None] * (near - 1)
    for other in reversed(range(1, near)):
        values[other] = lax.ppermute(
            chunk(other), NEAR, [(index, index ^ other) for index in range(near)]
        )

    deep = 2 * share // (LANES // cycle_dev)
    peers = groups * near
    lines = peers * deep

    def exchanged(packed):
        tiles = packed.reshape(peers, deep, LANES)
        return lax.all_to_all(tiles, TEAM, 0, 0, tiled=True).reshape(lines, LANES)

    packed = forward(elevation[0], cycle_weight[:, None], coarse, fine, turn, lines)
    moved = exchanged(packed)
    spot_row = spot[None].astype(jnp.int32)
    partial = analyse(spot_row, assignment, moved, values)
    rows = partial.shape[0] // far
    arrived = lax.all_to_all(partial.reshape(far, rows, degrees), FAR, 0, 0, tiled=True)
    analysis = jnp.sum(arrived.astype(jnp.float32), axis=0)
    scaled = (analysis * love_factor[None, :]).astype(jnp.bfloat16)
    copies = jnp.broadcast_to(scaled[None], (far, rows, degrees))
    coefficients = lax.all_to_all(copies, FAR, 0, 0, tiled=True).reshape(-1, degrees)
    first = ((lax.axis_index("cons") * near + spot) * share)[None].astype(jnp.int32)
    synthesis = synthesise(spot_row, first, coefficients, values, lines)
    returned = exchanged(synthesis)
    return inverse(returned, coarse, fine, turn, cycle_dev, longitudes)[None]


def solution(mesh):
    torus = Mesh(
        mesh.devices.reshape(mesh.shape["cons"], 2, 4, 2, 2), ("cons", *BLK)
    )
    placed = (P("cons", BLK, None), P(BLK, "cons", None), P(BLK), P(), P())
    return jax.shard_map(
        local, mesh=torus, in_specs=placed, out_specs=P("cons", BLK, None), check_vma=False
    )
```

```python
import jax
import jax.numpy as jnp
import numpy as np
from jax import lax
from jax.experimental import pallas as pl
from jax.experimental.pallas import tpu as pltpu
from jax.sharding import Mesh
from jax.sharding import PartitionSpec as P

BLK = ("blk_0", "blk_1", "blk_2", "blk_3")
NEAR = ("blk_0", "blk_2", "blk_3")
FAR = "blk_1"
TEAM = ("cons", *NEAR)
FINE = 16
INNER = FINE * FINE
LANES = 128
NEAR_SIZE = 8
SHARE = 6
EARLY = (6, 7)
LATE = (4, 2, 5, 3, 1)
ROOM = 24 << 20
SCALARS = pl.BlockSpec(memory_space=pltpu.SMEM)
NEARBY = pl.BlockSpec(memory_space=pltpu.VMEM)


def angle_tables(steps, stride, period, orders):
    phases = (np.arange(steps)[:, None] * stride * np.arange(orders)[None, :]) % period
    angles = phases * (2.0 * np.pi / period)
    return np.stack([np.cos(angles), np.sin(angles)]).astype(np.float32)


def inner_table(coarse_ref, fine_ref, table_ref, lanes):
    fine_cos, fine_sin = fine_ref[0, :, lanes], fine_ref[1, :, lanes]
    for step in range(FINE):
        rows = slice(step * FINE, (step + 1) * FINE)
        coarse_cos = coarse_ref[0, step : step + 1, lanes]
        coarse_sin = coarse_ref[1, step : step + 1, lanes]
        cosine = coarse_cos * fine_cos - coarse_sin * fine_sin
        sine = coarse_sin * fine_cos + coarse_cos * fine_sin
        table_ref[0, rows, lanes] = cosine.astype(jnp.bfloat16)
        table_ref[1, rows, lanes] = (-sine).astype(jnp.bfloat16)


def shift(values, amount):
    amount %= LANES
    return values if amount == 0 else pltpu.roll(values, amount, values.ndim - 1)


def side_by_side(pieces, width):
    lane = lax.broadcasted_iota(jnp.int32, pieces[0].shape, pieces[0].ndim - 1)
    joined = jnp.zeros_like(pieces[0])
    for index, piece in reversed(list(enumerate(pieces))):
        joined = jnp.where(lane < (index + 1) * width, shift(piece, index * width), joined)
    return jnp.where(lane < len(pieces) * width, joined, 0.0)


def forward_kernel(
    elevation_ref,
    weight_ref,
    coarse_ref,
    fine_ref,
    turn_ref,
    out_ref,
    rows_ref,
    table_ref,
    flip_ref,
    pack_ref,
):
    cycles = elevation_ref.shape[0]
    turns = turn_ref.shape[1]
    orders = flip_ref.shape[1]
    for turn in range(turns):
        rows_ref[turn * cycles : (turn + 1) * cycles, :] = elevation_ref[
            :, turn * INNER : (turn + 1) * INNER
        ]
    weight = weight_ref[...]
    inner_table(coarse_ref, fine_ref, table_ref, slice(None))
    for part in range(orders // INNER):
        lanes = slice(part * INNER, (part + 1) * INNER)
        even = jnp.dot(rows_ref[...], table_ref[0, :, lanes], preferred_element_type=jnp.float32)
        odd = jnp.dot(rows_ref[...], table_ref[1, :, lanes], preferred_element_type=jnp.float32)
        first = second = None
        for turn in range(turns):
            rows = slice(turn * cycles, (turn + 1) * cycles)
            cosine, sine = turn_ref[0, turn : turn + 1, lanes], turn_ref[1, turn : turn + 1, lanes]
            one = even[rows] * cosine + odd[rows] * sine
            two = odd[rows] * cosine - even[rows] * sine
            first = one if first is None else first + one
            second = two if second is None else second + two
        flip_ref[0, lanes, :cycles] = jnp.transpose(first * weight)
        flip_ref[1, lanes, :cycles] = jnp.transpose(second * weight)

    beside = LANES // cycles
    peers = orders // SHARE
    deep = out_ref.shape[0] // peers
    for row in range(deep):
        pieces = []
        for column in range(beside):
            which, order = divmod(deep * column + row, SHARE)
            pieces.append(flip_ref[which, pl.ds(order, peers, stride=SHARE), :])
        pack_ref[pl.ds(row, peers, stride=deep), :] = side_by_side(pieces, cycles)
    out_ref[...] = pack_ref[...].astype(jnp.bfloat16)


def forward(elevation, weight, coarse, fine, turn, lines):
    cycles, longitudes = elevation.shape
    orders = coarse.shape[2]
    turns = longitudes // INNER
    return pl.pallas_call(
        forward_kernel,
        in_specs=[NEARBY] * 5,
        out_specs=NEARBY,
        out_shape=jax.ShapeDtypeStruct((lines, LANES), jnp.bfloat16),
        scratch_shapes=[
            pltpu.VMEM((turns * cycles, INNER), jnp.bfloat16),
            pltpu.VMEM((2, INNER, orders), jnp.bfloat16),
            pltpu.VMEM((2, orders, LANES), jnp.float32),
            pltpu.VMEM((lines, LANES), jnp.float32),
        ],
        cost_estimate=pl.CostEstimate(
            flops=4 * cycles * longitudes * orders, bytes_accessed=1 << 20, transcendentals=0
        ),
        compiler_params=pltpu.CompilerParams(vmem_limit_bytes=ROOM),
        name="forward_dft",
    )(elevation, weight, coarse, fine, turn)


def analysis_kernel(spot_ref, *refs):
    near = NEAR_SIZE
    assignment_ref, moved_ref, *value_refs = refs[: near + 2]
    out_ref, row_ref, left_ref, joined_ref = refs[near + 2 :]
    share, _, two_fields, _ = left_ref.shape
    fields = two_fields // 2
    cycles = value_refs[0].shape[1]
    beside = LANES // cycles
    lines = moved_ref.shape[0]
    block = lines // fields
    deep = block // near
    spot = spot_ref[0]

    for slot in range(fields):
        source = pl.multiple_of(assignment_ref[slot] * block, block)
        row_ref[slot * block : (slot + 1) * block, :] = moved_ref[
            pl.ds(source, block), :
        ].astype(jnp.float32)
    for other in range(near):
        peer = jnp.bitwise_xor(spot, other)
        for row in range(deep):
            taken = row_ref[pl.ds(peer * deep + row, fields, stride=block), :]
            for column in range(beside):
                which, order = divmod(deep * column + row, share)
                left_ref[order, other, which * fields : (which + 1) * fields, :] = shift(
                    taken, -column * cycles
                ).astype(jnp.bfloat16)

    for order in range(share):
        for other in range(near):
            joined_ref[order % 2, other * cycles : (other + 1) * cycles, :] = value_refs[other][
                order
            ]
        left = jnp.concatenate(
            [left_ref[order, other][:, :cycles] for other in range(near)], axis=1
        )
        out_ref[2 * fields * order : 2 * fields * (order + 1), :] = jnp.dot(
            left, joined_ref[order % 2], preferred_element_type=jnp.float32
        ).astype(jnp.bfloat16)


def analyse(spot, assignment, moved, values):
    share, cycles, degrees = values[0].shape
    fields = assignment.shape[0]
    return pl.pallas_call(
        analysis_kernel,
        in_specs=[SCALARS] * 2 + [NEARBY] * (1 + len(values)),
        out_specs=NEARBY,
        scratch_shapes=[
            pltpu.VMEM(moved.shape, jnp.float32),
            pltpu.VMEM((share, len(values), 2 * fields, LANES), jnp.bfloat16),
            pltpu.VMEM((2, len(values) * cycles, degrees), jnp.bfloat16),
        ],
        out_shape=jax.ShapeDtypeStruct((share * 2 * fields, degrees), jnp.bfloat16),
        cost_estimate=pl.CostEstimate(
            flops=4 * fields * share * cycles * degrees * len(values),
            bytes_accessed=4 << 20,
            transcendentals=0,
        ),
        compiler_params=pltpu.CompilerParams(vmem_limit_bytes=ROOM),
        name="analysis",
    )(spot, assignment, moved, *values)


def synthesis_kernel(spot_ref, first_ref, *refs):
    near = NEAR_SIZE
    coefficient_ref, *value_refs = refs[: near + 1]
    out_ref, right_ref, row_ref, joined_ref = refs[near + 1 :]
    share, _, two_fields, _ = right_ref.shape
    fields = two_fields // 2
    cycles = value_refs[0].shape[1]
    beside = LANES // cycles
    lines = out_ref.shape[0]
    block = lines // fields
    deep = block // near
    dims = (((1,), (1,)), ((), ()))
    for order in range(share):
        factor = jnp.where(first_ref[0] + order == 0, 1.0, 2.0).astype(jnp.float32)
        for other in range(near):
            joined_ref[order % 2, other * cycles : (other + 1) * cycles, :] = value_refs[other][
                order
            ]
        product = factor * lax.dot_general(
            coefficient_ref[2 * fields * order : 2 * fields * (order + 1), :],
            joined_ref[order % 2],
            dims,
            preferred_element_type=jnp.float32,
        )
        for other in range(near):
            right_ref[order, other, :, :cycles] = product[
                :, other * cycles : (other + 1) * cycles
            ]
    for other in range(near):
        peer = jnp.bitwise_xor(spot_ref[0], other)
        for row in range(deep):
            pieces = []
            for column in range(beside):
                which, own = divmod(deep * column + row, share)
                pieces.append(right_ref[own, other, which * fields : (which + 1) * fields, :])
            row_ref[pl.ds(peer * deep + row, fields, stride=block), :] = side_by_side(
                pieces, cycles
            )
    out_ref[...] = row_ref[...].astype(jnp.bfloat16)


def synthesise(spot, first, coefficients, values, lines):
    share, cycles, degrees = values[0].shape
    fields = coefficients.shape[0] // (2 * share)
    return pl.pallas_call(
        synthesis_kernel,
        in_specs=[SCALARS] * 2 + [NEARBY] * (1 + len(values)),
        out_specs=NEARBY,
        scratch_shapes=[
            pltpu.VMEM((share, len(values), 2 * fields, LANES), jnp.float32),
            pltpu.VMEM((lines, LANES), jnp.float32),
            pltpu.VMEM((2, len(values) * cycles, degrees), jnp.bfloat16),
        ],
        out_shape=jax.ShapeDtypeStruct((lines, LANES), jnp.bfloat16),
        cost_estimate=pl.CostEstimate(
            flops=4 * fields * share * cycles * degrees * len(values),
            bytes_accessed=4 << 20,
            transcendentals=0,
        ),
        compiler_params=pltpu.CompilerParams(vmem_limit_bytes=ROOM),
        name="synthesis",
    )(spot, first, coefficients, *values)


def inverse_kernel(
    moved_ref,
    coarse_ref,
    fine_ref,
    turn_ref,
    out_ref,
    rows_ref,
    table_ref,
    row_ref,
    flip_ref,
    part_ref,
    sems,
):
    parts, cycles, span = part_ref.shape
    count = span // INNER
    orders = flip_ref.shape[1]
    inner_table(coarse_ref, fine_ref, table_ref, slice(None))
    row_ref[...] = moved_ref[...].astype(jnp.float32)
    peers = orders // SHARE
    deep = moved_ref.shape[0] // peers
    for row in range(deep):
        taken = row_ref[pl.ds(row, peers, stride=deep), :]
        for column in range(LANES // cycles):
            which, order = divmod(deep * column + row, SHARE)
            flip_ref[which, pl.ds(order, peers, stride=SHARE), :] = shift(
                taken, -column * cycles
            )
    first = jnp.transpose(flip_ref[0])[:cycles]
    second = jnp.transpose(flip_ref[1])[:cycles]
    dims = (((1,), (1,)), ((), ()))
    copies = []
    for part in range(parts):
        for step in range(count):
            rows = slice(step * cycles, (step + 1) * cycles)
            turn = part * count + step
            cosine, sine = turn_ref[0, turn : turn + 1, :], turn_ref[1, turn : turn + 1, :]
            rows_ref[part % 2, 0, rows, :] = (first * cosine - second * sine).astype(jnp.bfloat16)
            rows_ref[part % 2, 1, rows, :] = (first * sine + second * cosine).astype(jnp.bfloat16)
        result = lax.dot_general(
            rows_ref[part % 2, 0], table_ref[0], dims, preferred_element_type=jnp.float32
        ) + lax.dot_general(
            rows_ref[part % 2, 1], table_ref[1], dims, preferred_element_type=jnp.float32
        )
        for step in range(count):
            part_ref[part, :, step * INNER : (step + 1) * INNER] = result[
                step * cycles : (step + 1) * cycles
            ]
        copy = pltpu.make_async_copy(
            part_ref.at[part], out_ref.at[:, part * span : (part + 1) * span], sems.at[part]
        )
        copy.start()
        copies.append(copy)
    for copy in copies:
        copy.wait()


def inverse(moved, coarse, fine, turn, cycles, longitudes):
    orders = coarse.shape[2]
    count = 6
    parts = longitudes // INNER // count
    return pl.pallas_call(
        inverse_kernel,
        in_specs=[NEARBY] * 4,
        out_specs=pl.BlockSpec(memory_space=pltpu.HBM),
        out_shape=jax.ShapeDtypeStruct((cycles, longitudes), jnp.float32),
        scratch_shapes=[
            pltpu.VMEM((2, 2, count * cycles, orders), jnp.bfloat16),
            pltpu.VMEM((2, INNER, orders), jnp.bfloat16),
            pltpu.VMEM(moved.shape, jnp.float32),
            pltpu.VMEM((2, orders, LANES), jnp.float32),
            pltpu.VMEM((parts, cycles, count * INNER), jnp.float32),
            pltpu.SemaphoreType.DMA((parts,)),
        ],
        cost_estimate=pl.CostEstimate(
            flops=4 * cycles * longitudes * orders, bytes_accessed=1 << 20, transcendentals=0
        ),
        compiler_params=pltpu.CompilerParams(vmem_limit_bytes=ROOM),
        name="inverse_dft",
    )(moved, coarse, fine, turn)


def local(elevation, legendre, cycle_weight, love_factor, assignment):
    _, cycle_dev, longitudes = elevation.shape
    orders_dev, degrees = legendre.shape[1:]
    groups = lax.axis_size("cons")
    near = lax.axis_size(NEAR)
    far = lax.axis_size(FAR)
    orders = orders_dev * groups
    share = orders_dev // near
    spot = lax.axis_index(NEAR)
    coarse = jnp.asarray(angle_tables(FINE, FINE, longitudes, orders))
    fine = jnp.asarray(angle_tables(FINE, 1, longitudes, orders))
    turn = jnp.asarray(angle_tables(longitudes // INNER, INNER, longitudes, orders))

    by_order = legendre.transpose(1, 0, 2).reshape(near, share, cycle_dev, degrees)

    def chunk(other):
        return lax.dynamic_index_in_dim(by_order, spot ^ other, 0, keepdims=False)

    values = [chunk(0)] + [None] * (near - 1)
    for other in (*EARLY, *LATE):
        values[other] = lax.ppermute(
            chunk(other), NEAR, [(index, index ^ other) for index in range(near)]
        )

    deep = 2 * share // (LANES // cycle_dev)
    peers = groups * near
    lines = peers * deep

    def exchanged(packed):
        tiles = packed.reshape(peers, deep, LANES)
        tiles = lax.all_to_all(tiles, TEAM, 0, 0, tiled=True)
        return tiles.reshape(lines, LANES)

    packed = forward(elevation[0], cycle_weight[:, None], coarse, fine, turn, lines)
    moved = exchanged(packed)
    spot_row = spot[None].astype(jnp.int32)
    partial = analyse(spot_row, assignment, moved, values)
    rows = partial.shape[0] // far
    arrived = lax.all_to_all(partial.reshape(far, rows, degrees), FAR, 0, 0, tiled=True)
    analysis = jnp.sum(arrived.astype(jnp.float32), axis=0)
    scaled = (analysis * love_factor[None, :]).astype(jnp.bfloat16)
    copies = jnp.broadcast_to(scaled[None], (far, rows, degrees))
    coefficients = lax.all_to_all(copies, FAR, 0, 0, tiled=True).reshape(-1, degrees)
    first = ((lax.axis_index("cons") * near + spot) * share)[None].astype(jnp.int32)
    synthesis = synthesise(spot_row, first, coefficients, values, lines)
    returned = exchanged(synthesis)
    return inverse(returned, coarse, fine, turn, cycle_dev, longitudes)[None]


def solution(mesh):
    torus = Mesh(
        mesh.devices.reshape(mesh.shape["cons"], 2, 4, 2, 2), ("cons", *BLK)
    )
    placed = (P("cons", BLK, None), P(BLK, "cons", None), P(BLK), P(), P())
    return jax.shard_map(
        local, mesh=torus, in_specs=placed, out_specs=P("cons", BLK, None), check_vma=False
    )
```

```python
import jax
import jax.numpy as jnp
import numpy as np
from jax import lax
from jax.experimental import pallas as pl
from jax.experimental.pallas import tpu as pltpu
from jax.sharding import Mesh
from jax.sharding import PartitionSpec as P

BLK = ("blk_0", "blk_1", "blk_2")
NEAR = ("blk_0", "blk_2")
FAR = "blk_1"
TEAM = ("cons", *NEAR)
FINE = 16
INNER = FINE * FINE
LANES = 128
TILE = 8
NEAR_SIZE = 4
SHARE = 12
SWAPS = (2, 3, 1)
ROOM = 24 << 20
SCALARS = pl.BlockSpec(memory_space=pltpu.SMEM)
NEARBY = pl.BlockSpec(memory_space=pltpu.VMEM)


def angle_tables(steps, stride, period, orders):
    phases = (np.arange(steps)[:, None] * stride * np.arange(orders)[None, :]) % period
    angles = phases * (2.0 * np.pi / period)
    return np.stack([np.cos(angles), np.sin(angles)]).astype(np.float32)


def inner_table(coarse_ref, fine_ref, table_ref, lanes):
    fine_cos, fine_sin = fine_ref[0, :, lanes], fine_ref[1, :, lanes]
    for step in range(FINE):
        rows = slice(step * FINE, (step + 1) * FINE)
        coarse_cos = coarse_ref[0, step : step + 1, lanes]
        coarse_sin = coarse_ref[1, step : step + 1, lanes]
        cosine = coarse_cos * fine_cos - coarse_sin * fine_sin
        sine = coarse_sin * fine_cos + coarse_cos * fine_sin
        table_ref[0, rows, lanes] = cosine.astype(jnp.bfloat16)
        table_ref[1, rows, lanes] = (-sine).astype(jnp.bfloat16)


def shift(values, amount):
    amount %= LANES
    return values if amount == 0 else pltpu.roll(values, amount, values.ndim - 1)


def side_by_side(pieces, width):
    lane = lax.broadcasted_iota(jnp.int32, pieces[0].shape, pieces[0].ndim - 1)
    joined = jnp.zeros_like(pieces[0])
    for index, piece in reversed(list(enumerate(pieces))):
        joined = jnp.where(lane < (index + 1) * width, shift(piece, index * width), joined)
    return jnp.where(lane < len(pieces) * width, joined, 0.0)


def forward_kernel(
    elevation_ref,
    weight_ref,
    coarse_ref,
    fine_ref,
    turn_ref,
    out_ref,
    rows_ref,
    table_ref,
    flip_ref,
    pack_ref,
):
    cycles = elevation_ref.shape[0]
    turns = turn_ref.shape[1]
    orders = flip_ref.shape[1]
    for turn in range(turns):
        rows_ref[turn * cycles : (turn + 1) * cycles, :] = elevation_ref[
            :, turn * INNER : (turn + 1) * INNER
        ]
    weight = weight_ref[...]
    inner_table(coarse_ref, fine_ref, table_ref, slice(None))
    for part in range(orders // INNER):
        lanes = slice(part * INNER, (part + 1) * INNER)
        even = jnp.dot(rows_ref[...], table_ref[0, :, lanes], preferred_element_type=jnp.float32)
        odd = jnp.dot(rows_ref[...], table_ref[1, :, lanes], preferred_element_type=jnp.float32)
        first = second = None
        for turn in range(turns):
            rows = slice(turn * cycles, (turn + 1) * cycles)
            cosine, sine = turn_ref[0, turn : turn + 1, lanes], turn_ref[1, turn : turn + 1, lanes]
            one = even[rows] * cosine + odd[rows] * sine
            two = odd[rows] * cosine - even[rows] * sine
            first = one if first is None else first + one
            second = two if second is None else second + two
        flip_ref[0, lanes, :cycles] = jnp.transpose(first * weight)
        flip_ref[1, lanes, :cycles] = jnp.transpose(second * weight)

    beside = LANES // cycles
    peers = orders // SHARE
    deep = out_ref.shape[0] // peers
    for row in range(deep):
        pieces = []
        for column in range(beside):
            which, order = divmod(deep * column + row, SHARE)
            pieces.append(flip_ref[which, pl.ds(order, peers, stride=SHARE), :])
        pack_ref[pl.ds(row, peers, stride=deep), :] = side_by_side(pieces, cycles)
    out_ref[...] = pack_ref[...].astype(jnp.bfloat16)


def forward(elevation, weight, coarse, fine, turn, lines):
    cycles, longitudes = elevation.shape
    orders = coarse.shape[2]
    turns = longitudes // INNER
    return pl.pallas_call(
        forward_kernel,
        in_specs=[NEARBY] * 5,
        out_specs=NEARBY,
        out_shape=jax.ShapeDtypeStruct((lines, LANES), jnp.bfloat16),
        scratch_shapes=[
            pltpu.VMEM((turns * cycles, INNER), jnp.bfloat16),
            pltpu.VMEM((2, INNER, orders), jnp.bfloat16),
            pltpu.VMEM((2, orders, LANES), jnp.float32),
            pltpu.VMEM((lines, LANES), jnp.float32),
        ],
        cost_estimate=pl.CostEstimate(
            flops=4 * cycles * longitudes * orders, bytes_accessed=1 << 20, transcendentals=0
        ),
        compiler_params=pltpu.CompilerParams(vmem_limit_bytes=ROOM),
        name="forward_dft",
    )(elevation, weight, coarse, fine, turn)


def split_kernel(spot_ref, legendre_ref, same_ref, other_ref, stage_ref):
    flip_half, core = spot_ref[0], spot_ref[1]
    share = same_ref.shape[0]
    orders = stage_ref.shape[0]
    for first in range(0, orders, TILE):
        start = pl.multiple_of(flip_half * orders + first, TILE)
        stage_ref[first : first + TILE] = jnp.swapaxes(
            legendre_ref[:, pl.ds(start, TILE), :], 0, 1
        )
    same_ref[...] = stage_ref[pl.ds(core * share, share)]
    other_ref[...] = stage_ref[pl.ds((1 - core) * share, share)]


def split(spot, legendre):
    cycles, _, degrees = legendre.shape
    piece = jax.ShapeDtypeStruct((SHARE, cycles, degrees), legendre.dtype)
    return pl.pallas_call(
        split_kernel,
        in_specs=[SCALARS, NEARBY],
        out_specs=[NEARBY] * 2,
        out_shape=[piece] * 2,
        scratch_shapes=[pltpu.VMEM((2 * SHARE, cycles, degrees), legendre.dtype)],
        cost_estimate=pl.CostEstimate(
            flops=1 << 20, bytes_accessed=4 * cycles * SHARE * degrees * 2, transcendentals=0
        ),
        compiler_params=pltpu.CompilerParams(vmem_limit_bytes=ROOM),
        name="split",
    )(spot, legendre)


def analysis_kernel(spot_ref, *refs):
    near = NEAR_SIZE
    assignment_ref, moved_ref, *value_refs = refs[: near + 2]
    out_ref, row_ref, left_ref, joined_ref = refs[near + 2 :]
    share, _, two_fields, _ = left_ref.shape
    fields = two_fields // 2
    cycles = value_refs[0].shape[1]
    beside = LANES // cycles
    lines = moved_ref.shape[0]
    block = lines // fields
    deep = block // near
    spot = spot_ref[0]

    for slot in range(fields):
        source = pl.multiple_of(assignment_ref[slot] * block, block)
        row_ref[slot * block : (slot + 1) * block, :] = moved_ref[
            pl.ds(source, block), :
        ].astype(jnp.float32)
    for other in range(near):
        peer = jnp.bitwise_xor(spot, other)
        for row in range(deep):
            taken = row_ref[pl.ds(peer * deep + row, fields, stride=block), :]
            for column in range(beside):
                which, order = divmod(deep * column + row, share)
                left_ref[order, other, which * fields : (which + 1) * fields, :] = shift(
                    taken, -column * cycles
                ).astype(jnp.bfloat16)

    for order in range(share):
        for other in range(near):
            joined_ref[order % 2, other * cycles : (other + 1) * cycles, :] = value_refs[other][
                order
            ]
        left = jnp.concatenate(
            [left_ref[order, other][:, :cycles] for other in range(near)], axis=1
        )
        out_ref[2 * fields * order : 2 * fields * (order + 1), :] = jnp.dot(
            left, joined_ref[order % 2], preferred_element_type=jnp.float32
        ).astype(jnp.bfloat16)


def analyse(spot, assignment, moved, values):
    share, cycles, degrees = values[0].shape
    fields = assignment.shape[0]
    return pl.pallas_call(
        analysis_kernel,
        in_specs=[SCALARS] * 2 + [NEARBY] * (1 + len(values)),
        out_specs=NEARBY,
        scratch_shapes=[
            pltpu.VMEM(moved.shape, jnp.float32),
            pltpu.VMEM((share, len(values), 2 * fields, LANES), jnp.bfloat16),
            pltpu.VMEM((2, len(values) * cycles, degrees), jnp.bfloat16),
        ],
        out_shape=jax.ShapeDtypeStruct((share * 2 * fields, degrees), jnp.bfloat16),
        cost_estimate=pl.CostEstimate(
            flops=4 * fields * share * cycles * degrees * len(values),
            bytes_accessed=4 << 20,
            transcendentals=0,
        ),
        compiler_params=pltpu.CompilerParams(vmem_limit_bytes=ROOM),
        name="analysis",
    )(spot, assignment, moved, *values)


def synthesis_kernel(spot_ref, first_ref, *refs):
    near = NEAR_SIZE
    coefficient_ref, *value_refs = refs[: near + 1]
    out_ref, right_ref, row_ref, joined_ref = refs[near + 1 :]
    share, _, two_fields, _ = right_ref.shape
    fields = two_fields // 2
    cycles = value_refs[0].shape[1]
    beside = LANES // cycles
    lines = out_ref.shape[0]
    block = lines // fields
    deep = block // near
    dims = (((1,), (1,)), ((), ()))
    for order in range(share):
        factor = jnp.where(first_ref[0] + order == 0, 1.0, 2.0).astype(jnp.float32)
        for other in range(near):
            joined_ref[order % 2, other * cycles : (other + 1) * cycles, :] = value_refs[other][
                order
            ]
        product = factor * lax.dot_general(
            coefficient_ref[2 * fields * order : 2 * fields * (order + 1), :],
            joined_ref[order % 2],
            dims,
            preferred_element_type=jnp.float32,
        )
        for other in range(near):
            right_ref[order, other, :, :cycles] = product[
                :, other * cycles : (other + 1) * cycles
            ]
    for other in range(near):
        peer = jnp.bitwise_xor(spot_ref[0], other)
        for row in range(deep):
            pieces = []
            for column in range(beside):
                which, own = divmod(deep * column + row, share)
                pieces.append(right_ref[own, other, which * fields : (which + 1) * fields, :])
            row_ref[pl.ds(peer * deep + row, fields, stride=block), :] = side_by_side(
                pieces, cycles
            )
    out_ref[...] = row_ref[...].astype(jnp.bfloat16)


def synthesise(spot, first, coefficients, values, lines):
    share, cycles, degrees = values[0].shape
    fields = coefficients.shape[0] // (2 * share)
    return pl.pallas_call(
        synthesis_kernel,
        in_specs=[SCALARS] * 2 + [NEARBY] * (1 + len(values)),
        out_specs=NEARBY,
        scratch_shapes=[
            pltpu.VMEM((share, len(values), 2 * fields, LANES), jnp.float32),
            pltpu.VMEM((lines, LANES), jnp.float32),
            pltpu.VMEM((2, len(values) * cycles, degrees), jnp.bfloat16),
        ],
        out_shape=jax.ShapeDtypeStruct((lines, LANES), jnp.bfloat16),
        cost_estimate=pl.CostEstimate(
            flops=4 * fields * share * cycles * degrees * len(values),
            bytes_accessed=4 << 20,
            transcendentals=0,
        ),
        compiler_params=pltpu.CompilerParams(vmem_limit_bytes=ROOM),
        name="synthesis",
    )(spot, first, coefficients, *values)


def inverse_kernel(
    moved_ref,
    coarse_ref,
    fine_ref,
    turn_ref,
    out_ref,
    rows_ref,
    table_ref,
    row_ref,
    flip_ref,
    part_ref,
    sems,
):
    parts, cycles, span = part_ref.shape
    count = span // INNER
    orders = flip_ref.shape[1]
    inner_table(coarse_ref, fine_ref, table_ref, slice(None))
    row_ref[...] = moved_ref[...].astype(jnp.float32)
    peers = orders // SHARE
    deep = moved_ref.shape[0] // peers
    for row in range(deep):
        taken = row_ref[pl.ds(row, peers, stride=deep), :]
        for column in range(LANES // cycles):
            which, order = divmod(deep * column + row, SHARE)
            flip_ref[which, pl.ds(order, peers, stride=SHARE), :] = shift(
                taken, -column * cycles
            )
    first = jnp.transpose(flip_ref[0])[:cycles]
    second = jnp.transpose(flip_ref[1])[:cycles]
    dims = (((1,), (1,)), ((), ()))
    copies = []
    for part in range(parts):
        for step in range(count):
            rows = slice(step * cycles, (step + 1) * cycles)
            turn = part * count + step
            cosine, sine = turn_ref[0, turn : turn + 1, :], turn_ref[1, turn : turn + 1, :]
            rows_ref[part % 2, 0, rows, :] = (first * cosine - second * sine).astype(jnp.bfloat16)
            rows_ref[part % 2, 1, rows, :] = (first * sine + second * cosine).astype(jnp.bfloat16)
        result = lax.dot_general(
            rows_ref[part % 2, 0], table_ref[0], dims, preferred_element_type=jnp.float32
        ) + lax.dot_general(
            rows_ref[part % 2, 1], table_ref[1], dims, preferred_element_type=jnp.float32
        )
        for step in range(count):
            part_ref[part, :, step * INNER : (step + 1) * INNER] = result[
                step * cycles : (step + 1) * cycles
            ]
        copy = pltpu.make_async_copy(
            part_ref.at[part], out_ref.at[:, part * span : (part + 1) * span], sems.at[part]
        )
        copy.start()
        copies.append(copy)
    for copy in copies:
        copy.wait()


def inverse(moved, coarse, fine, turn, cycles, longitudes):
    orders = coarse.shape[2]
    count = 6
    parts = longitudes // INNER // count
    return pl.pallas_call(
        inverse_kernel,
        in_specs=[NEARBY] * 4,
        out_specs=pl.BlockSpec(memory_space=pltpu.HBM),
        out_shape=jax.ShapeDtypeStruct((cycles, longitudes), jnp.float32),
        scratch_shapes=[
            pltpu.VMEM((2, 2, count * cycles, orders), jnp.bfloat16),
            pltpu.VMEM((2, INNER, orders), jnp.bfloat16),
            pltpu.VMEM(moved.shape, jnp.float32),
            pltpu.VMEM((2, orders, LANES), jnp.float32),
            pltpu.VMEM((parts, cycles, count * INNER), jnp.float32),
            pltpu.SemaphoreType.DMA((parts,)),
        ],
        cost_estimate=pl.CostEstimate(
            flops=4 * cycles * longitudes * orders, bytes_accessed=1 << 20, transcendentals=0
        ),
        compiler_params=pltpu.CompilerParams(vmem_limit_bytes=ROOM),
        name="inverse_dft",
    )(moved, coarse, fine, turn)


def local(elevation, legendre, cycle_weight, love_factor, assignment):
    _, cycle_dev, longitudes = elevation.shape
    orders_dev, degrees = legendre.shape[1:]
    groups = lax.axis_size("cons")
    near = lax.axis_size(NEAR)
    far = lax.axis_size(FAR)
    orders = orders_dev * groups
    share = orders_dev // near
    spot = lax.axis_index(NEAR)
    coarse = jnp.asarray(angle_tables(FINE, FINE, longitudes, orders))
    fine = jnp.asarray(angle_tables(FINE, 1, longitudes, orders))
    turn = jnp.asarray(angle_tables(longitudes // INNER, INNER, longitudes, orders))

    far_half, core = lax.axis_index("blk_0"), lax.axis_index("blk_2")
    values = [None] * near
    for flip in (1, 0):
        place = jnp.stack([far_half ^ flip, core]).astype(jnp.int32)
        values[2 * flip], values[2 * flip + 1] = split(place, legendre)
    for other in SWAPS:
        values[other] = lax.ppermute(
            values[other], NEAR, [(index, index ^ other) for index in range(near)]
        )

    deep = 2 * share // (LANES // cycle_dev)
    peers = groups * near
    lines = peers * deep

    def exchanged(packed):
        tiles = packed.reshape(peers, deep, LANES)
        tiles = lax.all_to_all(tiles, TEAM, 0, 0, tiled=True)
        return tiles.reshape(lines, LANES)

    packed = forward(elevation[0], cycle_weight[:, None], coarse, fine, turn, lines)
    moved = exchanged(packed)
    spot_row = spot[None].astype(jnp.int32)
    partial = analyse(spot_row, assignment, moved, values)
    rows = partial.shape[0] // far
    arrived = lax.all_to_all(partial.reshape(far, rows, degrees), FAR, 0, 0, tiled=True)
    analysis = jnp.sum(arrived.astype(jnp.float32), axis=0)
    scaled = (analysis * love_factor[None, :]).astype(jnp.bfloat16)
    copies = jnp.broadcast_to(scaled[None], (far, rows, degrees))
    coefficients = lax.all_to_all(copies, FAR, 0, 0, tiled=True).reshape(-1, degrees)
    first = ((lax.axis_index("cons") * near + spot) * share)[None].astype(jnp.int32)
    synthesis = synthesise(spot_row, first, coefficients, values, lines)
    returned = exchanged(synthesis)
    return inverse(returned, coarse, fine, turn, cycle_dev, longitudes)[None]


def solution(mesh):
    torus = Mesh(
        mesh.devices.reshape(mesh.shape["cons"], 2, 8, 2), ("cons", *BLK)
    )
    placed = (P("cons", BLK, None), P(BLK, "cons", None), P(BLK), P(), P())
    return jax.shard_map(
        local, mesh=torus, in_specs=placed, out_specs=P("cons", BLK, None), check_vma=False
    )
```

```python
import functools
import math

import jax
import jax.numpy as jnp
import numpy as np
from jax import lax
from jax.experimental import pallas as pl
from jax.experimental.pallas import tpu as pltpu
from jax.sharding import Mesh
from jax.sharding import PartitionSpec as P

BLK = ("blk_0", "blk_1", "blk_2")
NEAR = ("blk_2", "blk_0")
CORE = "blk_2"
DEEP = "blk_1"
FAR = ("blk_0", "blk_1")
FINE = 16
INNER = FINE * FINE
LANES = 128
TILE = 8
ROOM = 24 << 20
SCALARS = pl.BlockSpec(memory_space=pltpu.SMEM)
NEARBY = pl.BlockSpec(memory_space=pltpu.VMEM)


def angle_tables(steps, stride, period, orders):
    phases = (np.arange(steps)[:, None] * stride * np.arange(orders)[None, :]) % period
    angles = phases * (2.0 * np.pi / period)
    return np.stack([np.cos(angles), np.sin(angles)]).astype(np.float32)


def inner_table(coarse_ref, fine_ref, table_ref, lanes):
    fine_cos, fine_sin = fine_ref[0, :, lanes], fine_ref[1, :, lanes]
    for step in range(FINE):
        rows = slice(step * FINE, (step + 1) * FINE)
        coarse_cos = coarse_ref[0, step : step + 1, lanes]
        coarse_sin = coarse_ref[1, step : step + 1, lanes]
        cosine = coarse_cos * fine_cos - coarse_sin * fine_sin
        sine = coarse_sin * fine_cos + coarse_cos * fine_sin
        table_ref[0, rows, lanes] = cosine.astype(jnp.bfloat16)
        table_ref[1, rows, lanes] = (-sine).astype(jnp.bfloat16)


def shift(values, amount):
    amount %= LANES
    return values if amount == 0 else pltpu.roll(values, amount, values.ndim - 1)


def side_by_side(pieces, width):
    lane = lax.broadcasted_iota(jnp.int32, pieces[0].shape, pieces[0].ndim - 1)
    joined = jnp.zeros_like(pieces[0])
    for index, piece in reversed(list(enumerate(pieces))):
        joined = jnp.where(lane < (index + 1) * width, shift(piece, index * width), joined)
    return jnp.where(lane < len(pieces) * width, joined, 0.0)


def forward_kernel(
    peers,
    elevation_ref,
    weight_ref,
    coarse_ref,
    fine_ref,
    turn_ref,
    out_ref,
    rows_ref,
    table_ref,
    flip_ref,
    pack_ref,
):
    cycles = elevation_ref.shape[0]
    turns = turn_ref.shape[1]
    orders = flip_ref.shape[1]
    for turn in range(turns):
        rows_ref[turn * cycles : (turn + 1) * cycles, :] = elevation_ref[
            :, turn * INNER : (turn + 1) * INNER
        ]
    weight = weight_ref[...]
    inner_table(coarse_ref, fine_ref, table_ref, slice(None))
    for part in range(orders // INNER):
        lanes = slice(part * INNER, (part + 1) * INNER)
        even = jnp.dot(rows_ref[...], table_ref[0, :, lanes], preferred_element_type=jnp.float32)
        odd = jnp.dot(rows_ref[...], table_ref[1, :, lanes], preferred_element_type=jnp.float32)
        first = second = None
        for turn in range(turns):
            rows = slice(turn * cycles, (turn + 1) * cycles)
            cosine, sine = turn_ref[0, turn : turn + 1, lanes], turn_ref[1, turn : turn + 1, lanes]
            one = even[rows] * cosine + odd[rows] * sine
            two = odd[rows] * cosine - even[rows] * sine
            first = one if first is None else first + one
            second = two if second is None else second + two
        flip_ref[0, lanes, :cycles] = jnp.transpose(first * weight)
        flip_ref[1, lanes, :cycles] = jnp.transpose(second * weight)

    beside = LANES // cycles
    deep = out_ref.shape[0] // peers
    share = orders // peers
    for row in range(deep):
        pieces = []
        for column in range(beside):
            which, order = divmod(deep * column + row, share)
            pieces.append(flip_ref[which, pl.ds(order, peers, stride=share), :])
        pack_ref[pl.ds(row, peers, stride=deep), :] = side_by_side(pieces, cycles)
    out_ref[...] = pack_ref[...].astype(jnp.bfloat16)


def forward(elevation, weight, coarse, fine, turn, lines, peers):
    cycles, longitudes = elevation.shape
    orders = coarse.shape[2]
    turns = longitudes // INNER
    return pl.pallas_call(
        functools.partial(forward_kernel, peers),
        in_specs=[NEARBY] * 5,
        out_specs=NEARBY,
        out_shape=jax.ShapeDtypeStruct((lines, LANES), jnp.bfloat16),
        scratch_shapes=[
            pltpu.VMEM((turns * cycles, INNER), jnp.bfloat16),
            pltpu.VMEM((2, INNER, orders), jnp.bfloat16),
            pltpu.VMEM((2, orders, LANES), jnp.float32),
            pltpu.VMEM((lines, LANES), jnp.float32),
        ],
        cost_estimate=pl.CostEstimate(
            flops=4 * cycles * longitudes * orders, bytes_accessed=1 << 20, transcendentals=0
        ),
        compiler_params=pltpu.CompilerParams(vmem_limit_bytes=ROOM),
        name="forward_dft",
    )(elevation, weight, coarse, fine, turn)


def split_kernel(place_ref, legendre_ref, half_ref):
    orders = half_ref.shape[0]
    for first in range(0, orders, TILE):
        start = pl.multiple_of(place_ref[0] * orders + first, TILE)
        half_ref[first : first + TILE] = jnp.swapaxes(
            legendre_ref[:, pl.ds(start, TILE), :], 0, 1
        )


def part_kernel(place_ref, half_ref, part_ref):
    share = part_ref.shape[0]
    part_ref[...] = half_ref[pl.ds(place_ref[0] * share, share)]


def halved(kernel, place, values, shape):
    return pl.pallas_call(
        kernel,
        in_specs=[SCALARS, NEARBY],
        out_specs=NEARBY,
        out_shape=jax.ShapeDtypeStruct(shape, values.dtype),
        cost_estimate=pl.CostEstimate(
            flops=1 << 20, bytes_accessed=4 * math.prod(shape), transcendentals=0
        ),
        compiler_params=pltpu.CompilerParams(vmem_limit_bytes=ROOM),
    )(place[None].astype(jnp.int32), values)


def analysis_kernel(near, spot_ref, *refs):
    assignment_ref, moved_ref, *value_refs = refs[: near + 2]
    out_ref, row_ref, left_ref, joined_ref = refs[near + 2 :]
    share, _, two_fields, _ = left_ref.shape
    fields = two_fields // 2
    cycles = value_refs[0].shape[1]
    beside = LANES // cycles
    lines = moved_ref.shape[0]
    block = lines // fields
    deep = block // near
    spot = spot_ref[0]

    for slot in range(fields):
        source = pl.multiple_of(assignment_ref[slot] * block, block)
        row_ref[slot * block : (slot + 1) * block, :] = moved_ref[
            pl.ds(source, block), :
        ].astype(jnp.float32)
    for other in range(near):
        peer = jnp.bitwise_xor(spot, other)
        for row in range(deep):
            taken = row_ref[pl.ds(peer * deep + row, fields, stride=block), :]
            for column in range(beside):
                which, order = divmod(deep * column + row, share)
                left_ref[order, other, which * fields : (which + 1) * fields, :] = shift(
                    taken, -column * cycles
                ).astype(jnp.bfloat16)

    for order in range(share):
        for other in range(near):
            joined_ref[order % 2, other * cycles : (other + 1) * cycles, :] = value_refs[other][
                order
            ]
        left = jnp.concatenate(
            [left_ref[order, other][:, :cycles] for other in range(near)], axis=1
        )
        out_ref[2 * fields * order : 2 * fields * (order + 1), :] = jnp.dot(
            left, joined_ref[order % 2], preferred_element_type=jnp.float32
        ).astype(jnp.bfloat16)


def analyse(spot, assignment, moved, values):
    share, cycles, degrees = values[0].shape
    fields = assignment.shape[0]
    return pl.pallas_call(
        functools.partial(analysis_kernel, len(values)),
        in_specs=[SCALARS] * 2 + [NEARBY] * (1 + len(values)),
        out_specs=NEARBY,
        scratch_shapes=[
            pltpu.VMEM(moved.shape, jnp.float32),
            pltpu.VMEM((share, len(values), 2 * fields, LANES), jnp.bfloat16),
            pltpu.VMEM((2, len(values) * cycles, degrees), jnp.bfloat16),
        ],
        out_shape=jax.ShapeDtypeStruct((share * 2 * fields, degrees), jnp.bfloat16),
        cost_estimate=pl.CostEstimate(
            flops=4 * fields * share * cycles * degrees * len(values),
            bytes_accessed=4 << 20,
            transcendentals=0,
        ),
        compiler_params=pltpu.CompilerParams(vmem_limit_bytes=ROOM),
        name="analysis",
    )(spot, assignment, moved, *values)


def synthesis_kernel(near, spot_ref, first_ref, *refs):
    coefficient_ref, *value_refs = refs[: near + 1]
    out_ref, right_ref, row_ref, joined_ref = refs[near + 1 :]
    share, _, two_fields, _ = right_ref.shape
    fields = two_fields // 2
    cycles = value_refs[0].shape[1]
    beside = LANES // cycles
    lines = out_ref.shape[0]
    block = lines // fields
    deep = block // near
    dims = (((1,), (1,)), ((), ()))
    for order in range(share):
        factor = jnp.where(first_ref[0] + order == 0, 1.0, 2.0).astype(jnp.float32)
        for other in range(near):
            skip = 0 if value_refs[other].shape[0] == share else share * (spot_ref[0] % 2)
            joined_ref[order % 2, other * cycles : (other + 1) * cycles, :] = value_refs[other][
                skip + order
            ]
        product = factor * lax.dot_general(
            coefficient_ref[2 * fields * order : 2 * fields * (order + 1), :],
            joined_ref[order % 2],
            dims,
            preferred_element_type=jnp.float32,
        )
        for other in range(near):
            right_ref[order, other, :, :cycles] = product[
                :, other * cycles : (other + 1) * cycles
            ]
    for other in range(near):
        peer = jnp.bitwise_xor(spot_ref[0], other)
        for row in range(deep):
            pieces = []
            for column in range(beside):
                which, own = divmod(deep * column + row, share)
                pieces.append(right_ref[own, other, which * fields : (which + 1) * fields, :])
            row_ref[pl.ds(peer * deep + row, fields, stride=block), :] = side_by_side(
                pieces, cycles
            )
    out_ref[...] = row_ref[...].astype(jnp.bfloat16)


def synthesise(spot, first, coefficients, values, lines):
    share = min(value.shape[0] for value in values)
    _, cycles, degrees = values[0].shape
    fields = coefficients.shape[0] // (2 * share)
    return pl.pallas_call(
        functools.partial(synthesis_kernel, len(values)),
        in_specs=[SCALARS] * 2 + [NEARBY] * (1 + len(values)),
        out_specs=NEARBY,
        scratch_shapes=[
            pltpu.VMEM((share, len(values), 2 * fields, LANES), jnp.float32),
            pltpu.VMEM((lines, LANES), jnp.float32),
            pltpu.VMEM((2, len(values) * cycles, degrees), jnp.bfloat16),
        ],
        out_shape=jax.ShapeDtypeStruct((lines, LANES), jnp.bfloat16),
        cost_estimate=pl.CostEstimate(
            flops=4 * fields * share * cycles * degrees * len(values),
            bytes_accessed=4 << 20,
            transcendentals=0,
        ),
        compiler_params=pltpu.CompilerParams(vmem_limit_bytes=ROOM),
        name="synthesis",
    )(spot, first, coefficients, *values)


def inverse_kernel(
    peers,
    moved_ref,
    coarse_ref,
    fine_ref,
    turn_ref,
    out_ref,
    rows_ref,
    table_ref,
    row_ref,
    flip_ref,
    part_ref,
    sems,
):
    parts, cycles, span = part_ref.shape
    count = span // INNER
    orders = flip_ref.shape[1]
    inner_table(coarse_ref, fine_ref, table_ref, slice(None))
    row_ref[...] = moved_ref[...].astype(jnp.float32)
    deep = moved_ref.shape[0] // peers
    share = orders // peers
    for row in range(deep):
        taken = row_ref[pl.ds(row, peers, stride=deep), :]
        for column in range(LANES // cycles):
            which, order = divmod(deep * column + row, share)
            flip_ref[which, pl.ds(order, peers, stride=share), :] = shift(
                taken, -column * cycles
            )
    first = jnp.transpose(flip_ref[0])[:cycles]
    second = jnp.transpose(flip_ref[1])[:cycles]
    dims = (((1,), (1,)), ((), ()))
    copies = []
    for part in range(parts):
        for step in range(count):
            rows = slice(step * cycles, (step + 1) * cycles)
            turn = part * count + step
            cosine, sine = turn_ref[0, turn : turn + 1, :], turn_ref[1, turn : turn + 1, :]
            rows_ref[part % 2, 0, rows, :] = (first * cosine - second * sine).astype(jnp.bfloat16)
            rows_ref[part % 2, 1, rows, :] = (first * sine + second * cosine).astype(jnp.bfloat16)
        result = lax.dot_general(
            rows_ref[part % 2, 0], table_ref[0], dims, preferred_element_type=jnp.float32
        ) + lax.dot_general(
            rows_ref[part % 2, 1], table_ref[1], dims, preferred_element_type=jnp.float32
        )
        for step in range(count):
            part_ref[part, :, step * INNER : (step + 1) * INNER] = result[
                step * cycles : (step + 1) * cycles
            ]
        copy = pltpu.make_async_copy(
            part_ref.at[part], out_ref.at[:, part * span : (part + 1) * span], sems.at[part]
        )
        copy.start()
        copies.append(copy)
    for copy in copies:
        copy.wait()


def inverse(moved, coarse, fine, turn, cycles, longitudes, peers):
    orders = coarse.shape[2]
    count = 6
    parts = longitudes // INNER // count
    return pl.pallas_call(
        functools.partial(inverse_kernel, peers),
        in_specs=[NEARBY] * 4,
        out_specs=pl.BlockSpec(memory_space=pltpu.HBM),
        out_shape=jax.ShapeDtypeStruct((cycles, longitudes), jnp.float32),
        scratch_shapes=[
            pltpu.VMEM((2, 2, count * cycles, orders), jnp.bfloat16),
            pltpu.VMEM((2, INNER, orders), jnp.bfloat16),
            pltpu.VMEM(moved.shape, jnp.float32),
            pltpu.VMEM((2, orders, LANES), jnp.float32),
            pltpu.VMEM((parts, cycles, count * INNER), jnp.float32),
            pltpu.SemaphoreType.DMA((parts,)),
        ],
        cost_estimate=pl.CostEstimate(
            flops=4 * cycles * longitudes * orders, bytes_accessed=1 << 20, transcendentals=0
        ),
        compiler_params=pltpu.CompilerParams(vmem_limit_bytes=ROOM),
        name="inverse_dft",
    )(moved, coarse, fine, turn)


def local(elevation, legendre, cycle_weight, love_factor, assignment):
    _, cycle_dev, longitudes = elevation.shape
    orders_dev, degrees = legendre.shape[1:]
    groups = lax.axis_size("cons")
    cores, near = lax.axis_size(CORE), lax.axis_size(NEAR)
    deep, far = lax.axis_size(DEEP), lax.axis_size(FAR)
    orders = orders_dev * groups
    spot, core = lax.axis_index(NEAR), lax.axis_index(CORE)
    side = lax.axis_index("blk_0")
    coarse = jnp.asarray(angle_tables(FINE, FINE, longitudes, orders))
    fine = jnp.asarray(angle_tables(FINE, 1, longitudes, orders))
    turn = jnp.asarray(angle_tables(longitudes // INNER, INNER, longitudes, orders))

    def swapped(values, other):
        pairs = [(index, index ^ other) for index in range(near)]
        return lax.ppermute(values, NEAR[::-1], pairs)

    half, share = orders_dev // cores, orders_dev // near

    def placed(which):
        shape = (half, cycle_dev, degrees)
        return halved(split_kernel, which, legendre, shape)

    def part_of(values):
        shape = (share, cycle_dev, degrees)
        return halved(part_kernel, 1 - side, values, shape)

    def exchanged(packed, axes):
        peers = lax.axis_size(axes)
        tiles = packed.reshape(peers, -1, LANES)
        tiles = lax.all_to_all(tiles, axes, 0, 0, tiled=True)
        return tiles.reshape(-1, LANES)

    sent = placed(1 - core)
    met = swapped(sent, 1)
    own = placed(core)
    lines = groups * orders_dev * 2 // (LANES // cycle_dev)
    packed = forward(elevation[0], cycle_weight[:, None], coarse, fine, turn, lines, groups * cores)
    moved = exchanged(packed, ("cons", CORE))
    partial = analyse(core[None].astype(jnp.int32), assignment, moved, [own, met])
    rows = partial.shape[0] // far
    arrived = lax.all_to_all(partial.reshape(far, rows, degrees), FAR, 0, 0, tiled=True)
    own_side = swapped(part_of(own), 2)
    analysis = jnp.sum(arrived.astype(jnp.float32), axis=0)
    scaled = (analysis * love_factor[None, :]).astype(jnp.bfloat16)
    copies = jnp.broadcast_to(scaled[None], (deep, rows, degrees))
    coefficients = lax.all_to_all(copies, DEEP, 0, 0, tiled=True)
    met_side = swapped(part_of(sent), 3)
    first = ((lax.axis_index("cons") * near + spot) * share)[None].astype(jnp.int32)
    synthesis = synthesise(
        spot[None].astype(jnp.int32),
        first,
        coefficients.reshape(-1, degrees),
        [own, own_side, met, met_side],
        lines,
    )
    returned = exchanged(synthesis, ("cons", *NEAR))
    return inverse(
        returned, coarse, fine, turn, cycle_dev, longitudes, groups * near
    )[None]


def solution(mesh):
    torus = Mesh(
        mesh.devices.reshape(mesh.shape["cons"], 2, 8, 2), ("cons", *BLK)
    )
    placed = (P("cons", BLK, None), P(BLK, "cons", None), P(BLK), P(), P())
    return jax.shard_map(
        local, mesh=torus, in_specs=placed, out_specs=P("cons", BLK, None), check_vma=False
    )
```

```python
import functools
import math

import jax
import jax.numpy as jnp
import numpy as np
from jax import lax
from jax.experimental import pallas as pl
from jax.experimental.pallas import tpu as pltpu
from jax.sharding import Mesh
from jax.sharding import PartitionSpec as P

BLK = ("blk_0", "blk_1", "blk_2")
NEAR = ("blk_2", "blk_0")
CORE = "blk_2"
DEEP = "blk_1"
FAR = ("blk_0", "blk_1")
FINE = 16
INNER = FINE * FINE
LANES = 128
TILE = 8
ROOM = 24 << 20
SCALARS = pl.BlockSpec(memory_space=pltpu.SMEM)
NEARBY = pl.BlockSpec(memory_space=pltpu.VMEM)


def angle_tables(steps, stride, period, orders):
    phases = (np.arange(steps)[:, None] * stride * np.arange(orders)[None, :]) % period
    angles = phases * (2.0 * np.pi / period)
    return np.stack([np.cos(angles), np.sin(angles)]).astype(np.float32)


def inner_table(coarse_ref, fine_ref, table_ref, lanes):
    fine_cos, fine_sin = fine_ref[0, :, lanes], fine_ref[1, :, lanes]
    for step in range(FINE):
        rows = slice(step * FINE, (step + 1) * FINE)
        coarse_cos = coarse_ref[0, step : step + 1, lanes]
        coarse_sin = coarse_ref[1, step : step + 1, lanes]
        cosine = coarse_cos * fine_cos - coarse_sin * fine_sin
        sine = coarse_sin * fine_cos + coarse_cos * fine_sin
        table_ref[0, rows, lanes] = cosine.astype(jnp.bfloat16)
        table_ref[1, rows, lanes] = (-sine).astype(jnp.bfloat16)


def shift(values, amount):
    amount %= LANES
    return values if amount == 0 else pltpu.roll(values, amount, values.ndim - 1)


def side_by_side(pieces, width):
    lane = lax.broadcasted_iota(jnp.int32, pieces[0].shape, pieces[0].ndim - 1)
    joined = jnp.zeros_like(pieces[0])
    for index, piece in reversed(list(enumerate(pieces))):
        joined = jnp.where(lane < (index + 1) * width, shift(piece, index * width), joined)
    return jnp.where(lane < len(pieces) * width, joined, 0.0)


def forward_kernel(
    peers,
    elevation_ref,
    weight_ref,
    coarse_ref,
    fine_ref,
    turn_ref,
    out_ref,
    rows_ref,
    table_ref,
    flip_ref,
    pack_ref,
):
    cycles = elevation_ref.shape[0]
    turns = turn_ref.shape[1]
    orders = flip_ref.shape[1]
    for turn in range(turns):
        rows_ref[turn * cycles : (turn + 1) * cycles, :] = elevation_ref[
            :, turn * INNER : (turn + 1) * INNER
        ]
    weight = weight_ref[...]
    inner_table(coarse_ref, fine_ref, table_ref, slice(None))
    for part in range(orders // INNER):
        lanes = slice(part * INNER, (part + 1) * INNER)
        even = jnp.dot(rows_ref[...], table_ref[0, :, lanes], preferred_element_type=jnp.float32)
        odd = jnp.dot(rows_ref[...], table_ref[1, :, lanes], preferred_element_type=jnp.float32)
        first = second = None
        for turn in range(turns):
            rows = slice(turn * cycles, (turn + 1) * cycles)
            cosine, sine = turn_ref[0, turn : turn + 1, lanes], turn_ref[1, turn : turn + 1, lanes]
            one = even[rows] * cosine + odd[rows] * sine
            two = odd[rows] * cosine - even[rows] * sine
            first = one if first is None else first + one
            second = two if second is None else second + two
        flip_ref[0, lanes, :cycles] = jnp.transpose(first * weight)
        flip_ref[1, lanes, :cycles] = jnp.transpose(second * weight)

    beside = LANES // cycles
    deep = out_ref.shape[0] // peers
    share = orders // peers
    for row in range(deep):
        pieces = []
        for column in range(beside):
            which, order = divmod(deep * column + row, share)
            pieces.append(flip_ref[which, pl.ds(order, peers, stride=share), :])
        pack_ref[pl.ds(row, peers, stride=deep), :] = side_by_side(pieces, cycles)
    out_ref[...] = pack_ref[...].astype(jnp.bfloat16)


def forward(elevation, weight, coarse, fine, turn, lines, peers):
    cycles, longitudes = elevation.shape
    orders = coarse.shape[2]
    turns = longitudes // INNER
    return pl.pallas_call(
        functools.partial(forward_kernel, peers),
        in_specs=[NEARBY] * 5,
        out_specs=NEARBY,
        out_shape=jax.ShapeDtypeStruct((lines, LANES), jnp.bfloat16),
        scratch_shapes=[
            pltpu.VMEM((turns * cycles, INNER), jnp.bfloat16),
            pltpu.VMEM((2, INNER, orders), jnp.bfloat16),
            pltpu.VMEM((2, orders, LANES), jnp.float32),
            pltpu.VMEM((lines, LANES), jnp.float32),
        ],
        cost_estimate=pl.CostEstimate(
            flops=4 * cycles * longitudes * orders, bytes_accessed=1 << 20, transcendentals=0
        ),
        name="forward_dft",
    )(elevation, weight, coarse, fine, turn)


def split_kernel(place_ref, legendre_ref, sent_ref, own_ref, part_ref):
    core, side = place_ref[0], place_ref[1]
    orders, share = own_ref.shape[0], part_ref.shape[0]
    for target, index in ((sent_ref, 1 - core), (own_ref, core)):
        for first in range(0, orders, TILE):
            start = pl.multiple_of(index * orders + first, TILE)
            target[first : first + TILE] = jnp.swapaxes(
                legendre_ref[:, pl.ds(start, TILE), :], 0, 1
            )
    part_ref[...] = own_ref[pl.ds((1 - side) * share, share)]


def part_kernel(place_ref, half_ref, part_ref):
    share = part_ref.shape[0]
    part_ref[...] = half_ref[pl.ds((1 - place_ref[1]) * share, share)]


def divided(kernel, place, values, orders, cycles):
    degrees = values.shape[2]
    return pl.pallas_call(
        kernel,
        in_specs=[SCALARS, NEARBY],
        out_specs=[NEARBY] * len(orders),
        out_shape=[
            jax.ShapeDtypeStruct((count, cycles, degrees), values.dtype) for count in orders
        ],
        cost_estimate=pl.CostEstimate(
            flops=1 << 20, bytes_accessed=4 * cycles * sum(orders) * degrees, transcendentals=0
        ),
        compiler_params=pltpu.CompilerParams(vmem_limit_bytes=ROOM),
    )(place, values)


def table_kernel(coarse_ref, fine_ref, table_ref):
    inner_table(coarse_ref, fine_ref, table_ref, slice(None))


def inner_tables(coarse, fine):
    shape = (2, INNER, coarse.shape[2])
    return pl.pallas_call(
        table_kernel,
        in_specs=[NEARBY] * 2,
        out_specs=NEARBY,
        out_shape=jax.ShapeDtypeStruct(shape, jnp.bfloat16),
        cost_estimate=pl.CostEstimate(
            flops=1 << 20, bytes_accessed=2 * math.prod(shape), transcendentals=0
        ),
        compiler_params=pltpu.CompilerParams(vmem_limit_bytes=ROOM),
        name="tables",
    )(coarse, fine)


def analysis_kernel(near, spot_ref, *refs):
    assignment_ref, moved_ref, *value_refs = refs[: near + 2]
    out_ref, row_ref, left_ref, joined_ref = refs[near + 2 :]
    share, _, two_fields, _ = left_ref.shape
    fields = two_fields // 2
    cycles = value_refs[0].shape[1]
    beside = LANES // cycles
    lines = moved_ref.shape[0]
    block = lines // fields
    deep = block // near
    spot = spot_ref[0]

    for slot in range(fields):
        source = pl.multiple_of(assignment_ref[slot] * block, block)
        row_ref[slot * block : (slot + 1) * block, :] = moved_ref[
            pl.ds(source, block), :
        ].astype(jnp.float32)
    for other in range(near):
        peer = jnp.bitwise_xor(spot, other)
        for row in range(deep):
            taken = row_ref[pl.ds(peer * deep + row, fields, stride=block), :]
            for column in range(beside):
                which, order = divmod(deep * column + row, share)
                left_ref[order, other, which * fields : (which + 1) * fields, :] = shift(
                    taken, -column * cycles
                ).astype(jnp.bfloat16)

    for order in range(share):
        for other in range(near):
            joined_ref[order % 2, other * cycles : (other + 1) * cycles, :] = value_refs[other][
                order
            ]
        left = jnp.concatenate(
            [left_ref[order, other][:, :cycles] for other in range(near)], axis=1
        )
        out_ref[2 * fields * order : 2 * fields * (order + 1), :] = jnp.dot(
            left, joined_ref[order % 2], preferred_element_type=jnp.float32
        ).astype(jnp.bfloat16)


def analyse(spot, assignment, moved, values):
    share, cycles, degrees = values[0].shape
    fields = assignment.shape[0]
    return pl.pallas_call(
        functools.partial(analysis_kernel, len(values)),
        in_specs=[SCALARS] * 2 + [NEARBY] * (1 + len(values)),
        out_specs=NEARBY,
        scratch_shapes=[
            pltpu.VMEM(moved.shape, jnp.float32),
            pltpu.VMEM((share, len(values), 2 * fields, LANES), jnp.bfloat16),
            pltpu.VMEM((2, len(values) * cycles, degrees), jnp.bfloat16),
        ],
        out_shape=jax.ShapeDtypeStruct((share * 2 * fields, degrees), jnp.bfloat16),
        cost_estimate=pl.CostEstimate(
            flops=4 * fields * share * cycles * degrees * len(values),
            bytes_accessed=4 << 20,
            transcendentals=0,
        ),
        compiler_params=pltpu.CompilerParams(vmem_limit_bytes=ROOM),
        name="analysis",
    )(spot, assignment, moved, *values)


def synthesis_kernel(near, spot_ref, first_ref, *refs):
    coefficient_ref, *value_refs = refs[: near + 1]
    out_ref, right_ref, row_ref, joined_ref = refs[near + 1 :]
    share, _, two_fields, _ = right_ref.shape
    fields = two_fields // 2
    cycles = value_refs[0].shape[1]
    beside = LANES // cycles
    lines = out_ref.shape[0]
    block = lines // fields
    deep = block // near
    dims = (((1,), (1,)), ((), ()))
    for order in range(share):
        factor = jnp.where(first_ref[0] + order == 0, 1.0, 2.0).astype(jnp.float32)
        for other in range(near):
            skip = 0 if value_refs[other].shape[0] == share else share * (spot_ref[0] % 2)
            joined_ref[order % 2, other * cycles : (other + 1) * cycles, :] = value_refs[other][
                skip + order
            ]
        product = factor * lax.dot_general(
            coefficient_ref[2 * fields * order : 2 * fields * (order + 1), :],
            joined_ref[order % 2],
            dims,
            preferred_element_type=jnp.float32,
        )
        for other in range(near):
            right_ref[order, other, :, :cycles] = product[
                :, other * cycles : (other + 1) * cycles
            ]
    for other in range(near):
        peer = jnp.bitwise_xor(spot_ref[0], other)
        for row in range(deep):
            pieces = []
            for column in range(beside):
                which, own = divmod(deep * column + row, share)
                pieces.append(right_ref[own, other, which * fields : (which + 1) * fields, :])
            row_ref[pl.ds(peer * deep + row, fields, stride=block), :] = side_by_side(
                pieces, cycles
            )
    out_ref[...] = row_ref[...].astype(jnp.bfloat16)


def synthesise(spot, first, coefficients, values, lines):
    share = min(value.shape[0] for value in values)
    _, cycles, degrees = values[0].shape
    fields = coefficients.shape[0] // (2 * share)
    return pl.pallas_call(
        functools.partial(synthesis_kernel, len(values)),
        in_specs=[SCALARS] * 2 + [NEARBY] * (1 + len(values)),
        out_specs=NEARBY,
        scratch_shapes=[
            pltpu.VMEM((share, len(values), 2 * fields, LANES), jnp.float32),
            pltpu.VMEM((lines, LANES), jnp.float32),
            pltpu.VMEM((2, len(values) * cycles, degrees), jnp.bfloat16),
        ],
        out_shape=jax.ShapeDtypeStruct((lines, LANES), jnp.bfloat16),
        cost_estimate=pl.CostEstimate(
            flops=4 * fields * share * cycles * degrees * len(values),
            bytes_accessed=4 << 20,
            transcendentals=0,
        ),
        compiler_params=pltpu.CompilerParams(vmem_limit_bytes=ROOM),
        name="synthesis",
    )(spot, first, coefficients, *values)


def inverse_kernel(
    peers,
    moved_ref,
    table_ref,
    turn_ref,
    out_ref,
    rows_ref,
    row_ref,
    flip_ref,
    part_ref,
    sems,
):
    parts, cycles, span = part_ref.shape
    count = span // INNER
    orders = flip_ref.shape[1]
    row_ref[...] = moved_ref[...].astype(jnp.float32)
    deep = moved_ref.shape[0] // peers
    share = orders // peers
    for row in range(deep):
        taken = row_ref[pl.ds(row, peers, stride=deep), :]
        for column in range(LANES // cycles):
            which, order = divmod(deep * column + row, share)
            flip_ref[which, pl.ds(order, peers, stride=share), :] = shift(
                taken, -column * cycles
            )
    first = jnp.transpose(flip_ref[0])[:cycles]
    second = jnp.transpose(flip_ref[1])[:cycles]
    dims = (((1,), (1,)), ((), ()))
    copies = []
    for part in range(parts):
        for step in range(count):
            rows = slice(step * cycles, (step + 1) * cycles)
            turn = part * count + step
            cosine, sine = turn_ref[0, turn : turn + 1, :], turn_ref[1, turn : turn + 1, :]
            rows_ref[part % 2, 0, rows, :] = (first * cosine - second * sine).astype(jnp.bfloat16)
            rows_ref[part % 2, 1, rows, :] = (first * sine + second * cosine).astype(jnp.bfloat16)
        result = lax.dot_general(
            rows_ref[part % 2, 0], table_ref[0], dims, preferred_element_type=jnp.float32
        ) + lax.dot_general(
            rows_ref[part % 2, 1], table_ref[1], dims, preferred_element_type=jnp.float32
        )
        for step in range(count):
            part_ref[part, :, step * INNER : (step + 1) * INNER] = result[
                step * cycles : (step + 1) * cycles
            ]
        copy = pltpu.make_async_copy(
            part_ref.at[part], out_ref.at[:, part * span : (part + 1) * span], sems.at[part]
        )
        copy.start()
        copies.append(copy)
    for copy in copies:
        copy.wait()


def inverse(moved, table, turn, cycles, longitudes, peers):
    orders = turn.shape[2]
    count = 6
    parts = longitudes // INNER // count
    return pl.pallas_call(
        functools.partial(inverse_kernel, peers),
        in_specs=[NEARBY] * 3,
        out_specs=pl.BlockSpec(memory_space=pltpu.HBM),
        out_shape=jax.ShapeDtypeStruct((cycles, longitudes), jnp.float32),
        scratch_shapes=[
            pltpu.VMEM((2, 2, count * cycles, orders), jnp.bfloat16),
            pltpu.VMEM(moved.shape, jnp.float32),
            pltpu.VMEM((2, orders, LANES), jnp.float32),
            pltpu.VMEM((parts, cycles, count * INNER), jnp.float32),
            pltpu.SemaphoreType.DMA((parts,)),
        ],
        cost_estimate=pl.CostEstimate(
            flops=4 * cycles * longitudes * orders, bytes_accessed=1 << 20, transcendentals=0
        ),
        compiler_params=pltpu.CompilerParams(vmem_limit_bytes=ROOM),
        name="inverse_dft",
    )(moved, table, turn)


def local(elevation, legendre, cycle_weight, love_factor, assignment):
    _, cycle_dev, longitudes = elevation.shape
    orders_dev, degrees = legendre.shape[1:]
    groups = lax.axis_size("cons")
    cores, near = lax.axis_size(CORE), lax.axis_size(NEAR)
    deep, far = lax.axis_size(DEEP), lax.axis_size(FAR)
    orders = orders_dev * groups
    spot, core = lax.axis_index(NEAR), lax.axis_index(CORE)
    side = lax.axis_index("blk_0")
    coarse = jnp.asarray(angle_tables(FINE, FINE, longitudes, orders))
    fine = jnp.asarray(angle_tables(FINE, 1, longitudes, orders))
    turn = jnp.asarray(angle_tables(longitudes // INNER, INNER, longitudes, orders))

    def swapped(values, other):
        pairs = [(index, index ^ other) for index in range(near)]
        return lax.ppermute(values, NEAR[::-1], pairs)

    half, share = orders_dev // cores, orders_dev // near
    place = jnp.stack([core, side]).astype(jnp.int32)

    def exchanged(packed, axes):
        peers = lax.axis_size(axes)
        tiles = packed.reshape(peers, -1, LANES)
        tiles = lax.all_to_all(tiles, axes, 0, 0, tiled=True)
        return tiles.reshape(-1, LANES)

    sent, own, own_part = divided(split_kernel, place, legendre, (half, half, share), cycle_dev)
    met = swapped(sent, 1)
    own_side = swapped(own_part, 2)
    (sent_part,) = divided(part_kernel, place, sent, (share,), cycle_dev)
    met_side = swapped(sent_part, 3)
    table = inner_tables(coarse, fine)
    lines = groups * orders_dev * 2 // (LANES // cycle_dev)
    packed = forward(elevation[0], cycle_weight[:, None], coarse, fine, turn, lines, groups * cores)
    moved = exchanged(packed, ("cons", CORE))
    partial = analyse(core[None].astype(jnp.int32), assignment, moved, [own, met])
    rows = partial.shape[0] // far
    arrived = lax.all_to_all(partial.reshape(far, rows, degrees), FAR, 0, 0, tiled=True)
    analysis = jnp.sum(arrived.astype(jnp.float32), axis=0)
    scaled = (analysis * love_factor[None, :]).astype(jnp.bfloat16)
    copies = jnp.broadcast_to(scaled[None], (deep, rows, degrees))
    coefficients = lax.all_to_all(copies, DEEP, 0, 0, tiled=True)
    first = ((lax.axis_index("cons") * near + spot) * share)[None].astype(jnp.int32)
    synthesis = synthesise(
        spot[None].astype(jnp.int32),
        first,
        coefficients.reshape(-1, degrees),
        [own, own_side, met, met_side],
        lines,
    )
    returned = exchanged(synthesis, ("cons", *NEAR))
    return inverse(returned, table, turn, cycle_dev, longitudes, groups * near)[None]


def solution(mesh):
    torus = Mesh(
        mesh.devices.reshape(mesh.shape["cons"], 2, 8, 2), ("cons", *BLK)
    )
    placed = (P("cons", BLK, None), P(BLK, "cons", None), P(BLK), P(), P())
    return jax.shard_map(
        local, mesh=torus, in_specs=placed, out_specs=P("cons", BLK, None), check_vma=False
    )
```

```python
import functools
import math

import jax
import jax.numpy as jnp
import numpy as np
from jax import lax
from jax.experimental import pallas as pl
from jax.experimental.pallas import tpu as pltpu
from jax.sharding import Mesh
from jax.sharding import PartitionSpec as P

BLK = ("blk_0", "blk_1", "blk_2")
NEAR = ("blk_2", "blk_0")
CORE = "blk_2"
DEEP = "blk_1"
FAR = ("blk_0", "blk_1")
FINE = 16
INNER = FINE * FINE
LANES = 128
TILE = 8
ROOM = 24 << 20
SCALARS = pl.BlockSpec(memory_space=pltpu.SMEM)
NEARBY = pl.BlockSpec(memory_space=pltpu.VMEM)


def angle_tables(steps, stride, period, orders):
    phases = (np.arange(steps)[:, None] * stride * np.arange(orders)[None, :]) % period
    angles = phases * (2.0 * np.pi / period)
    return np.stack([np.cos(angles), np.sin(angles)]).astype(np.float32)


def inner_table(coarse_ref, fine_ref, table_ref, lanes):
    fine_cos, fine_sin = fine_ref[0, :, lanes], fine_ref[1, :, lanes]
    for step in range(FINE):
        rows = slice(step * FINE, (step + 1) * FINE)
        coarse_cos = coarse_ref[0, step : step + 1, lanes]
        coarse_sin = coarse_ref[1, step : step + 1, lanes]
        cosine = coarse_cos * fine_cos - coarse_sin * fine_sin
        sine = coarse_sin * fine_cos + coarse_cos * fine_sin
        table_ref[0, rows, lanes] = cosine.astype(jnp.bfloat16)
        table_ref[1, rows, lanes] = (-sine).astype(jnp.bfloat16)


def shift(values, amount):
    amount %= LANES
    return values if amount == 0 else pltpu.roll(values, amount, values.ndim - 1)


def side_by_side(pieces, width):
    lane = lax.broadcasted_iota(jnp.int32, pieces[0].shape, pieces[0].ndim - 1)
    joined = jnp.zeros_like(pieces[0])
    for index, piece in reversed(list(enumerate(pieces))):
        joined = jnp.where(lane < (index + 1) * width, shift(piece, index * width), joined)
    return jnp.where(lane < len(pieces) * width, joined, 0.0)


def forward_kernel(
    peers,
    elevation_ref,
    weight_ref,
    coarse_ref,
    fine_ref,
    turn_ref,
    out_ref,
    rows_ref,
    table_ref,
    flip_ref,
    pack_ref,
):
    cycles = elevation_ref.shape[0]
    turns = turn_ref.shape[1]
    orders = flip_ref.shape[1]
    for turn in range(turns):
        rows_ref[turn * cycles : (turn + 1) * cycles, :] = elevation_ref[
            :, turn * INNER : (turn + 1) * INNER
        ]
    weight = weight_ref[...]
    inner_table(coarse_ref, fine_ref, table_ref, slice(None))
    for part in range(orders // INNER):
        lanes = slice(part * INNER, (part + 1) * INNER)
        even = jnp.dot(rows_ref[...], table_ref[0, :, lanes], preferred_element_type=jnp.float32)
        odd = jnp.dot(rows_ref[...], table_ref[1, :, lanes], preferred_element_type=jnp.float32)
        first = second = None
        for turn in range(turns):
            rows = slice(turn * cycles, (turn + 1) * cycles)
            cosine, sine = turn_ref[0, turn : turn + 1, lanes], turn_ref[1, turn : turn + 1, lanes]
            one = even[rows] * cosine + odd[rows] * sine
            two = odd[rows] * cosine - even[rows] * sine
            first = one if first is None else first + one
            second = two if second is None else second + two
        flip_ref[0, lanes, :cycles] = jnp.transpose(first) * weight
        flip_ref[1, lanes, :cycles] = jnp.transpose(second) * weight

    beside = LANES // cycles
    deep = out_ref.shape[0] // peers
    share = orders // peers
    for row in range(deep):
        pieces = []
        for column in range(beside):
            which, order = divmod(deep * column + row, share)
            pieces.append(flip_ref[which, pl.ds(order, peers, stride=share), :])
        pack_ref[pl.ds(row, peers, stride=deep), :] = side_by_side(pieces, cycles)
    out_ref[...] = pack_ref[...].astype(jnp.bfloat16)


def forward(elevation, weight, coarse, fine, turn, lines, peers):
    cycles, longitudes = elevation.shape
    orders = coarse.shape[2]
    turns = longitudes // INNER
    return pl.pallas_call(
        functools.partial(forward_kernel, peers),
        in_specs=[NEARBY] * 5,
        out_specs=NEARBY,
        out_shape=jax.ShapeDtypeStruct((lines, LANES), jnp.bfloat16),
        scratch_shapes=[
            pltpu.VMEM((turns * cycles, INNER), jnp.bfloat16),
            pltpu.VMEM((2, INNER, orders), jnp.bfloat16),
            pltpu.VMEM((2, orders, LANES), jnp.float32),
            pltpu.VMEM((lines, LANES), jnp.float32),
        ],
        cost_estimate=pl.CostEstimate(
            flops=4 * cycles * longitudes * orders, bytes_accessed=1 << 20, transcendentals=0
        ),
        name="forward_dft",
    )(elevation, weight, coarse, fine, turn)


def split_kernel(place_ref, legendre_ref, sent_ref, own_ref, part_ref):
    core, side = place_ref[0], place_ref[1]
    orders, share = own_ref.shape[0], part_ref.shape[0]
    for target, index in ((sent_ref, 1 - core), (own_ref, core)):
        for first in range(0, orders, TILE):
            start = pl.multiple_of(index * orders + first, TILE)
            target[first : first + TILE] = jnp.swapaxes(
                legendre_ref[:, pl.ds(start, TILE), :], 0, 1
            )
    part_ref[...] = own_ref[pl.ds((1 - side) * share, share)]


def part_kernel(place_ref, half_ref, part_ref):
    share = part_ref.shape[0]
    part_ref[...] = half_ref[pl.ds((1 - place_ref[1]) * share, share)]


def divided(kernel, place, values, orders, cycles):
    degrees = values.shape[2]
    return pl.pallas_call(
        kernel,
        in_specs=[SCALARS, NEARBY],
        out_specs=[NEARBY] * len(orders),
        out_shape=[
            jax.ShapeDtypeStruct((count, cycles, degrees), values.dtype) for count in orders
        ],
        cost_estimate=pl.CostEstimate(
            flops=1 << 20, bytes_accessed=4 * cycles * sum(orders) * degrees, transcendentals=0
        ),
        compiler_params=pltpu.CompilerParams(vmem_limit_bytes=ROOM),
    )(place, values)


def table_kernel(coarse_ref, fine_ref, table_ref):
    inner_table(coarse_ref, fine_ref, table_ref, slice(None))


def inner_tables(coarse, fine):
    shape = (2, INNER, coarse.shape[2])
    return pl.pallas_call(
        table_kernel,
        in_specs=[NEARBY] * 2,
        out_specs=NEARBY,
        out_shape=jax.ShapeDtypeStruct(shape, jnp.bfloat16),
        cost_estimate=pl.CostEstimate(
            flops=1 << 20, bytes_accessed=2 * math.prod(shape), transcendentals=0
        ),
        compiler_params=pltpu.CompilerParams(vmem_limit_bytes=ROOM),
        name="tables",
    )(coarse, fine)


def analysis_kernel(near, spot_ref, *refs):
    assignment_ref, moved_ref, *value_refs = refs[: near + 2]
    out_ref, row_ref, left_ref, joined_ref = refs[near + 2 :]
    share, _, two_fields, _ = left_ref.shape
    fields = two_fields // 2
    cycles = value_refs[0].shape[1]
    beside = LANES // cycles
    lines = moved_ref.shape[0]
    block = lines // fields
    deep = block // near
    spot = spot_ref[0]

    for slot in range(fields):
        source = pl.multiple_of(assignment_ref[slot] * block, block)
        row_ref[slot * block : (slot + 1) * block, :] = moved_ref[
            pl.ds(source, block), :
        ].astype(jnp.float32)
    for other in range(near):
        peer = jnp.bitwise_xor(spot, other)
        for row in range(deep):
            taken = row_ref[pl.ds(peer * deep + row, fields, stride=block), :]
            for column in range(beside):
                which, order = divmod(deep * column + row, share)
                left_ref[order, other, which * fields : (which + 1) * fields, :] = shift(
                    taken, -column * cycles
                ).astype(jnp.bfloat16)

    for order in range(share):
        for other in range(near):
            joined_ref[order % 2, other * cycles : (other + 1) * cycles, :] = value_refs[other][
                order
            ]
        left = jnp.concatenate(
            [left_ref[order, other][:, :cycles] for other in range(near)], axis=1
        )
        out_ref[2 * fields * order : 2 * fields * (order + 1), :] = jnp.dot(
            left, joined_ref[order % 2], preferred_element_type=jnp.float32
        ).astype(jnp.bfloat16)


def analyse(spot, assignment, moved, values):
    share, cycles, degrees = values[0].shape
    fields = assignment.shape[0]
    return pl.pallas_call(
        functools.partial(analysis_kernel, len(values)),
        in_specs=[SCALARS] * 2 + [NEARBY] * (1 + len(values)),
        out_specs=NEARBY,
        scratch_shapes=[
            pltpu.VMEM(moved.shape, jnp.float32),
            pltpu.VMEM((share, len(values), 2 * fields, LANES), jnp.bfloat16),
            pltpu.VMEM((2, len(values) * cycles, degrees), jnp.bfloat16),
        ],
        out_shape=jax.ShapeDtypeStruct((share * 2 * fields, degrees), jnp.bfloat16),
        cost_estimate=pl.CostEstimate(
            flops=4 * fields * share * cycles * degrees * len(values),
            bytes_accessed=4 << 20,
            transcendentals=0,
        ),
        compiler_params=pltpu.CompilerParams(vmem_limit_bytes=ROOM),
        name="analysis",
    )(spot, assignment, moved, *values)


def synthesis_kernel(near, spot_ref, first_ref, *refs):
    coefficient_ref, *value_refs = refs[: near + 1]
    out_ref, right_ref, row_ref, joined_ref = refs[near + 1 :]
    share, _, two_fields, _ = right_ref.shape
    fields = two_fields // 2
    cycles = value_refs[0].shape[1]
    beside = LANES // cycles
    lines = out_ref.shape[0]
    block = lines // fields
    deep = block // near
    dims = (((1,), (1,)), ((), ()))
    for order in range(share):
        factor = jnp.where(first_ref[0] + order == 0, 1.0, 2.0).astype(jnp.float32)
        for other in range(near):
            skip = 0 if value_refs[other].shape[0] == share else share * (spot_ref[0] % 2)
            joined_ref[order % 2, other * cycles : (other + 1) * cycles, :] = value_refs[other][
                skip + order
            ]
        product = factor * lax.dot_general(
            coefficient_ref[2 * fields * order : 2 * fields * (order + 1), :],
            joined_ref[order % 2],
            dims,
            preferred_element_type=jnp.float32,
        )
        for other in range(near):
            right_ref[order, other, :, :cycles] = product[
                :, other * cycles : (other + 1) * cycles
            ]
    for other in range(near):
        peer = jnp.bitwise_xor(spot_ref[0], other)
        for row in range(deep):
            pieces = []
            for column in range(beside):
                which, own = divmod(deep * column + row, share)
                pieces.append(right_ref[own, other, which * fields : (which + 1) * fields, :])
            row_ref[pl.ds(peer * deep + row, fields, stride=block), :] = side_by_side(
                pieces, cycles
            )
    out_ref[...] = row_ref[...].astype(jnp.bfloat16)


def synthesise(spot, first, coefficients, values, lines):
    share = min(value.shape[0] for value in values)
    _, cycles, degrees = values[0].shape
    fields = coefficients.shape[0] // (2 * share)
    return pl.pallas_call(
        functools.partial(synthesis_kernel, len(values)),
        in_specs=[SCALARS] * 2 + [NEARBY] * (1 + len(values)),
        out_specs=NEARBY,
        scratch_shapes=[
            pltpu.VMEM((share, len(values), 2 * fields, LANES), jnp.float32),
            pltpu.VMEM((lines, LANES), jnp.float32),
            pltpu.VMEM((2, len(values) * cycles, degrees), jnp.bfloat16),
        ],
        out_shape=jax.ShapeDtypeStruct((lines, LANES), jnp.bfloat16),
        cost_estimate=pl.CostEstimate(
            flops=4 * fields * share * cycles * degrees * len(values),
            bytes_accessed=4 << 20,
            transcendentals=0,
        ),
        compiler_params=pltpu.CompilerParams(vmem_limit_bytes=ROOM),
        name="synthesis",
    )(spot, first, coefficients, *values)


def inverse_kernel(
    peers,
    moved_ref,
    table_ref,
    turn_ref,
    out_ref,
    rows_ref,
    row_ref,
    flip_ref,
    part_ref,
    sems,
):
    parts, cycles, span = part_ref.shape
    count = span // INNER
    orders = flip_ref.shape[1]
    row_ref[...] = moved_ref[...].astype(jnp.float32)
    deep = moved_ref.shape[0] // peers
    share = orders // peers
    for row in range(deep):
        taken = row_ref[pl.ds(row, peers, stride=deep), :]
        for column in range(LANES // cycles):
            which, order = divmod(deep * column + row, share)
            flip_ref[which, pl.ds(order, peers, stride=share), :] = shift(
                taken, -column * cycles
            )
    first = jnp.transpose(flip_ref[0])[:cycles]
    second = jnp.transpose(flip_ref[1])[:cycles]
    dims = (((1,), (1,)), ((), ()))
    copies = []
    for part in range(parts):
        for step in range(count):
            rows = slice(step * cycles, (step + 1) * cycles)
            turn = part * count + step
            cosine, sine = turn_ref[0, turn : turn + 1, :], turn_ref[1, turn : turn + 1, :]
            rows_ref[part % 2, 0, rows, :] = (first * cosine - second * sine).astype(jnp.bfloat16)
            rows_ref[part % 2, 1, rows, :] = (first * sine + second * cosine).astype(jnp.bfloat16)
        result = lax.dot_general(
            rows_ref[part % 2, 0], table_ref[0], dims, preferred_element_type=jnp.float32
        ) + lax.dot_general(
            rows_ref[part % 2, 1], table_ref[1], dims, preferred_element_type=jnp.float32
        )
        for step in range(count):
            part_ref[part, :, step * INNER : (step + 1) * INNER] = result[
                step * cycles : (step + 1) * cycles
            ]
        copy = pltpu.make_async_copy(
            part_ref.at[part], out_ref.at[:, part * span : (part + 1) * span], sems.at[part]
        )
        copy.start()
        copies.append(copy)
    for copy in copies:
        copy.wait()


def inverse(moved, table, turn, cycles, longitudes, peers):
    orders = turn.shape[2]
    count = 6
    parts = longitudes // INNER // count
    return pl.pallas_call(
        functools.partial(inverse_kernel, peers),
        in_specs=[NEARBY] * 3,
        out_specs=pl.BlockSpec(memory_space=pltpu.HBM),
        out_shape=jax.ShapeDtypeStruct((cycles, longitudes), jnp.float32),
        scratch_shapes=[
            pltpu.VMEM((2, 2, count * cycles, orders), jnp.bfloat16),
            pltpu.VMEM(moved.shape, jnp.float32),
            pltpu.VMEM((2, orders, LANES), jnp.float32),
            pltpu.VMEM((parts, cycles, count * INNER), jnp.float32),
            pltpu.SemaphoreType.DMA((parts,)),
        ],
        cost_estimate=pl.CostEstimate(
            flops=4 * cycles * longitudes * orders, bytes_accessed=1 << 20, transcendentals=0
        ),
        compiler_params=pltpu.CompilerParams(vmem_limit_bytes=ROOM),
        name="inverse_dft",
    )(moved, table, turn)


def local(elevation, legendre, cycle_weight, love_factor, assignment):
    _, cycle_dev, longitudes = elevation.shape
    orders_dev, degrees = legendre.shape[1:]
    groups = lax.axis_size("cons")
    cores, near = lax.axis_size(CORE), lax.axis_size(NEAR)
    deep, far = lax.axis_size(DEEP), lax.axis_size(FAR)
    orders = orders_dev * groups
    spot, core = lax.axis_index(NEAR), lax.axis_index(CORE)
    side = lax.axis_index("blk_0")
    coarse = jnp.asarray(angle_tables(FINE, FINE, longitudes, orders))
    fine = jnp.asarray(angle_tables(FINE, 1, longitudes, orders))
    turn = jnp.asarray(angle_tables(longitudes // INNER, INNER, longitudes, orders))

    def swapped(values, other):
        pairs = [(index, index ^ other) for index in range(near)]
        return lax.ppermute(values, NEAR[::-1], pairs)

    half, share = orders_dev // cores, orders_dev // near
    place = jnp.stack([core, side]).astype(jnp.int32)

    def exchanged(packed, axes):
        peers = lax.axis_size(axes)
        tiles = packed.reshape(peers, -1, LANES)
        tiles = lax.all_to_all(tiles, axes, 0, 0, tiled=True)
        return tiles.reshape(-1, LANES)

    sent, own, own_part = divided(split_kernel, place, legendre, (half, half, share), cycle_dev)
    met = swapped(sent, 1)
    own_side = swapped(own_part, 2)
    (sent_part,) = divided(part_kernel, place, sent, (share,), cycle_dev)
    met_side = swapped(sent_part, 3)
    table = inner_tables(coarse, fine)
    lines = groups * orders_dev * 2 // (LANES // cycle_dev)
    packed = forward(elevation[0], cycle_weight[None, :], coarse, fine, turn, lines, groups * cores)
    moved = exchanged(packed, ("cons", CORE))
    partial = analyse(core[None].astype(jnp.int32), assignment, moved, [own, met])
    rows = partial.shape[0] // far
    arrived = lax.all_to_all(partial.reshape(far, rows, degrees), FAR, 0, 0, tiled=True)
    analysis = jnp.sum(arrived.astype(jnp.float32), axis=0)
    scaled = (analysis * love_factor[None, :]).astype(jnp.bfloat16)
    copies = jnp.broadcast_to(scaled[None], (deep, rows, degrees))
    coefficients = lax.all_to_all(copies, DEEP, 0, 0, tiled=True)
    first = ((lax.axis_index("cons") * near + spot) * share)[None].astype(jnp.int32)
    synthesis = synthesise(
        spot[None].astype(jnp.int32),
        first,
        coefficients.reshape(-1, degrees),
        [own, own_side, met, met_side],
        lines,
    )
    returned = exchanged(synthesis, ("cons", *NEAR))
    return inverse(returned, table, turn, cycle_dev, longitudes, groups * near)[None]


def solution(mesh):
    torus = Mesh(
        mesh.devices.reshape(mesh.shape["cons"], 2, 8, 2), ("cons", *BLK)
    )
    placed = (P("cons", BLK, None), P(BLK, "cons", None), P(BLK), P(), P())
    return jax.shard_map(
        local, mesh=torus, in_specs=placed, out_specs=P("cons", BLK, None), check_vma=False
    )
```

```python
import functools
import math

import jax
import jax.numpy as jnp
import numpy as np
from jax import lax
from jax.experimental import pallas as pl
from jax.experimental.pallas import tpu as pltpu
from jax.sharding import Mesh
from jax.sharding import PartitionSpec as P

BLK = ("blk_0", "blk_1", "blk_2")
NEAR = ("blk_2", "blk_0")
CORE = "blk_2"
DEEP = "blk_1"
FAR = ("blk_0", "blk_1")
FINE = 16
INNER = FINE * FINE
LANES = 128
TILE = 8
ROOM = 24 << 20
SCALARS = pl.BlockSpec(memory_space=pltpu.SMEM)
NEARBY = pl.BlockSpec(memory_space=pltpu.VMEM)


def angle_tables(steps, stride, period, orders):
    phases = (np.arange(steps)[:, None] * stride * np.arange(orders)[None, :]) % period
    angles = phases * (2.0 * np.pi / period)
    return np.stack([np.cos(angles), np.sin(angles)]).astype(np.float32)


def inner_table(coarse_ref, fine_ref, table_ref, lanes):
    fine_cos, fine_sin = fine_ref[0, :, lanes], fine_ref[1, :, lanes]
    for step in range(FINE):
        rows = slice(step * FINE, (step + 1) * FINE)
        coarse_cos = coarse_ref[0, step : step + 1, lanes]
        coarse_sin = coarse_ref[1, step : step + 1, lanes]
        cosine = coarse_cos * fine_cos - coarse_sin * fine_sin
        sine = coarse_sin * fine_cos + coarse_cos * fine_sin
        table_ref[0, rows, lanes] = cosine.astype(jnp.bfloat16)
        table_ref[1, rows, lanes] = (-sine).astype(jnp.bfloat16)


def shift(values, amount):
    amount %= LANES
    return values if amount == 0 else pltpu.roll(values, amount, values.ndim - 1)


def side_by_side(pieces, width):
    lane = lax.broadcasted_iota(jnp.int32, pieces[0].shape, pieces[0].ndim - 1)
    joined = jnp.zeros_like(pieces[0])
    for index, piece in reversed(list(enumerate(pieces))):
        joined = jnp.where(lane < (index + 1) * width, shift(piece, index * width), joined)
    return jnp.where(lane < len(pieces) * width, joined, 0.0)


def forward_kernel(
    peers,
    elevation_ref,
    weight_ref,
    coarse_ref,
    fine_ref,
    turn_ref,
    out_ref,
    rows_ref,
    table_ref,
    flip_ref,
    pack_ref,
):
    cycles = elevation_ref.shape[0]
    turns = turn_ref.shape[1]
    orders = flip_ref.shape[1]
    for turn in range(turns):
        rows_ref[turn * cycles : (turn + 1) * cycles, :] = elevation_ref[
            :, turn * INNER : (turn + 1) * INNER
        ]
    weight = weight_ref[...]
    inner_table(coarse_ref, fine_ref, table_ref, slice(None))
    for part in range(orders // INNER):
        lanes = slice(part * INNER, (part + 1) * INNER)
        even = jnp.dot(rows_ref[...], table_ref[0, :, lanes], preferred_element_type=jnp.float32)
        odd = jnp.dot(rows_ref[...], table_ref[1, :, lanes], preferred_element_type=jnp.float32)
        first = second = None
        for turn in range(turns):
            rows = slice(turn * cycles, (turn + 1) * cycles)
            cosine, sine = turn_ref[0, turn : turn + 1, lanes], turn_ref[1, turn : turn + 1, lanes]
            one = even[rows] * cosine + odd[rows] * sine
            two = odd[rows] * cosine - even[rows] * sine
            first = one if first is None else first + one
            second = two if second is None else second + two
        flip_ref[0, lanes, :cycles] = jnp.transpose(first) * weight
        flip_ref[1, lanes, :cycles] = jnp.transpose(second) * weight

    beside = LANES // cycles
    deep = out_ref.shape[0] // peers
    share = orders // peers
    for row in range(deep):
        pieces = []
        for column in range(beside):
            which, order = divmod(deep * column + row, share)
            pieces.append(flip_ref[which, pl.ds(order, peers, stride=share), :])
        pack_ref[pl.ds(row, peers, stride=deep), :] = side_by_side(pieces, cycles)
    out_ref[...] = pack_ref[...].astype(jnp.bfloat16)


def forward(elevation, weight, coarse, fine, turn, lines, peers):
    cycles, longitudes = elevation.shape
    orders = coarse.shape[2]
    turns = longitudes // INNER
    return pl.pallas_call(
        functools.partial(forward_kernel, peers),
        in_specs=[NEARBY] * 5,
        out_specs=NEARBY,
        out_shape=jax.ShapeDtypeStruct((lines, LANES), jnp.bfloat16),
        scratch_shapes=[
            pltpu.VMEM((turns * cycles, INNER), jnp.bfloat16),
            pltpu.VMEM((2, INNER, orders), jnp.bfloat16),
            pltpu.VMEM((2, orders, LANES), jnp.float32),
            pltpu.VMEM((lines, LANES), jnp.float32),
        ],
        cost_estimate=pl.CostEstimate(
            flops=4 * cycles * longitudes * orders, bytes_accessed=1 << 20, transcendentals=0
        ),
        name="forward_dft",
    )(elevation, weight, coarse, fine, turn)


def split_kernel(place_ref, legendre_ref, sent_ref, own_ref, part_ref):
    core, side = place_ref[0], place_ref[1]
    orders, share = own_ref.shape[0], part_ref.shape[0]
    for target, index in ((sent_ref, 1 - core), (own_ref, core)):
        for first in range(0, orders, TILE):
            start = pl.multiple_of(index * orders + first, TILE)
            target[first : first + TILE] = jnp.swapaxes(
                legendre_ref[:, pl.ds(start, TILE), :], 0, 1
            )
    part_ref[...] = own_ref[pl.ds((1 - side) * share, share)]


def part_kernel(place_ref, half_ref, part_ref):
    share = part_ref.shape[0]
    part_ref[...] = half_ref[pl.ds((1 - place_ref[1]) * share, share)]


def divided(kernel, place, values, orders, cycles):
    degrees = values.shape[2]
    return pl.pallas_call(
        kernel,
        in_specs=[SCALARS, NEARBY],
        out_specs=[NEARBY] * len(orders),
        out_shape=[
            jax.ShapeDtypeStruct((count, cycles, degrees), values.dtype) for count in orders
        ],
        cost_estimate=pl.CostEstimate(
            flops=1 << 20, bytes_accessed=4 * cycles * sum(orders) * degrees, transcendentals=0
        ),
        compiler_params=pltpu.CompilerParams(vmem_limit_bytes=ROOM),
    )(place, values)


def table_kernel(which, coarse_ref, fine_ref, table_ref):
    fine_cos, fine_sin = fine_ref[0], fine_ref[1]
    for step in range(FINE):
        coarse_cos = coarse_ref[0, step : step + 1, :]
        coarse_sin = coarse_ref[1, step : step + 1, :]
        if which == "cosine":
            part = coarse_cos * fine_cos - coarse_sin * fine_sin
        else:
            part = -(coarse_sin * fine_cos + coarse_cos * fine_sin)
        table_ref[step * FINE : (step + 1) * FINE, :] = part.astype(jnp.bfloat16)


def table_of(which, coarse, fine):
    shape = (INNER, coarse.shape[2])
    return pl.pallas_call(
        functools.partial(table_kernel, which),
        in_specs=[NEARBY] * 2,
        out_specs=NEARBY,
        out_shape=jax.ShapeDtypeStruct(shape, jnp.bfloat16),
        cost_estimate=pl.CostEstimate(
            flops=1 << 20, bytes_accessed=2 * math.prod(shape), transcendentals=0
        ),
        compiler_params=pltpu.CompilerParams(vmem_limit_bytes=ROOM),
    )(coarse, fine)


def analysis_kernel(near, spot_ref, *refs):
    assignment_ref, moved_ref, *value_refs = refs[: near + 2]
    out_ref, row_ref, left_ref, joined_ref = refs[near + 2 :]
    share, _, two_fields, _ = left_ref.shape
    fields = two_fields // 2
    cycles = value_refs[0].shape[1]
    beside = LANES // cycles
    lines = moved_ref.shape[0]
    block = lines // fields
    deep = block // near
    spot = spot_ref[0]

    for slot in range(fields):
        source = pl.multiple_of(assignment_ref[slot] * block, block)
        row_ref[slot * block : (slot + 1) * block, :] = moved_ref[
            pl.ds(source, block), :
        ].astype(jnp.float32)
    for other in range(near):
        peer = jnp.bitwise_xor(spot, other)
        for row in range(deep):
            taken = row_ref[pl.ds(peer * deep + row, fields, stride=block), :]
            for column in range(beside):
                which, order = divmod(deep * column + row, share)
                left_ref[order, other, which * fields : (which + 1) * fields, :] = shift(
                    taken, -column * cycles
                ).astype(jnp.bfloat16)

    for order in range(share):
        for other in range(near):
            joined_ref[order % 2, other * cycles : (other + 1) * cycles, :] = value_refs[other][
                order
            ]
        left = jnp.concatenate(
            [left_ref[order, other][:, :cycles] for other in range(near)], axis=1
        )
        out_ref[2 * fields * order : 2 * fields * (order + 1), :] = jnp.dot(
            left, joined_ref[order % 2], preferred_element_type=jnp.float32
        ).astype(jnp.bfloat16)


def analyse(spot, assignment, moved, values):
    share, cycles, degrees = values[0].shape
    fields = assignment.shape[0]
    return pl.pallas_call(
        functools.partial(analysis_kernel, len(values)),
        in_specs=[SCALARS] * 2 + [NEARBY] * (1 + len(values)),
        out_specs=NEARBY,
        scratch_shapes=[
            pltpu.VMEM(moved.shape, jnp.float32),
            pltpu.VMEM((share, len(values), 2 * fields, LANES), jnp.bfloat16),
            pltpu.VMEM((2, len(values) * cycles, degrees), jnp.bfloat16),
        ],
        out_shape=jax.ShapeDtypeStruct((share * 2 * fields, degrees), jnp.bfloat16),
        cost_estimate=pl.CostEstimate(
            flops=4 * fields * share * cycles * degrees * len(values),
            bytes_accessed=4 << 20,
            transcendentals=0,
        ),
        compiler_params=pltpu.CompilerParams(vmem_limit_bytes=ROOM),
        name="analysis",
    )(spot, assignment, moved, *values)


def synthesis_kernel(near, spot_ref, first_ref, *refs):
    coefficient_ref, *value_refs = refs[: near + 1]
    out_ref, right_ref, row_ref, joined_ref = refs[near + 1 :]
    share, _, two_fields, _ = right_ref.shape
    fields = two_fields // 2
    cycles = value_refs[0].shape[1]
    beside = LANES // cycles
    lines = out_ref.shape[0]
    block = lines // fields
    deep = block // near
    dims = (((1,), (1,)), ((), ()))
    for order in range(share):
        factor = jnp.where(first_ref[0] + order == 0, 1.0, 2.0).astype(jnp.float32)
        for other in range(near):
            skip = 0 if value_refs[other].shape[0] == share else share * (spot_ref[0] % 2)
            joined_ref[order % 2, other * cycles : (other + 1) * cycles, :] = value_refs[other][
                skip + order
            ]
        product = factor * lax.dot_general(
            coefficient_ref[2 * fields * order : 2 * fields * (order + 1), :],
            joined_ref[order % 2],
            dims,
            preferred_element_type=jnp.float32,
        )
        for other in range(near):
            right_ref[order, other, :, :cycles] = product[
                :, other * cycles : (other + 1) * cycles
            ]
    for other in range(near):
        peer = jnp.bitwise_xor(spot_ref[0], other)
        for row in range(deep):
            pieces = []
            for column in range(beside):
                which, own = divmod(deep * column + row, share)
                pieces.append(right_ref[own, other, which * fields : (which + 1) * fields, :])
            row_ref[pl.ds(peer * deep + row, fields, stride=block), :] = side_by_side(
                pieces, cycles
            )
    out_ref[...] = row_ref[...].astype(jnp.bfloat16)


def synthesise(spot, first, coefficients, values, lines):
    share = min(value.shape[0] for value in values)
    _, cycles, degrees = values[0].shape
    fields = coefficients.shape[0] // (2 * share)
    return pl.pallas_call(
        functools.partial(synthesis_kernel, len(values)),
        in_specs=[SCALARS] * 2 + [NEARBY] * (1 + len(values)),
        out_specs=NEARBY,
        scratch_shapes=[
            pltpu.VMEM((share, len(values), 2 * fields, LANES), jnp.float32),
            pltpu.VMEM((lines, LANES), jnp.float32),
            pltpu.VMEM((2, len(values) * cycles, degrees), jnp.bfloat16),
        ],
        out_shape=jax.ShapeDtypeStruct((lines, LANES), jnp.bfloat16),
        cost_estimate=pl.CostEstimate(
            flops=4 * fields * share * cycles * degrees * len(values),
            bytes_accessed=4 << 20,
            transcendentals=0,
        ),
        compiler_params=pltpu.CompilerParams(vmem_limit_bytes=ROOM),
        name="synthesis",
    )(spot, first, coefficients, *values)


def inverse_kernel(
    peers,
    moved_ref,
    cosine_ref,
    sine_ref,
    turn_ref,
    out_ref,
    rows_ref,
    row_ref,
    flip_ref,
    part_ref,
    sems,
):
    parts, cycles, span = part_ref.shape
    count = span // INNER
    orders = flip_ref.shape[1]
    row_ref[...] = moved_ref[...].astype(jnp.float32)
    deep = moved_ref.shape[0] // peers
    share = orders // peers
    for row in range(deep):
        taken = row_ref[pl.ds(row, peers, stride=deep), :]
        for column in range(LANES // cycles):
            which, order = divmod(deep * column + row, share)
            flip_ref[which, pl.ds(order, peers, stride=share), :] = shift(
                taken, -column * cycles
            )
    first = jnp.transpose(flip_ref[0])[:cycles]
    second = jnp.transpose(flip_ref[1])[:cycles]
    dims = (((1,), (1,)), ((), ()))
    copies = []
    for part in range(parts):
        for step in range(count):
            rows = slice(step * cycles, (step + 1) * cycles)
            turn = part * count + step
            cosine, sine = turn_ref[0, turn : turn + 1, :], turn_ref[1, turn : turn + 1, :]
            rows_ref[part % 2, 0, rows, :] = (first * cosine - second * sine).astype(jnp.bfloat16)
            rows_ref[part % 2, 1, rows, :] = (first * sine + second * cosine).astype(jnp.bfloat16)
        result = lax.dot_general(
            rows_ref[part % 2, 0], cosine_ref[...], dims, preferred_element_type=jnp.float32
        ) + lax.dot_general(
            rows_ref[part % 2, 1], sine_ref[...], dims, preferred_element_type=jnp.float32
        )
        for step in range(count):
            part_ref[part, :, step * INNER : (step + 1) * INNER] = result[
                step * cycles : (step + 1) * cycles
            ]
        copy = pltpu.make_async_copy(
            part_ref.at[part], out_ref.at[:, part * span : (part + 1) * span], sems.at[part]
        )
        copy.start()
        copies.append(copy)
    for copy in copies:
        copy.wait()


def inverse(moved, tables, turn, cycles, longitudes, peers):
    orders = turn.shape[2]
    count = 6
    parts = longitudes // INNER // count
    return pl.pallas_call(
        functools.partial(inverse_kernel, peers),
        in_specs=[NEARBY] * 4,
        out_specs=pl.BlockSpec(memory_space=pltpu.HBM),
        out_shape=jax.ShapeDtypeStruct((cycles, longitudes), jnp.float32),
        scratch_shapes=[
            pltpu.VMEM((2, 2, count * cycles, orders), jnp.bfloat16),
            pltpu.VMEM(moved.shape, jnp.float32),
            pltpu.VMEM((2, orders, LANES), jnp.float32),
            pltpu.VMEM((parts, cycles, count * INNER), jnp.float32),
            pltpu.SemaphoreType.DMA((parts,)),
        ],
        cost_estimate=pl.CostEstimate(
            flops=4 * cycles * longitudes * orders, bytes_accessed=1 << 20, transcendentals=0
        ),
        compiler_params=pltpu.CompilerParams(vmem_limit_bytes=ROOM),
        name="inverse_dft",
    )(moved, *tables, turn)


def local(elevation, legendre, cycle_weight, love_factor, assignment):
    _, cycle_dev, longitudes = elevation.shape
    orders_dev, degrees = legendre.shape[1:]
    groups = lax.axis_size("cons")
    cores, near = lax.axis_size(CORE), lax.axis_size(NEAR)
    deep, far = lax.axis_size(DEEP), lax.axis_size(FAR)
    orders = orders_dev * groups
    spot, core = lax.axis_index(NEAR), lax.axis_index(CORE)
    side = lax.axis_index("blk_0")
    coarse = jnp.asarray(angle_tables(FINE, FINE, longitudes, orders))
    fine = jnp.asarray(angle_tables(FINE, 1, longitudes, orders))
    turn = jnp.asarray(angle_tables(longitudes // INNER, INNER, longitudes, orders))

    def swapped(values, other):
        pairs = [(index, index ^ other) for index in range(near)]
        return lax.ppermute(values, NEAR[::-1], pairs)

    half, share = orders_dev // cores, orders_dev // near
    place = jnp.stack([core, side]).astype(jnp.int32)

    def exchanged(packed, axes):
        peers = lax.axis_size(axes)
        tiles = packed.reshape(peers, -1, LANES)
        tiles = lax.all_to_all(tiles, axes, 0, 0, tiled=True)
        return tiles.reshape(-1, LANES)

    sent, own, own_part = divided(split_kernel, place, legendre, (half, half, share), cycle_dev)
    met = swapped(sent, 1)
    own_side = swapped(own_part, 2)
    (sent_part,) = divided(part_kernel, place, sent, (share,), cycle_dev)
    met_side = swapped(sent_part, 3)
    tables = [table_of(which, coarse, fine) for which in ("cosine", "sine")]
    lines = groups * orders_dev * 2 // (LANES // cycle_dev)
    packed = forward(elevation[0], cycle_weight[None, :], coarse, fine, turn, lines, groups * cores)
    moved = exchanged(packed, ("cons", CORE))
    partial = analyse(core[None].astype(jnp.int32), assignment, moved, [own, met])
    rows = partial.shape[0] // far
    arrived = lax.all_to_all(partial.reshape(far, rows, degrees), FAR, 0, 0, tiled=True)
    analysis = jnp.sum(arrived.astype(jnp.float32), axis=0)
    scaled = (analysis * love_factor[None, :]).astype(jnp.bfloat16)
    copies = jnp.broadcast_to(scaled[None], (deep, rows, degrees))
    coefficients = lax.all_to_all(copies, DEEP, 0, 0, tiled=True)
    first = ((lax.axis_index("cons") * near + spot) * share)[None].astype(jnp.int32)
    synthesis = synthesise(
        spot[None].astype(jnp.int32),
        first,
        coefficients.reshape(-1, degrees),
        [own, own_side, met, met_side],
        lines,
    )
    returned = exchanged(synthesis, ("cons", *NEAR))
    return inverse(returned, tables, turn, cycle_dev, longitudes, groups * near)[None]


def solution(mesh):
    torus = Mesh(
        mesh.devices.reshape(mesh.shape["cons"], 2, 8, 2), ("cons", *BLK)
    )
    placed = (P("cons", BLK, None), P(BLK, "cons", None), P(BLK), P(), P())
    return jax.shard_map(
        local, mesh=torus, in_specs=placed, out_specs=P("cons", BLK, None), check_vma=False
    )
```

```python
import functools
import math

import jax
import jax.numpy as jnp
import numpy as np
from jax import lax
from jax.experimental import pallas as pl
from jax.experimental.pallas import tpu as pltpu
from jax.sharding import Mesh
from jax.sharding import PartitionSpec as P

BLK = ("blk_0", "blk_1", "blk_2")
NEAR = ("blk_2", "blk_0")
CORE = "blk_2"
DEEP = "blk_1"
FAR = ("blk_0", "blk_1")
FINE = 16
INNER = FINE * FINE
LANES = 128
TILE = 8
ROOM = 24 << 20
SCALARS = pl.BlockSpec(memory_space=pltpu.SMEM)
NEARBY = pl.BlockSpec(memory_space=pltpu.VMEM)


def angle_tables(steps, stride, period, orders):
    phases = (np.arange(steps)[:, None] * stride * np.arange(orders)[None, :]) % period
    angles = phases * (2.0 * np.pi / period)
    return np.stack([np.cos(angles), np.sin(angles)]).astype(np.float32)


def inner_table(coarse_ref, fine_ref, table_ref, lanes):
    fine_cos, fine_sin = fine_ref[0, :, lanes], fine_ref[1, :, lanes]
    for step in range(FINE):
        rows = slice(step * FINE, (step + 1) * FINE)
        coarse_cos = coarse_ref[0, step : step + 1, lanes]
        coarse_sin = coarse_ref[1, step : step + 1, lanes]
        cosine = coarse_cos * fine_cos - coarse_sin * fine_sin
        sine = coarse_sin * fine_cos + coarse_cos * fine_sin
        table_ref[0, rows, lanes] = cosine.astype(jnp.bfloat16)
        table_ref[1, rows, lanes] = (-sine).astype(jnp.bfloat16)


def shift(values, amount):
    amount %= LANES
    return values if amount == 0 else pltpu.roll(values, amount, values.ndim - 1)


def side_by_side(pieces, width):
    lane = lax.broadcasted_iota(jnp.int32, pieces[0].shape, pieces[0].ndim - 1)
    joined = jnp.zeros_like(pieces[0])
    for index, piece in reversed(list(enumerate(pieces))):
        joined = jnp.where(lane < (index + 1) * width, shift(piece, index * width), joined)
    return jnp.where(lane < len(pieces) * width, joined, 0.0)


def forward_kernel(
    peers,
    elevation_ref,
    weight_ref,
    coarse_ref,
    fine_ref,
    turn_ref,
    out_ref,
    rows_ref,
    table_ref,
    flip_ref,
    pack_ref,
):
    cycles = elevation_ref.shape[0]
    turns = turn_ref.shape[1]
    orders = flip_ref.shape[1]
    for turn in range(turns):
        rows_ref[turn * cycles : (turn + 1) * cycles, :] = elevation_ref[
            :, turn * INNER : (turn + 1) * INNER
        ]
    weight = weight_ref[...]
    inner_table(coarse_ref, fine_ref, table_ref, slice(None))
    for part in range(orders // INNER):
        lanes = slice(part * INNER, (part + 1) * INNER)
        even = jnp.dot(rows_ref[...], table_ref[0, :, lanes], preferred_element_type=jnp.float32)
        odd = jnp.dot(rows_ref[...], table_ref[1, :, lanes], preferred_element_type=jnp.float32)
        first = second = None
        for turn in range(turns):
            rows = slice(turn * cycles, (turn + 1) * cycles)
            cosine, sine = turn_ref[0, turn : turn + 1, lanes], turn_ref[1, turn : turn + 1, lanes]
            one = even[rows] * cosine + odd[rows] * sine
            two = odd[rows] * cosine - even[rows] * sine
            first = one if first is None else first + one
            second = two if second is None else second + two
        flip_ref[0, lanes, :cycles] = jnp.transpose(first) * weight
        flip_ref[1, lanes, :cycles] = jnp.transpose(second) * weight

    beside = LANES // cycles
    deep = out_ref.shape[0] // peers
    share = orders // peers
    for row in range(deep):
        pieces = []
        for column in range(beside):
            which, order = divmod(deep * column + row, share)
            pieces.append(flip_ref[which, pl.ds(order, peers, stride=share), :])
        pack_ref[pl.ds(row, peers, stride=deep), :] = side_by_side(pieces, cycles)
    out_ref[...] = pack_ref[...].astype(jnp.bfloat16)


def forward(elevation, weight, coarse, fine, turn, lines, peers):
    cycles, longitudes = elevation.shape
    orders = coarse.shape[2]
    turns = longitudes // INNER
    return pl.pallas_call(
        functools.partial(forward_kernel, peers),
        in_specs=[NEARBY] * 5,
        out_specs=NEARBY,
        out_shape=jax.ShapeDtypeStruct((lines, LANES), jnp.bfloat16),
        scratch_shapes=[
            pltpu.VMEM((turns * cycles, INNER), jnp.bfloat16),
            pltpu.VMEM((2, INNER, orders), jnp.bfloat16),
            pltpu.VMEM((2, orders, LANES), jnp.float32),
            pltpu.VMEM((lines, LANES), jnp.float32),
        ],
        cost_estimate=pl.CostEstimate(
            flops=4 * cycles * longitudes * orders, bytes_accessed=1 << 20, transcendentals=0
        ),
        name="forward_dft",
    )(elevation, weight, coarse, fine, turn)


def split_kernel(place_ref, legendre_ref, sent_ref, own_ref):
    core = place_ref[0]
    orders = own_ref.shape[0]
    for target, index in ((sent_ref, 1 - core), (own_ref, core)):
        for first in range(0, orders, TILE):
            start = pl.multiple_of(index * orders + first, TILE)
            target[first : first + TILE] = jnp.swapaxes(
                legendre_ref[:, pl.ds(start, TILE), :], 0, 1
            )


def part_kernel(place_ref, half_ref, part_ref):
    share = part_ref.shape[0]
    part_ref[...] = half_ref[pl.ds((1 - place_ref[1]) * share, share)]


def divided(kernel, place, values, orders, cycles):
    degrees = values.shape[2]
    return pl.pallas_call(
        kernel,
        in_specs=[SCALARS, NEARBY],
        out_specs=[NEARBY] * len(orders),
        out_shape=[
            jax.ShapeDtypeStruct((count, cycles, degrees), values.dtype) for count in orders
        ],
        cost_estimate=pl.CostEstimate(
            flops=1 << 20, bytes_accessed=4 * cycles * sum(orders) * degrees, transcendentals=0
        ),
        compiler_params=pltpu.CompilerParams(vmem_limit_bytes=ROOM),
    )(place, values)


def table_kernel(which, coarse_ref, fine_ref, table_ref):
    fine_cos, fine_sin = fine_ref[0], fine_ref[1]
    for step in range(FINE):
        coarse_cos = coarse_ref[0, step : step + 1, :]
        coarse_sin = coarse_ref[1, step : step + 1, :]
        if which == "cosine":
            part = coarse_cos * fine_cos - coarse_sin * fine_sin
        else:
            part = -(coarse_sin * fine_cos + coarse_cos * fine_sin)
        table_ref[step * FINE : (step + 1) * FINE, :] = part.astype(jnp.bfloat16)


def table_of(which, coarse, fine):
    shape = (INNER, coarse.shape[2])
    return pl.pallas_call(
        functools.partial(table_kernel, which),
        in_specs=[NEARBY] * 2,
        out_specs=NEARBY,
        out_shape=jax.ShapeDtypeStruct(shape, jnp.bfloat16),
        cost_estimate=pl.CostEstimate(
            flops=1 << 20, bytes_accessed=2 * math.prod(shape), transcendentals=0
        ),
        compiler_params=pltpu.CompilerParams(vmem_limit_bytes=ROOM),
    )(coarse, fine)


def analysis_kernel(near, spot_ref, *refs):
    assignment_ref, moved_ref, *value_refs = refs[: near + 2]
    out_ref, row_ref, left_ref, joined_ref = refs[near + 2 :]
    share, _, two_fields, _ = left_ref.shape
    fields = two_fields // 2
    cycles = value_refs[0].shape[1]
    beside = LANES // cycles
    lines = moved_ref.shape[0]
    block = lines // fields
    deep = block // near
    spot = spot_ref[0]

    for slot in range(fields):
        source = pl.multiple_of(assignment_ref[slot] * block, block)
        row_ref[slot * block : (slot + 1) * block, :] = moved_ref[
            pl.ds(source, block), :
        ].astype(jnp.float32)
    for other in range(near):
        peer = jnp.bitwise_xor(spot, other)
        for row in range(deep):
            taken = row_ref[pl.ds(peer * deep + row, fields, stride=block), :]
            for column in range(beside):
                which, order = divmod(deep * column + row, share)
                left_ref[order, other, which * fields : (which + 1) * fields, :] = shift(
                    taken, -column * cycles
                ).astype(jnp.bfloat16)

    for order in range(share):
        for other in range(near):
            joined_ref[order % 2, other * cycles : (other + 1) * cycles, :] = value_refs[other][
                order
            ]
        left = jnp.concatenate(
            [left_ref[order, other][:, :cycles] for other in range(near)], axis=1
        )
        out_ref[2 * fields * order : 2 * fields * (order + 1), :] = jnp.dot(
            left, joined_ref[order % 2], preferred_element_type=jnp.float32
        ).astype(jnp.bfloat16)


def analyse(spot, assignment, moved, values):
    share, cycles, degrees = values[0].shape
    fields = assignment.shape[0]
    return pl.pallas_call(
        functools.partial(analysis_kernel, len(values)),
        in_specs=[SCALARS] * 2 + [NEARBY] * (1 + len(values)),
        out_specs=NEARBY,
        scratch_shapes=[
            pltpu.VMEM(moved.shape, jnp.float32),
            pltpu.VMEM((share, len(values), 2 * fields, LANES), jnp.bfloat16),
            pltpu.VMEM((2, len(values) * cycles, degrees), jnp.bfloat16),
        ],
        out_shape=jax.ShapeDtypeStruct((share * 2 * fields, degrees), jnp.bfloat16),
        cost_estimate=pl.CostEstimate(
            flops=4 * fields * share * cycles * degrees * len(values),
            bytes_accessed=4 << 20,
            transcendentals=0,
        ),
        compiler_params=pltpu.CompilerParams(vmem_limit_bytes=ROOM),
        name="analysis",
    )(spot, assignment, moved, *values)


def synthesis_kernel(near, spot_ref, first_ref, *refs):
    coefficient_ref, *value_refs = refs[: near + 1]
    out_ref, right_ref, row_ref, joined_ref = refs[near + 1 :]
    share, _, two_fields, _ = right_ref.shape
    fields = two_fields // 2
    cycles = value_refs[0].shape[1]
    beside = LANES // cycles
    lines = out_ref.shape[0]
    block = lines // fields
    deep = block // near
    dims = (((1,), (1,)), ((), ()))
    for order in range(share):
        factor = jnp.where(first_ref[0] + order == 0, 1.0, 2.0).astype(jnp.float32)
        for other in range(near):
            skip = 0 if value_refs[other].shape[0] == share else share * (spot_ref[0] % 2)
            joined_ref[order % 2, other * cycles : (other + 1) * cycles, :] = value_refs[other][
                skip + order
            ]
        product = factor * lax.dot_general(
            coefficient_ref[2 * fields * order : 2 * fields * (order + 1), :],
            joined_ref[order % 2],
            dims,
            preferred_element_type=jnp.float32,
        )
        for other in range(near):
            right_ref[order, other, :, :cycles] = product[
                :, other * cycles : (other + 1) * cycles
            ]
    for other in range(near):
        peer = jnp.bitwise_xor(spot_ref[0], other)
        for row in range(deep):
            pieces = []
            for column in range(beside):
                which, own = divmod(deep * column + row, share)
                pieces.append(right_ref[own, other, which * fields : (which + 1) * fields, :])
            row_ref[pl.ds(peer * deep + row, fields, stride=block), :] = side_by_side(
                pieces, cycles
            )
    out_ref[...] = row_ref[...].astype(jnp.bfloat16)


def synthesise(spot, first, coefficients, values, lines):
    share = min(value.shape[0] for value in values)
    _, cycles, degrees = values[0].shape
    fields = coefficients.shape[0] // (2 * share)
    return pl.pallas_call(
        functools.partial(synthesis_kernel, len(values)),
        in_specs=[SCALARS] * 2 + [NEARBY] * (1 + len(values)),
        out_specs=NEARBY,
        scratch_shapes=[
            pltpu.VMEM((share, len(values), 2 * fields, LANES), jnp.float32),
            pltpu.VMEM((lines, LANES), jnp.float32),
            pltpu.VMEM((2, len(values) * cycles, degrees), jnp.bfloat16),
        ],
        out_shape=jax.ShapeDtypeStruct((lines, LANES), jnp.bfloat16),
        cost_estimate=pl.CostEstimate(
            flops=4 * fields * share * cycles * degrees * len(values),
            bytes_accessed=4 << 20,
            transcendentals=0,
        ),
        compiler_params=pltpu.CompilerParams(vmem_limit_bytes=ROOM),
        name="synthesis",
    )(spot, first, coefficients, *values)


def inverse_kernel(
    peers,
    moved_ref,
    cosine_ref,
    sine_ref,
    turn_ref,
    out_ref,
    rows_ref,
    row_ref,
    flip_ref,
    part_ref,
    sems,
):
    parts, cycles, span = part_ref.shape
    count = span // INNER
    orders = flip_ref.shape[1]
    row_ref[...] = moved_ref[...].astype(jnp.float32)
    deep = moved_ref.shape[0] // peers
    share = orders // peers
    for row in range(deep):
        taken = row_ref[pl.ds(row, peers, stride=deep), :]
        for column in range(LANES // cycles):
            which, order = divmod(deep * column + row, share)
            flip_ref[which, pl.ds(order, peers, stride=share), :] = shift(
                taken, -column * cycles
            )
    first = jnp.transpose(flip_ref[0])[:cycles]
    second = jnp.transpose(flip_ref[1])[:cycles]
    dims = (((1,), (1,)), ((), ()))
    copies = []
    for part in range(parts):
        for step in range(count):
            rows = slice(step * cycles, (step + 1) * cycles)
            turn = part * count + step
            cosine, sine = turn_ref[0, turn : turn + 1, :], turn_ref[1, turn : turn + 1, :]
            rows_ref[part % 2, 0, rows, :] = (first * cosine - second * sine).astype(jnp.bfloat16)
            rows_ref[part % 2, 1, rows, :] = (first * sine + second * cosine).astype(jnp.bfloat16)
        result = lax.dot_general(
            rows_ref[part % 2, 0], cosine_ref[...], dims, preferred_element_type=jnp.float32
        ) + lax.dot_general(
            rows_ref[part % 2, 1], sine_ref[...], dims, preferred_element_type=jnp.float32
        )
        for step in range(count):
            part_ref[part, :, step * INNER : (step + 1) * INNER] = result[
                step * cycles : (step + 1) * cycles
            ]
        copy = pltpu.make_async_copy(
            part_ref.at[part], out_ref.at[:, part * span : (part + 1) * span], sems.at[part]
        )
        copy.start()
        copies.append(copy)
    for copy in copies:
        copy.wait()


def inverse(moved, tables, turn, cycles, longitudes, peers):
    orders = turn.shape[2]
    count = 6
    parts = longitudes // INNER // count
    return pl.pallas_call(
        functools.partial(inverse_kernel, peers),
        in_specs=[NEARBY] * 4,
        out_specs=pl.BlockSpec(memory_space=pltpu.HBM),
        out_shape=jax.ShapeDtypeStruct((cycles, longitudes), jnp.float32),
        scratch_shapes=[
            pltpu.VMEM((2, 2, count * cycles, orders), jnp.bfloat16),
            pltpu.VMEM(moved.shape, jnp.float32),
            pltpu.VMEM((2, orders, LANES), jnp.float32),
            pltpu.VMEM((parts, cycles, count * INNER), jnp.float32),
            pltpu.SemaphoreType.DMA((parts,)),
        ],
        cost_estimate=pl.CostEstimate(
            flops=4 * cycles * longitudes * orders, bytes_accessed=1 << 20, transcendentals=0
        ),
        compiler_params=pltpu.CompilerParams(vmem_limit_bytes=ROOM),
        name="inverse_dft",
    )(moved, *tables, turn)


def local(elevation, legendre, cycle_weight, love_factor, assignment):
    _, cycle_dev, longitudes = elevation.shape
    orders_dev, degrees = legendre.shape[1:]
    groups = lax.axis_size("cons")
    cores, near = lax.axis_size(CORE), lax.axis_size(NEAR)
    deep, far = lax.axis_size(DEEP), lax.axis_size(FAR)
    orders = orders_dev * groups
    spot, core = lax.axis_index(NEAR), lax.axis_index(CORE)
    side = lax.axis_index("blk_0")
    coarse = jnp.asarray(angle_tables(FINE, FINE, longitudes, orders))
    fine = jnp.asarray(angle_tables(FINE, 1, longitudes, orders))
    turn = jnp.asarray(angle_tables(longitudes // INNER, INNER, longitudes, orders))

    def swapped(values, other):
        pairs = [(index, index ^ other) for index in range(near)]
        return lax.ppermute(values, NEAR[::-1], pairs)

    half, share = orders_dev // cores, orders_dev // near
    place = jnp.stack([core, side]).astype(jnp.int32)

    def exchanged(packed, axes):
        peers = lax.axis_size(axes)
        tiles = packed.reshape(peers, -1, LANES)
        tiles = lax.all_to_all(tiles, axes, 0, 0, tiled=True)
        return tiles.reshape(-1, LANES)

    sent, own = divided(split_kernel, place, legendre, (half, half), cycle_dev)

    def part_of(values):
        return divided(part_kernel, place, values, (share,), cycle_dev)[0]

    met = swapped(sent, 1)
    own_side = swapped(part_of(own), 2)
    met_side = swapped(part_of(sent), 3)
    tables = [table_of(which, coarse, fine) for which in ("cosine", "sine")]
    lines = groups * orders_dev * 2 // (LANES // cycle_dev)
    packed = forward(elevation[0], cycle_weight[None, :], coarse, fine, turn, lines, groups * cores)
    moved = exchanged(packed, ("cons", CORE))
    partial = analyse(core[None].astype(jnp.int32), assignment, moved, [own, met])
    rows = partial.shape[0] // far
    arrived = lax.all_to_all(partial.reshape(far, rows, degrees), FAR, 0, 0, tiled=True)
    analysis = jnp.sum(arrived.astype(jnp.float32), axis=0)
    scaled = (analysis * love_factor[None, :]).astype(jnp.bfloat16)
    copies = jnp.broadcast_to(scaled[None], (deep, rows, degrees))
    coefficients = lax.all_to_all(copies, DEEP, 0, 0, tiled=True)
    first = ((lax.axis_index("cons") * near + spot) * share)[None].astype(jnp.int32)
    synthesis = synthesise(
        spot[None].astype(jnp.int32),
        first,
        coefficients.reshape(-1, degrees),
        [own, own_side, met, met_side],
        lines,
    )
    returned = exchanged(synthesis, ("cons", *NEAR))
    return inverse(returned, tables, turn, cycle_dev, longitudes, groups * near)[None]


def solution(mesh):
    torus = Mesh(
        mesh.devices.reshape(mesh.shape["cons"], 2, 8, 2), ("cons", *BLK)
    )
    placed = (P("cons", BLK, None), P(BLK, "cons", None), P(BLK), P(), P())
    return jax.shard_map(
        local, mesh=torus, in_specs=placed, out_specs=P("cons", BLK, None), check_vma=False
    )
```

```python
import functools
import math

import jax
import jax.numpy as jnp
import numpy as np
from jax import lax
from jax.experimental import pallas as pl
from jax.experimental.pallas import tpu as pltpu
from jax.sharding import Mesh
from jax.sharding import PartitionSpec as P

BLK = ("blk_0", "blk_1", "blk_2")
NEAR = ("blk_2", "blk_0")
CORE = "blk_2"
DEEP = "blk_1"
FAR = ("blk_0", "blk_1")
FINE = 16
INNER = FINE * FINE
LANES = 128
TILE = 8
ROOM = 24 << 20
SCALARS = pl.BlockSpec(memory_space=pltpu.SMEM)
NEARBY = pl.BlockSpec(memory_space=pltpu.VMEM)


def angle_tables(steps, stride, period, orders):
    phases = (np.arange(steps)[:, None] * stride * np.arange(orders)[None, :]) % period
    angles = phases * (2.0 * np.pi / period)
    return np.stack([np.cos(angles), np.sin(angles)]).astype(np.float32)


def inner_table(coarse_ref, fine_ref, table_ref, lanes):
    fine_cos, fine_sin = fine_ref[0, :, lanes], fine_ref[1, :, lanes]
    for step in range(FINE):
        rows = slice(step * FINE, (step + 1) * FINE)
        coarse_cos = coarse_ref[0, step : step + 1, lanes]
        coarse_sin = coarse_ref[1, step : step + 1, lanes]
        cosine = coarse_cos * fine_cos - coarse_sin * fine_sin
        sine = coarse_sin * fine_cos + coarse_cos * fine_sin
        table_ref[0, rows, lanes] = cosine.astype(jnp.bfloat16)
        table_ref[1, rows, lanes] = (-sine).astype(jnp.bfloat16)


def shift(values, amount):
    amount %= LANES
    return values if amount == 0 else pltpu.roll(values, amount, values.ndim - 1)


def side_by_side(pieces, width):
    lane = lax.broadcasted_iota(jnp.int32, pieces[0].shape, pieces[0].ndim - 1)
    joined = jnp.zeros_like(pieces[0])
    for index, piece in reversed(list(enumerate(pieces))):
        joined = jnp.where(lane < (index + 1) * width, shift(piece, index * width), joined)
    return jnp.where(lane < len(pieces) * width, joined, 0.0)


def forward_kernel(
    peers,
    elevation_ref,
    weight_ref,
    coarse_ref,
    fine_ref,
    turn_ref,
    out_ref,
    rows_ref,
    table_ref,
    flip_ref,
    pack_ref,
):
    cycles = elevation_ref.shape[0]
    turns = turn_ref.shape[1]
    orders = flip_ref.shape[1]
    for turn in range(turns):
        rows_ref[turn * cycles : (turn + 1) * cycles, :] = elevation_ref[
            :, turn * INNER : (turn + 1) * INNER
        ]
    weight = weight_ref[...]
    inner_table(coarse_ref, fine_ref, table_ref, slice(None))
    for part in range(orders // INNER):
        lanes = slice(part * INNER, (part + 1) * INNER)
        even = jnp.dot(rows_ref[...], table_ref[0, :, lanes], preferred_element_type=jnp.float32)
        odd = jnp.dot(rows_ref[...], table_ref[1, :, lanes], preferred_element_type=jnp.float32)
        first = second = None
        for turn in range(turns):
            rows = slice(turn * cycles, (turn + 1) * cycles)
            cosine, sine = turn_ref[0, turn : turn + 1, lanes], turn_ref[1, turn : turn + 1, lanes]
            one = even[rows] * cosine + odd[rows] * sine
            two = odd[rows] * cosine - even[rows] * sine
            first = one if first is None else first + one
            second = two if second is None else second + two
        flip_ref[0, lanes, :cycles] = jnp.transpose(first) * weight
        flip_ref[1, lanes, :cycles] = jnp.transpose(second) * weight

    beside = LANES // cycles
    deep = out_ref.shape[0] // peers
    share = orders // peers
    for row in range(deep):
        pieces = []
        for column in range(beside):
            which, order = divmod(deep * column + row, share)
            pieces.append(flip_ref[which, pl.ds(order, peers, stride=share), :])
        pack_ref[pl.ds(row, peers, stride=deep), :] = side_by_side(pieces, cycles)
    out_ref[...] = pack_ref[...].astype(jnp.bfloat16)


def forward(elevation, weight, coarse, fine, turn, lines, peers):
    cycles, longitudes = elevation.shape
    orders = coarse.shape[2]
    turns = longitudes // INNER
    return pl.pallas_call(
        functools.partial(forward_kernel, peers),
        in_specs=[NEARBY] * 5,
        out_specs=NEARBY,
        out_shape=jax.ShapeDtypeStruct((lines, LANES), jnp.bfloat16),
        scratch_shapes=[
            pltpu.VMEM((turns * cycles, INNER), jnp.bfloat16),
            pltpu.VMEM((2, INNER, orders), jnp.bfloat16),
            pltpu.VMEM((2, orders, LANES), jnp.float32),
            pltpu.VMEM((lines, LANES), jnp.float32),
        ],
        cost_estimate=pl.CostEstimate(
            flops=4 * cycles * longitudes * orders, bytes_accessed=1 << 20, transcendentals=0
        ),
        name="forward_dft",
    )(elevation, weight, coarse, fine, turn)


def split_kernel(flip, place_ref, legendre_ref, half_ref):
    orders = half_ref.shape[0]
    index = jnp.bitwise_xor(place_ref[0], flip)
    for first in range(0, orders, TILE):
        start = pl.multiple_of(index * orders + first, TILE)
        half_ref[first : first + TILE] = jnp.swapaxes(
            legendre_ref[:, pl.ds(start, TILE), :], 0, 1
        )


def divided(kernel, place, values, orders, cycles):
    degrees = values.shape[2]
    return pl.pallas_call(
        kernel,
        in_specs=[SCALARS, NEARBY],
        out_specs=[NEARBY] * len(orders),
        out_shape=[
            jax.ShapeDtypeStruct((count, cycles, degrees), values.dtype) for count in orders
        ],
        cost_estimate=pl.CostEstimate(
            flops=1 << 20, bytes_accessed=4 * cycles * sum(orders) * degrees, transcendentals=0
        ),
        compiler_params=pltpu.CompilerParams(vmem_limit_bytes=ROOM),
    )(place, values)


def table_kernel(which, coarse_ref, fine_ref, table_ref):
    fine_cos, fine_sin = fine_ref[0], fine_ref[1]
    for step in range(FINE):
        coarse_cos = coarse_ref[0, step : step + 1, :]
        coarse_sin = coarse_ref[1, step : step + 1, :]
        if which == "cosine":
            part = coarse_cos * fine_cos - coarse_sin * fine_sin
        else:
            part = -(coarse_sin * fine_cos + coarse_cos * fine_sin)
        table_ref[step * FINE : (step + 1) * FINE, :] = part.astype(jnp.bfloat16)


def table_of(which, coarse, fine):
    shape = (INNER, coarse.shape[2])
    return pl.pallas_call(
        functools.partial(table_kernel, which),
        in_specs=[NEARBY] * 2,
        out_specs=NEARBY,
        out_shape=jax.ShapeDtypeStruct(shape, jnp.bfloat16),
        cost_estimate=pl.CostEstimate(
            flops=1 << 20, bytes_accessed=2 * math.prod(shape), transcendentals=0
        ),
        compiler_params=pltpu.CompilerParams(vmem_limit_bytes=ROOM),
    )(coarse, fine)


def analysis_kernel(near, spot_ref, *refs):
    assignment_ref, moved_ref, *value_refs = refs[: near + 2]
    out_ref, row_ref, left_ref, joined_ref = refs[near + 2 :]
    share, _, two_fields, _ = left_ref.shape
    fields = two_fields // 2
    cycles = value_refs[0].shape[1]
    beside = LANES // cycles
    lines = moved_ref.shape[0]
    block = lines // fields
    deep = block // near
    spot = spot_ref[0]

    for slot in range(fields):
        source = pl.multiple_of(assignment_ref[slot] * block, block)
        row_ref[slot * block : (slot + 1) * block, :] = moved_ref[
            pl.ds(source, block), :
        ].astype(jnp.float32)
    for other in range(near):
        peer = jnp.bitwise_xor(spot, other)
        for row in range(deep):
            taken = row_ref[pl.ds(peer * deep + row, fields, stride=block), :]
            for column in range(beside):
                which, order = divmod(deep * column + row, share)
                left_ref[order, other, which * fields : (which + 1) * fields, :] = shift(
                    taken, -column * cycles
                ).astype(jnp.bfloat16)

    for order in range(share):
        for other in range(near):
            joined_ref[order % 2, other * cycles : (other + 1) * cycles, :] = value_refs[other][
                order
            ]
        left = jnp.concatenate(
            [left_ref[order, other][:, :cycles] for other in range(near)], axis=1
        )
        out_ref[2 * fields * order : 2 * fields * (order + 1), :] = jnp.dot(
            left, joined_ref[order % 2], preferred_element_type=jnp.float32
        ).astype(jnp.bfloat16)


def analyse(spot, assignment, moved, values):
    share, cycles, degrees = values[0].shape
    fields = assignment.shape[0]
    return pl.pallas_call(
        functools.partial(analysis_kernel, len(values)),
        in_specs=[SCALARS] * 2 + [NEARBY] * (1 + len(values)),
        out_specs=NEARBY,
        scratch_shapes=[
            pltpu.VMEM(moved.shape, jnp.float32),
            pltpu.VMEM((share, len(values), 2 * fields, LANES), jnp.bfloat16),
            pltpu.VMEM((2, len(values) * cycles, degrees), jnp.bfloat16),
        ],
        out_shape=jax.ShapeDtypeStruct((share * 2 * fields, degrees), jnp.bfloat16),
        cost_estimate=pl.CostEstimate(
            flops=4 * fields * share * cycles * degrees * len(values),
            bytes_accessed=4 << 20,
            transcendentals=0,
        ),
        compiler_params=pltpu.CompilerParams(vmem_limit_bytes=ROOM),
        name="analysis",
    )(spot, assignment, moved, *values)


def synthesis_kernel(near, spot_ref, first_ref, *refs):
    coefficient_ref, *value_refs = refs[: near + 1]
    out_ref, right_ref, row_ref, joined_ref = refs[near + 1 :]
    share, _, two_fields, _ = right_ref.shape
    fields = two_fields // 2
    cycles = value_refs[0].shape[1]
    beside = LANES // cycles
    lines = out_ref.shape[0]
    block = lines // fields
    deep = block // near
    dims = (((1,), (1,)), ((), ()))
    for order in range(share):
        factor = jnp.where(first_ref[0] + order == 0, 1.0, 2.0).astype(jnp.float32)
        for other in range(near):
            skip = 0 if value_refs[other].shape[0] == share else share * (spot_ref[0] % 2)
            joined_ref[order % 2, other * cycles : (other + 1) * cycles, :] = value_refs[other][
                skip + order
            ]
        product = factor * lax.dot_general(
            coefficient_ref[2 * fields * order : 2 * fields * (order + 1), :],
            joined_ref[order % 2],
            dims,
            preferred_element_type=jnp.float32,
        )
        for other in range(near):
            right_ref[order, other, :, :cycles] = product[
                :, other * cycles : (other + 1) * cycles
            ]
    for other in range(near):
        peer = jnp.bitwise_xor(spot_ref[0], other)
        for row in range(deep):
            pieces = []
            for column in range(beside):
                which, own = divmod(deep * column + row, share)
                pieces.append(right_ref[own, other, which * fields : (which + 1) * fields, :])
            row_ref[pl.ds(peer * deep + row, fields, stride=block), :] = side_by_side(
                pieces, cycles
            )
    out_ref[...] = row_ref[...].astype(jnp.bfloat16)


def synthesise(spot, first, coefficients, values, lines):
    share = min(value.shape[0] for value in values)
    _, cycles, degrees = values[0].shape
    fields = coefficients.shape[0] // (2 * share)
    return pl.pallas_call(
        functools.partial(synthesis_kernel, len(values)),
        in_specs=[SCALARS] * 2 + [NEARBY] * (1 + len(values)),
        out_specs=NEARBY,
        scratch_shapes=[
            pltpu.VMEM((share, len(values), 2 * fields, LANES), jnp.float32),
            pltpu.VMEM((lines, LANES), jnp.float32),
            pltpu.VMEM((2, len(values) * cycles, degrees), jnp.bfloat16),
        ],
        out_shape=jax.ShapeDtypeStruct((lines, LANES), jnp.bfloat16),
        cost_estimate=pl.CostEstimate(
            flops=4 * fields * share * cycles * degrees * len(values),
            bytes_accessed=4 << 20,
            transcendentals=0,
        ),
        compiler_params=pltpu.CompilerParams(vmem_limit_bytes=ROOM),
        name="synthesis",
    )(spot, first, coefficients, *values)


def inverse_kernel(
    peers,
    moved_ref,
    cosine_ref,
    sine_ref,
    turn_ref,
    out_ref,
    rows_ref,
    row_ref,
    flip_ref,
    part_ref,
    sems,
):
    parts, cycles, span = part_ref.shape
    count = span // INNER
    orders = flip_ref.shape[1]
    row_ref[...] = moved_ref[...].astype(jnp.float32)
    deep = moved_ref.shape[0] // peers
    share = orders // peers
    for row in range(deep):
        taken = row_ref[pl.ds(row, peers, stride=deep), :]
        for column in range(LANES // cycles):
            which, order = divmod(deep * column + row, share)
            flip_ref[which, pl.ds(order, peers, stride=share), :] = shift(
                taken, -column * cycles
            )
    first = jnp.transpose(flip_ref[0])[:cycles]
    second = jnp.transpose(flip_ref[1])[:cycles]
    dims = (((1,), (1,)), ((), ()))
    copies = []
    for part in range(parts):
        for step in range(count):
            rows = slice(step * cycles, (step + 1) * cycles)
            turn = part * count + step
            cosine, sine = turn_ref[0, turn : turn + 1, :], turn_ref[1, turn : turn + 1, :]
            rows_ref[part % 2, 0, rows, :] = (first * cosine - second * sine).astype(jnp.bfloat16)
            rows_ref[part % 2, 1, rows, :] = (first * sine + second * cosine).astype(jnp.bfloat16)
        result = lax.dot_general(
            rows_ref[part % 2, 0], cosine_ref[...], dims, preferred_element_type=jnp.float32
        ) + lax.dot_general(
            rows_ref[part % 2, 1], sine_ref[...], dims, preferred_element_type=jnp.float32
        )
        for step in range(count):
            part_ref[part, :, step * INNER : (step + 1) * INNER] = result[
                step * cycles : (step + 1) * cycles
            ]
        copy = pltpu.make_async_copy(
            part_ref.at[part], out_ref.at[:, part * span : (part + 1) * span], sems.at[part]
        )
        copy.start()
        copies.append(copy)
    for copy in copies:
        copy.wait()


def inverse(moved, tables, turn, cycles, longitudes, peers):
    orders = turn.shape[2]
    count = 6
    parts = longitudes // INNER // count
    return pl.pallas_call(
        functools.partial(inverse_kernel, peers),
        in_specs=[NEARBY] * 4,
        out_specs=pl.BlockSpec(memory_space=pltpu.HBM),
        out_shape=jax.ShapeDtypeStruct((cycles, longitudes), jnp.float32),
        scratch_shapes=[
            pltpu.VMEM((2, 2, count * cycles, orders), jnp.bfloat16),
            pltpu.VMEM(moved.shape, jnp.float32),
            pltpu.VMEM((2, orders, LANES), jnp.float32),
            pltpu.VMEM((parts, cycles, count * INNER), jnp.float32),
            pltpu.SemaphoreType.DMA((parts,)),
        ],
        cost_estimate=pl.CostEstimate(
            flops=4 * cycles * longitudes * orders, bytes_accessed=1 << 20, transcendentals=0
        ),
        compiler_params=pltpu.CompilerParams(vmem_limit_bytes=ROOM),
        name="inverse_dft",
    )(moved, *tables, turn)


def local(elevation, legendre, cycle_weight, love_factor, assignment):
    _, cycle_dev, longitudes = elevation.shape
    orders_dev, degrees = legendre.shape[1:]
    groups = lax.axis_size("cons")
    cores, near = lax.axis_size(CORE), lax.axis_size(NEAR)
    deep, far = lax.axis_size(DEEP), lax.axis_size(FAR)
    orders = orders_dev * groups
    spot, core = lax.axis_index(NEAR), lax.axis_index(CORE)
    side = lax.axis_index("blk_0")
    coarse = jnp.asarray(angle_tables(FINE, FINE, longitudes, orders))
    fine = jnp.asarray(angle_tables(FINE, 1, longitudes, orders))
    turn = jnp.asarray(angle_tables(longitudes // INNER, INNER, longitudes, orders))

    def swapped(values, other):
        pairs = [(index, index ^ other) for index in range(near)]
        return lax.ppermute(values, NEAR[::-1], pairs)

    half, share = orders_dev // cores, orders_dev // near
    place = jnp.stack([core, side]).astype(jnp.int32)

    def exchanged(packed, axes):
        peers = lax.axis_size(axes)
        tiles = packed.reshape(peers, -1, LANES)
        tiles = lax.all_to_all(tiles, axes, 0, 0, tiled=True)
        return tiles.reshape(-1, LANES)

    def half_of(flip):
        kernel = functools.partial(split_kernel, flip)
        return divided(kernel, place, legendre, (half,), cycle_dev)[0]

    sent, own = half_of(1), half_of(0)

    def part_of(values):
        return lax.dynamic_slice_in_dim(values, (1 - side) * share, share, 0)

    met = swapped(sent, 1)
    own_side = swapped(part_of(own), 2)
    met_side = swapped(part_of(sent), 3)
    tables = [table_of(which, coarse, fine) for which in ("cosine", "sine")]
    lines = groups * orders_dev * 2 // (LANES // cycle_dev)
    packed = forward(elevation[0], cycle_weight[None, :], coarse, fine, turn, lines, groups * cores)
    moved = exchanged(packed, ("cons", CORE))
    partial = analyse(core[None].astype(jnp.int32), assignment, moved, [own, met])
    rows = partial.shape[0] // far
    arrived = lax.all_to_all(partial.reshape(far, rows, degrees), FAR, 0, 0, tiled=True)
    analysis = jnp.sum(arrived.astype(jnp.float32), axis=0)
    scaled = (analysis * love_factor[None, :]).astype(jnp.bfloat16)
    copies = jnp.broadcast_to(scaled[None], (deep, rows, degrees))
    coefficients = lax.all_to_all(copies, DEEP, 0, 0, tiled=True)
    first = ((lax.axis_index("cons") * near + spot) * share)[None].astype(jnp.int32)
    synthesis = synthesise(
        spot[None].astype(jnp.int32),
        first,
        coefficients.reshape(-1, degrees),
        [own, own_side, met, met_side],
        lines,
    )
    returned = exchanged(synthesis, ("cons", *NEAR))
    return inverse(returned, tables, turn, cycle_dev, longitudes, groups * near)[None]


def solution(mesh):
    torus = Mesh(
        mesh.devices.reshape(mesh.shape["cons"], 2, 8, 2), ("cons", *BLK)
    )
    placed = (P("cons", BLK, None), P(BLK, "cons", None), P(BLK), P(), P())
    return jax.shard_map(
        local, mesh=torus, in_specs=placed, out_specs=P("cons", BLK, None), check_vma=False
    )
```

```python
import functools
import math

import jax
import jax.numpy as jnp
import numpy as np
from jax import lax
from jax.experimental import pallas as pl
from jax.experimental.pallas import tpu as pltpu
from jax.sharding import Mesh
from jax.sharding import PartitionSpec as P

BLK = ("blk_0", "blk_1", "blk_2")
NEAR = ("blk_2", "blk_0")
CORE = "blk_2"
DEEP = "blk_1"
FAR = ("blk_0", "blk_1")
FINE = 16
INNER = FINE * FINE
LANES = 128
TILE = 8
ROOM = 24 << 20
SCALARS = pl.BlockSpec(memory_space=pltpu.SMEM)
NEARBY = pl.BlockSpec(memory_space=pltpu.VMEM)


def angle_tables(steps, stride, period, orders):
    phases = (np.arange(steps)[:, None] * stride * np.arange(orders)[None, :]) % period
    angles = phases * (2.0 * np.pi / period)
    return np.stack([np.cos(angles), np.sin(angles)]).astype(np.float32)


def inner_table(coarse_ref, fine_ref, table_ref, lanes):
    fine_cos, fine_sin = fine_ref[0, :, lanes], fine_ref[1, :, lanes]
    for step in range(FINE):
        rows = slice(step * FINE, (step + 1) * FINE)
        coarse_cos = coarse_ref[0, step : step + 1, lanes]
        coarse_sin = coarse_ref[1, step : step + 1, lanes]
        cosine = coarse_cos * fine_cos - coarse_sin * fine_sin
        sine = coarse_sin * fine_cos + coarse_cos * fine_sin
        table_ref[0, rows, lanes] = cosine.astype(jnp.bfloat16)
        table_ref[1, rows, lanes] = (-sine).astype(jnp.bfloat16)


def shift(values, amount):
    amount %= LANES
    return values if amount == 0 else pltpu.roll(values, amount, values.ndim - 1)


def side_by_side(pieces, width):
    lane = lax.broadcasted_iota(jnp.int32, pieces[0].shape, pieces[0].ndim - 1)
    joined = jnp.zeros_like(pieces[0])
    for index, piece in reversed(list(enumerate(pieces))):
        joined = jnp.where(lane < (index + 1) * width, shift(piece, index * width), joined)
    return jnp.where(lane < len(pieces) * width, joined, 0.0)


def forward_kernel(
    peers,
    elevation_ref,
    weight_ref,
    coarse_ref,
    fine_ref,
    turn_ref,
    out_ref,
    rows_ref,
    table_ref,
    flip_ref,
    pack_ref,
):
    cycles = elevation_ref.shape[0]
    turns = turn_ref.shape[1]
    orders = flip_ref.shape[1]
    for turn in range(turns):
        rows_ref[turn * cycles : (turn + 1) * cycles, :] = elevation_ref[
            :, turn * INNER : (turn + 1) * INNER
        ]
    weight = weight_ref[...]
    inner_table(coarse_ref, fine_ref, table_ref, slice(None))
    for part in range(orders // INNER):
        lanes = slice(part * INNER, (part + 1) * INNER)
        even = jnp.dot(rows_ref[...], table_ref[0, :, lanes], preferred_element_type=jnp.float32)
        odd = jnp.dot(rows_ref[...], table_ref[1, :, lanes], preferred_element_type=jnp.float32)
        first = second = None
        for turn in range(turns):
            rows = slice(turn * cycles, (turn + 1) * cycles)
            cosine, sine = turn_ref[0, turn : turn + 1, lanes], turn_ref[1, turn : turn + 1, lanes]
            one = even[rows] * cosine + odd[rows] * sine
            two = odd[rows] * cosine - even[rows] * sine
            first = one if first is None else first + one
            second = two if second is None else second + two
        flip_ref[0, lanes, :cycles] = jnp.transpose(first) * weight
        flip_ref[1, lanes, :cycles] = jnp.transpose(second) * weight

    beside = LANES // cycles
    deep = out_ref.shape[0] // peers
    share = orders // peers
    for row in range(deep):
        pieces = []
        for column in range(beside):
            which, order = divmod(deep * column + row, share)
            pieces.append(flip_ref[which, pl.ds(order, peers, stride=share), :])
        pack_ref[pl.ds(row, peers, stride=deep), :] = side_by_side(pieces, cycles)
    out_ref[...] = pack_ref[...].astype(jnp.bfloat16)


def forward(elevation, weight, coarse, fine, turn, lines, peers):
    cycles, longitudes = elevation.shape
    orders = coarse.shape[2]
    turns = longitudes // INNER
    return pl.pallas_call(
        functools.partial(forward_kernel, peers),
        in_specs=[NEARBY] * 5,
        out_specs=NEARBY,
        out_shape=jax.ShapeDtypeStruct((lines, LANES), jnp.bfloat16),
        scratch_shapes=[
            pltpu.VMEM((turns * cycles, INNER), jnp.bfloat16),
            pltpu.VMEM((2, INNER, orders), jnp.bfloat16),
            pltpu.VMEM((2, orders, LANES), jnp.float32),
            pltpu.VMEM((lines, LANES), jnp.float32),
        ],
        cost_estimate=pl.CostEstimate(
            flops=4 * cycles * longitudes * orders, bytes_accessed=1 << 20, transcendentals=0
        ),
        name="forward_dft",
    )(elevation, weight, coarse, fine, turn)


def split_kernel(flip, place_ref, legendre_ref, half_ref):
    orders = half_ref.shape[0]
    index = jnp.bitwise_xor(place_ref[0], flip)
    for first in range(0, orders, TILE):
        start = pl.multiple_of(index * orders + first, TILE)
        half_ref[first : first + TILE] = jnp.swapaxes(
            legendre_ref[:, pl.ds(start, TILE), :], 0, 1
        )


def part_kernel(place_ref, half_ref, part_ref):
    share = part_ref.shape[0]
    part_ref[...] = half_ref[pl.ds((1 - place_ref[1]) * share, share)]


def divided(kernel, place, values, orders, cycles):
    degrees = values.shape[2]
    return pl.pallas_call(
        kernel,
        in_specs=[SCALARS, NEARBY],
        out_specs=[NEARBY] * len(orders),
        out_shape=[
            jax.ShapeDtypeStruct((count, cycles, degrees), values.dtype) for count in orders
        ],
        cost_estimate=pl.CostEstimate(
            flops=1 << 20, bytes_accessed=4 * cycles * sum(orders) * degrees, transcendentals=0
        ),
        compiler_params=pltpu.CompilerParams(vmem_limit_bytes=ROOM),
    )(place, values)


def table_kernel(which, coarse_ref, fine_ref, table_ref):
    fine_cos, fine_sin = fine_ref[0], fine_ref[1]
    for step in range(FINE):
        coarse_cos = coarse_ref[0, step : step + 1, :]
        coarse_sin = coarse_ref[1, step : step + 1, :]
        if which == "cosine":
            part = coarse_cos * fine_cos - coarse_sin * fine_sin
        else:
            part = -(coarse_sin * fine_cos + coarse_cos * fine_sin)
        table_ref[step * FINE : (step + 1) * FINE, :] = part.astype(jnp.bfloat16)


def table_of(which, coarse, fine):
    shape = (INNER, coarse.shape[2])
    return pl.pallas_call(
        functools.partial(table_kernel, which),
        in_specs=[NEARBY] * 2,
        out_specs=NEARBY,
        out_shape=jax.ShapeDtypeStruct(shape, jnp.bfloat16),
        cost_estimate=pl.CostEstimate(
            flops=1 << 20, bytes_accessed=2 * math.prod(shape), transcendentals=0
        ),
        compiler_params=pltpu.CompilerParams(vmem_limit_bytes=ROOM),
    )(coarse, fine)


def analysis_kernel(near, spot_ref, *refs):
    assignment_ref, moved_ref, *value_refs = refs[: near + 2]
    out_ref, row_ref, left_ref, joined_ref = refs[near + 2 :]
    share, _, two_fields, _ = left_ref.shape
    fields = two_fields // 2
    cycles = value_refs[0].shape[1]
    beside = LANES // cycles
    lines = moved_ref.shape[0]
    block = lines // fields
    deep = block // near
    spot = spot_ref[0]

    for slot in range(fields):
        source = pl.multiple_of(assignment_ref[slot] * block, block)
        row_ref[slot * block : (slot + 1) * block, :] = moved_ref[
            pl.ds(source, block), :
        ].astype(jnp.float32)
    for other in range(near):
        peer = jnp.bitwise_xor(spot, other)
        for row in range(deep):
            taken = row_ref[pl.ds(peer * deep + row, fields, stride=block), :]
            for column in range(beside):
                which, order = divmod(deep * column + row, share)
                left_ref[order, other, which * fields : (which + 1) * fields, :] = shift(
                    taken, -column * cycles
                ).astype(jnp.bfloat16)

    for order in range(share):
        for other in range(near):
            joined_ref[order % 2, other * cycles : (other + 1) * cycles, :] = value_refs[other][
                order
            ]
        left = jnp.concatenate(
            [left_ref[order, other][:, :cycles] for other in range(near)], axis=1
        )
        out_ref[2 * fields * order : 2 * fields * (order + 1), :] = jnp.dot(
            left, joined_ref[order % 2], preferred_element_type=jnp.float32
        ).astype(jnp.bfloat16)


def analyse(spot, assignment, moved, values):
    share, cycles, degrees = values[0].shape
    fields = assignment.shape[0]
    return pl.pallas_call(
        functools.partial(analysis_kernel, len(values)),
        in_specs=[SCALARS] * 2 + [NEARBY] * (1 + len(values)),
        out_specs=NEARBY,
        scratch_shapes=[
            pltpu.VMEM(moved.shape, jnp.float32),
            pltpu.VMEM((share, len(values), 2 * fields, LANES), jnp.bfloat16),
            pltpu.VMEM((2, len(values) * cycles, degrees), jnp.bfloat16),
        ],
        out_shape=jax.ShapeDtypeStruct((share * 2 * fields, degrees), jnp.bfloat16),
        cost_estimate=pl.CostEstimate(
            flops=4 * fields * share * cycles * degrees * len(values),
            bytes_accessed=4 << 20,
            transcendentals=0,
        ),
        compiler_params=pltpu.CompilerParams(vmem_limit_bytes=ROOM),
        name="analysis",
    )(spot, assignment, moved, *values)


def synthesis_kernel(near, spot_ref, first_ref, *refs):
    coefficient_ref, *value_refs = refs[: near + 1]
    out_ref, right_ref, row_ref, joined_ref = refs[near + 1 :]
    share, _, two_fields, _ = right_ref.shape
    fields = two_fields // 2
    cycles = value_refs[0].shape[1]
    beside = LANES // cycles
    lines = out_ref.shape[0]
    block = lines // fields
    deep = block // near
    dims = (((1,), (1,)), ((), ()))
    for order in range(share):
        factor = jnp.where(first_ref[0] + order == 0, 1.0, 2.0).astype(jnp.float32)
        for other in range(near):
            skip = 0 if value_refs[other].shape[0] == share else share * (spot_ref[0] % 2)
            joined_ref[order % 2, other * cycles : (other + 1) * cycles, :] = value_refs[other][
                skip + order
            ]
        product = factor * lax.dot_general(
            coefficient_ref[2 * fields * order : 2 * fields * (order + 1), :],
            joined_ref[order % 2],
            dims,
            preferred_element_type=jnp.float32,
        )
        for other in range(near):
            right_ref[order, other, :, :cycles] = product[
                :, other * cycles : (other + 1) * cycles
            ]
    for other in range(near):
        peer = jnp.bitwise_xor(spot_ref[0], other)
        for row in range(deep):
            pieces = []
            for column in range(beside):
                which, own = divmod(deep * column + row, share)
                pieces.append(right_ref[own, other, which * fields : (which + 1) * fields, :])
            row_ref[pl.ds(peer * deep + row, fields, stride=block), :] = side_by_side(
                pieces, cycles
            )
    out_ref[...] = row_ref[...].astype(jnp.bfloat16)


def synthesise(spot, first, coefficients, values, lines):
    share = min(value.shape[0] for value in values)
    _, cycles, degrees = values[0].shape
    fields = coefficients.shape[0] // (2 * share)
    return pl.pallas_call(
        functools.partial(synthesis_kernel, len(values)),
        in_specs=[SCALARS] * 2 + [NEARBY] * (1 + len(values)),
        out_specs=NEARBY,
        scratch_shapes=[
            pltpu.VMEM((share, len(values), 2 * fields, LANES), jnp.float32),
            pltpu.VMEM((lines, LANES), jnp.float32),
            pltpu.VMEM((2, len(values) * cycles, degrees), jnp.bfloat16),
        ],
        out_shape=jax.ShapeDtypeStruct((lines, LANES), jnp.bfloat16),
        cost_estimate=pl.CostEstimate(
            flops=4 * fields * share * cycles * degrees * len(values),
            bytes_accessed=4 << 20,
            transcendentals=0,
        ),
        compiler_params=pltpu.CompilerParams(vmem_limit_bytes=ROOM),
        name="synthesis",
    )(spot, first, coefficients, *values)


def inverse_kernel(
    peers,
    moved_ref,
    cosine_ref,
    sine_ref,
    turn_ref,
    out_ref,
    rows_ref,
    row_ref,
    flip_ref,
    part_ref,
    sems,
):
    parts, cycles, span = part_ref.shape
    count = span // INNER
    orders = flip_ref.shape[1]
    row_ref[...] = moved_ref[...].astype(jnp.float32)
    deep = moved_ref.shape[0] // peers
    share = orders // peers
    for row in range(deep):
        taken = row_ref[pl.ds(row, peers, stride=deep), :]
        for column in range(LANES // cycles):
            which, order = divmod(deep * column + row, share)
            flip_ref[which, pl.ds(order, peers, stride=share), :] = shift(
                taken, -column * cycles
            )
    first = jnp.transpose(flip_ref[0])[:cycles]
    second = jnp.transpose(flip_ref[1])[:cycles]
    dims = (((1,), (1,)), ((), ()))
    copies = []
    for part in range(parts):
        for step in range(count):
            rows = slice(step * cycles, (step + 1) * cycles)
            turn = part * count + step
            cosine, sine = turn_ref[0, turn : turn + 1, :], turn_ref[1, turn : turn + 1, :]
            rows_ref[part % 2, 0, rows, :] = (first * cosine - second * sine).astype(jnp.bfloat16)
            rows_ref[part % 2, 1, rows, :] = (first * sine + second * cosine).astype(jnp.bfloat16)
        result = lax.dot_general(
            rows_ref[part % 2, 0], cosine_ref[...], dims, preferred_element_type=jnp.float32
        ) + lax.dot_general(
            rows_ref[part % 2, 1], sine_ref[...], dims, preferred_element_type=jnp.float32
        )
        for step in range(count):
            part_ref[part, :, step * INNER : (step + 1) * INNER] = result[
                step * cycles : (step + 1) * cycles
            ]
        copy = pltpu.make_async_copy(
            part_ref.at[part], out_ref.at[:, part * span : (part + 1) * span], sems.at[part]
        )
        copy.start()
        copies.append(copy)
    for copy in copies:
        copy.wait()


def inverse(moved, tables, turn, cycles, longitudes, peers):
    orders = turn.shape[2]
    count = 6
    parts = longitudes // INNER // count
    return pl.pallas_call(
        functools.partial(inverse_kernel, peers),
        in_specs=[NEARBY] * 4,
        out_specs=pl.BlockSpec(memory_space=pltpu.HBM),
        out_shape=jax.ShapeDtypeStruct((cycles, longitudes), jnp.float32),
        scratch_shapes=[
            pltpu.VMEM((2, 2, count * cycles, orders), jnp.bfloat16),
            pltpu.VMEM(moved.shape, jnp.float32),
            pltpu.VMEM((2, orders, LANES), jnp.float32),
            pltpu.VMEM((parts, cycles, count * INNER), jnp.float32),
            pltpu.SemaphoreType.DMA((parts,)),
        ],
        cost_estimate=pl.CostEstimate(
            flops=4 * cycles * longitudes * orders, bytes_accessed=1 << 20, transcendentals=0
        ),
        compiler_params=pltpu.CompilerParams(vmem_limit_bytes=ROOM),
        name="inverse_dft",
    )(moved, *tables, turn)


def local(elevation, legendre, cycle_weight, love_factor, assignment):
    _, cycle_dev, longitudes = elevation.shape
    orders_dev, degrees = legendre.shape[1:]
    groups = lax.axis_size("cons")
    cores, near = lax.axis_size(CORE), lax.axis_size(NEAR)
    deep, far = lax.axis_size(DEEP), lax.axis_size(FAR)
    orders = orders_dev * groups
    spot, core = lax.axis_index(NEAR), lax.axis_index(CORE)
    side = lax.axis_index("blk_0")
    coarse = jnp.asarray(angle_tables(FINE, FINE, longitudes, orders))
    fine = jnp.asarray(angle_tables(FINE, 1, longitudes, orders))
    turn = jnp.asarray(angle_tables(longitudes // INNER, INNER, longitudes, orders))

    def swapped(values, other):
        pairs = [(index, index ^ other) for index in range(near)]
        return lax.ppermute(values, NEAR[::-1], pairs)

    half, share = orders_dev // cores, orders_dev // near
    place = jnp.stack([core, side]).astype(jnp.int32)

    def exchanged(packed, axes):
        peers = lax.axis_size(axes)
        tiles = packed.reshape(peers, -1, LANES)
        tiles = lax.all_to_all(tiles, axes, 0, 0, tiled=True)
        return tiles.reshape(-1, LANES)

    def half_of(flip):
        kernel = functools.partial(split_kernel, flip)
        return divided(kernel, place, legendre, (half,), cycle_dev)[0]

    sent, own = half_of(1), half_of(0)

    def part_of(values):
        return divided(part_kernel, place, values, (share,), cycle_dev)[0]

    met = swapped(sent, 1)
    own_side = swapped(part_of(own), 2)
    sent_part = lax.dynamic_slice_in_dim(sent, (1 - side) * share, share, 0)
    met_side = swapped(sent_part, 3)
    tables = [table_of(which, coarse, fine) for which in ("cosine", "sine")]
    lines = groups * orders_dev * 2 // (LANES // cycle_dev)
    packed = forward(elevation[0], cycle_weight[None, :], coarse, fine, turn, lines, groups * cores)
    moved = exchanged(packed, ("cons", CORE))
    partial = analyse(core[None].astype(jnp.int32), assignment, moved, [own, met])
    rows = partial.shape[0] // far
    arrived = lax.all_to_all(partial.reshape(far, rows, degrees), FAR, 0, 0, tiled=True)
    analysis = jnp.sum(arrived.astype(jnp.float32), axis=0)
    scaled = (analysis * love_factor[None, :]).astype(jnp.bfloat16)
    copies = jnp.broadcast_to(scaled[None], (deep, rows, degrees))
    coefficients = lax.all_to_all(copies, DEEP, 0, 0, tiled=True)
    first = ((lax.axis_index("cons") * near + spot) * share)[None].astype(jnp.int32)
    synthesis = synthesise(
        spot[None].astype(jnp.int32),
        first,
        coefficients.reshape(-1, degrees),
        [own, own_side, met, met_side],
        lines,
    )
    returned = exchanged(synthesis, ("cons", *NEAR))
    return inverse(returned, tables, turn, cycle_dev, longitudes, groups * near)[None]


def solution(mesh):
    torus = Mesh(
        mesh.devices.reshape(mesh.shape["cons"], 2, 8, 2), ("cons", *BLK)
    )
    placed = (P("cons", BLK, None), P(BLK, "cons", None), P(BLK), P(), P())
    return jax.shard_map(
        local, mesh=torus, in_specs=placed, out_specs=P("cons", BLK, None), check_vma=False
    )
```
